32 devices in a mesh: cfg: 2 (over x), ta: 16 (over z, y, core).
Axes of the slice: x: 2, y: 2, z: 4, core: 2. Of those that a mesh axis runs over, the one named last changes fastest.
Arguments:
- fine_source: bfloat16 [32, 128, 2, 2, 24, 128], P('cfg', 'ta'), parts along dimension 0, may hold values from -24 to 24
- projectors: bfloat16 [32, 128, 2304], P(('cfg', 'ta')), parts along dimension 0, may hold values from -0.21875 to 0.21875
- stencil_links: bfloat16 [32, 8, 48, 864], P(('cfg', 'ta')), parts along dimension 0, may hold values from -0.21875 to 0.21875
- quark_mass: float32 [2], P('cfg'), parts along dimension 0, may hold values from 1.5 to 3
Outputs:
- solution: float32 [32, 8, 96, 128], P(('cfg', 'ta')), parts along dimension 0
- residual: float32 [32, 8, 96, 128], P(('cfg', 'ta')), parts along dimension 0
The draws below stay inside these ranges and needn't reach their ends.
There are 2 independent parts, one for each index of `cfg`. The reference program is written for one: setup_inputs(seed, part) draws one part's arguments, and reference() takes and returns one part's arrays. A program takes and returns all parts, laid end to end along the dimension named above; each array names one. Nothing has to cross between parts.
All inputs are finite; a program needn't handle non-finite values.
Results may differ from the reference program's by a relative error of at most 0.012.
The reference program's roundings to bfloat16 on the way count: a program that leaves them out, or rounds other values in their place, can miss the bound.
Values may be sent and summed in bfloat16 or wider, within the bound.
A program may use at most 128 MiB of HBM per device.

```python
import math
import jax
import jax.numpy as jnp
from jax import lax

NV = 24
LX = 4
LY = 2
LZ = 8
YX = 16
RHS = 128
ITERS = 3
CC = 48
LT = 2
PLANES = 16
XY = 8
COLS = 128
FK = 24


def draw_fine_source(key, part):
    shape_full = (PLANES, COLS, 2, 2, FK, RHS)
    key_base = jax.random.fold_in(key, 11)
    first_key = jax.random.fold_in(key_base, 0)
    third_key = jax.random.fold_in(key_base, 2)
    slices = (jnp.arange(PLANES) // LZ).astype(jnp.float32) / max(LT - 1, 1)
    values = jax.random.truncated_normal(first_key, -4.0, 4.0, shape_full)
    scales = jnp.exp(jax.random.uniform(third_key, (PLANES, COLS, 1, 1, 1, 1), minval=math.log(0.25), maxval=math.log(2.5)))
    time_ramp = jnp.exp(math.log(3.0) * slices - 0.5 * math.log(3.0))
    return (values * scales * time_ramp.reshape(PLANES, 1, 1, 1, 1, 1)).astype(jnp.bfloat16)


def steps_of(rng, extent, cuts, low, high):
    loudness, own = 1.0, jax.random.fold_in(rng, 6)
    for axis_at, parts in cuts:
        heights = jnp.exp(jax.random.uniform(jax.random.fold_in(own, axis_at), (parts,), jnp.float32, low / len(cuts), high / len(cuts)))
        loudness = loudness * jnp.repeat(heights, extent[axis_at] // parts).reshape([-1 if axis == axis_at else 1 for axis in range(len(extent))])
    return loudness


def normal_values(own_key, extent, spread, most, pieces=(), held_as=jnp.bfloat16):
    gain = steps_of(own_key, extent, pieces, -0.22, 0.18) if pieces else 1.0
    array = jax.random.normal(own_key, extent, jnp.float32) * spread * gain
    return jnp.minimum(jnp.maximum(array, -most), most).astype(held_as)


def setup_inputs(seed: int = 0, part: int = 0) -> dict:
    key_of = jax.random.split(jax.random.key(seed), 5)
    part_splits = jax.random.split(jax.random.fold_in(key_of[4], part), 5)
    return {
        "fine_source": draw_fine_source(jax.random.fold_in(jax.random.fold_in(key_of[4], part), 71), part),
        "projectors": normal_values(part_splits[1], (PLANES, COLS, 4 * NV * FK), (2 * YX * FK) ** -0.5, 0.21875, ((0, 16),)),
        "stencil_links": normal_values(part_splits[2], (PLANES, XY, CC, 18 * CC), (18 * CC) ** -0.5, 0.21875, ((0, 16),)),
        "quark_mass": jnp.clip(jax.random.uniform(part_splits[3], (1,), jnp.float32, 1.5, 3.0), 1.5, 3.0),
    }


roll_table = ((0, 0), (3, -1), (3, 1), (2, -1), (2, 1), (1, -1), (1, 1), (0, -1), (0, 1))

def restrict_plane(operands):
    fine_plane, proj_plane = operands
    fine_plane = fine_plane.astype(jnp.float32).reshape(XY, YX, 2, 2, FK, RHS)
    proj_plane = proj_plane.astype(jnp.float32).reshape(XY, YX, 2, NV, 2, FK)
    proj_re = proj_plane[:, :, :, :, 0, :]
    proj_im = proj_plane[:, :, :, :, 1, :]
    fine_re = fine_plane[:, :, 0]
    fine_im = fine_plane[:, :, 1]
    highest = lax.Precision.HIGHEST
    result_re = jnp.einsum('sohvk,sohkr->shvr', proj_re, fine_re, precision=highest) + jnp.einsum('sohvk,sohkr->shvr', proj_im, fine_im, precision=highest)
    result_im = jnp.einsum('sohvk,sohkr->shvr', proj_re, fine_im, precision=highest) - jnp.einsum('sohvk,sohkr->shvr', proj_im, fine_re, precision=highest)
    return jnp.stack([result_re, result_im], axis=1).reshape(XY, 2 * CC, RHS)

def apply_operator(vector, stencil_links, quark_mass):
    highest = lax.Precision.HIGHEST
    rounded = lax.optimization_barrier(vector.astype(jnp.bfloat16)).astype(jnp.float32)
    lattice = rounded.reshape(LT, LZ, LY, LX, 2 * CC, RHS)
    link_view = stencil_links.reshape(PLANES, XY, CC, 9, 2, CC)
    total_re = quark_mass[0] * rounded[:, :, :CC]
    total_im = quark_mass[0] * rounded[:, :, CC:]
    for direction in range(9):
        axis_number, offset = roll_table[direction]
        if direction == 0:
            neighbour = lattice
        else:
            neighbour = jnp.roll(lattice, offset, axis=axis_number)
        neighbour = neighbour.reshape(PLANES, XY, 2 * CC, RHS)
        near_re = neighbour[:, :, :CC]
        near_im = neighbour[:, :, CC:]
        link_re = link_view[:, :, :, direction, 0, :].astype(jnp.float32)
        link_im = link_view[:, :, :, direction, 1, :].astype(jnp.float32)
        total_re = total_re + jnp.einsum('psij,psjr->psir', link_re, near_re, precision=highest) - jnp.einsum('psij,psjr->psir', link_im, near_im, precision=highest)
        total_im = total_im + jnp.einsum('psij,psjr->psir', link_re, near_im, precision=highest) + jnp.einsum('psij,psjr->psir', link_im, near_re, precision=highest)
    return jnp.concatenate([total_re, total_im], axis=2)

def inner_product(left, right):
    left_re = left[:, :, :CC]
    left_im = left[:, :, CC:]
    right_re = right[:, :, :CC]
    right_im = right[:, :, CC:]
    return (lax.optimization_barrier(jnp.sum(left_re * right_re + left_im * right_im, axis=(0, 1, 2))), lax.optimization_barrier(jnp.sum(left_re * right_im - left_im * right_re, axis=(0, 1, 2))))

def scaled(vector, factor_re, factor_im):
    vector_re = vector[..., :CC, :]
    vector_im = vector[..., CC:, :]
    return jnp.concatenate([factor_re * vector_re - factor_im * vector_im, factor_re * vector_im + factor_im * vector_re], axis=-2)

def reference(fine_source, projectors, stencil_links, quark_mass):
    source = lax.map(restrict_plane, (fine_source, projectors))
    solution = jnp.zeros_like(source)
    residual = source
    basis_q = []
    basis_p = []
    for iteration in range(ITERS):
        direction = residual
        mapped = apply_operator(residual, stencil_links, quark_mass)
        coeffs = [inner_product(earlier, mapped) for earlier in basis_q]
        for number in range(iteration):
            mapped = mapped - scaled(basis_q[number], coeffs[number][0], coeffs[number][1])
            direction = direction - scaled(basis_p[number], coeffs[number][0], coeffs[number][1])
        squared = inner_product(mapped, mapped)[0]
        factor = 1.0 / jnp.sqrt(squared + 1e-06)
        unit_q = mapped * factor
        unit_p = direction * factor
        alpha_re, alpha_im = inner_product(unit_q, residual)
        solution = solution + scaled(unit_p, alpha_re, alpha_im)
        residual = residual - scaled(unit_q, alpha_re, alpha_im)
        basis_q.append(unit_q)
        basis_p.append(unit_p)
    return (solution, residual)
```

```python
import functools
import math

import jax
import jax.numpy as jnp
from jax import lax
from jax.experimental import pallas as pl
from jax.experimental.pallas import tpu as pltpu
from jax.sharding import PartitionSpec as P

LX = 4
LZ = 8
ITERS = 3


def from_behind(value, axis, steps):
    count = lax.axis_size(axis)
    pairs = [(source, (source + steps) % count) for source in range(count)]
    return lax.ppermute(value, axis, pairs)


def real_weights(proj_view):
    proj_re = proj_view[..., 0, :]
    proj_im = proj_view[..., 1, :]
    first_row = jnp.stack([proj_re, proj_im], axis=-4)
    second_row = jnp.stack([-proj_im, proj_re], axis=-4)
    return jnp.stack([first_row, second_row], axis=-5)


def inner_local(left, right, comp_count):
    left_re = left[:, :comp_count]
    left_im = left[:, comp_count:]
    right_re = right[:, :comp_count]
    right_im = right[:, comp_count:]
    return (
        jnp.sum(left_re * right_re + left_im * right_im, axis=(0, 1)),
        jnp.sum(left_re * right_im - left_im * right_re, axis=(0, 1)),
    )


def scaled(vector, factor_re, factor_im, comp_count):
    vector_re = vector[:, :comp_count]
    vector_im = vector[:, comp_count:]
    return jnp.concatenate(
        [
            factor_re * vector_re - factor_im * vector_im,
            factor_re * vector_im + factor_im * vector_re,
        ],
        axis=1,
    )


def shards_general(fine_source, projectors, stencil_links, quark_mass):
    comp_count = stencil_links.shape[2]
    null_count = comp_count // 2
    site_count = stencil_links.shape[1]
    column_count = projectors.shape[1]
    block_count = column_count // site_count
    fine_count = fine_source.shape[4]
    rhs_count = fine_source.shape[5]
    plane_count = fine_source.shape[0]
    moved_proj = lax.all_to_all(projectors, "ta", split_axis=1, concat_axis=0, tiled=True)
    local_columns = fine_source.shape[1]
    group_size = math.gcd(block_count, local_columns)
    groups = local_columns // group_size
    weights = real_weights(
        moved_proj.reshape(plane_count, groups, group_size, 2, null_count, 2, fine_count)
    )
    fine_local = fine_source.reshape(plane_count, groups, group_size, 2, 2, fine_count, rhs_count)
    partial_sums = jnp.einsum(
        "pmgdchvk,pmgchkr->pmdhvr", weights, fine_local, preferred_element_type=jnp.float32
    )
    partial_sums = partial_sums.reshape(plane_count, groups, 2 * comp_count, rhs_count)
    collected = lax.all_to_all(partial_sums, "ta", split_axis=0, concat_axis=1, tiled=True)
    source = jnp.sum(
        collected.reshape(site_count, block_count // group_size, 2 * comp_count, rhs_count), axis=1
    )
    link_view = stencil_links.reshape(site_count, comp_count, 9, 2, comp_count)
    link_re = link_view[:, :, :, 0, :]
    link_im = link_view[:, :, :, 1, :]
    upper_rows = jnp.stack([link_re, -link_im], axis=3)
    lower_rows = jnp.stack([link_im, link_re], axis=3)
    real_operator = jnp.stack([upper_rows, lower_rows], axis=1).reshape(
        site_count, 2 * comp_count, 18 * comp_count
    )
    mass_value = quark_mass[0]
    z_position = lax.axis_index("ta") % LZ
    line_count = site_count // LX

    def flatten_sites(shifted):
        return shifted.reshape(site_count, 2 * comp_count, rhs_count)

    solution = jnp.zeros_like(source)
    residual = source
    basis_q = []
    basis_p = []
    for iteration in range(ITERS):
        direction = residual
        rounded = residual.astype(jnp.bfloat16)
        plane_view = rounded.reshape(line_count, LX, 2 * comp_count, rhs_count)
        x_plus = flatten_sites(jnp.roll(plane_view, -1, axis=1))
        x_minus = flatten_sites(jnp.roll(plane_view, 1, axis=1))
        y_plus = flatten_sites(jnp.roll(plane_view, -1, axis=0))
        y_minus = flatten_sites(jnp.roll(plane_view, 1, axis=0))
        z_plus_near = from_behind(rounded, "ta", -1)
        z_minus_near = from_behind(rounded, "ta", 1)
        upper_pair = from_behind(jnp.stack([rounded, z_minus_near], axis=0), "ta", -LZ)
        lower_pair = from_behind(jnp.stack([rounded, z_plus_near], axis=0), "ta", LZ)
        t_plus = upper_pair[0]
        t_minus = lower_pair[0]
        z_plus = jnp.where(z_position == LZ - 1, lower_pair[1], z_plus_near)
        z_minus = jnp.where(z_position == 0, upper_pair[1], z_minus_near)
        stacked = jnp.stack(
            [rounded, x_plus, x_minus, y_plus, y_minus, z_plus, z_minus, t_plus, t_minus], axis=1
        )
        stacked = stacked.reshape(site_count, 18 * comp_count, rhs_count)
        product = jnp.einsum(
            "sij,sjr->sir", real_operator, stacked, preferred_element_type=jnp.float32
        )
        mapped = product + mass_value * rounded.astype(jnp.float32)
        square_loc = inner_local(mapped, mapped, comp_count)[0]
        cross_re, cross_im = inner_local(mapped, residual, comp_count)
        if iteration > 0:
            coef_pairs = [inner_local(earlier, mapped, comp_count) for earlier in basis_q]
            back_pairs = [inner_local(earlier, residual, comp_count) for earlier in basis_q]
            coef_re = jnp.stack([pair[0] for pair in coef_pairs])
            coef_im = jnp.stack([pair[1] for pair in coef_pairs])
            back_re = jnp.stack([pair[0] for pair in back_pairs])
            back_im = jnp.stack([pair[1] for pair in back_pairs])
        else:
            coef_re = jnp.zeros((1, rhs_count), jnp.float32)
            coef_im = jnp.zeros((1, rhs_count), jnp.float32)
            back_re = jnp.zeros((1, rhs_count), jnp.float32)
            back_im = jnp.zeros((1, rhs_count), jnp.float32)
        square_all, cross_re, cross_im, coef_re, coef_im, back_re, back_im = lax.psum(
            (square_loc, cross_re, cross_im, coef_re, coef_im, back_re, back_im), "ta"
        )
        squared = square_all
        proj_re = cross_re
        proj_im = cross_im
        for number in range(iteration):
            mapped = mapped - scaled(basis_q[number], coef_re[number], coef_im[number], comp_count)
            direction = direction - scaled(
                basis_p[number], coef_re[number], coef_im[number], comp_count
            )
            squared = squared - (
                coef_re[number] * coef_re[number] + coef_im[number] * coef_im[number]
            )
            proj_re = proj_re - (
                coef_re[number] * back_re[number] + coef_im[number] * back_im[number]
            )
            proj_im = proj_im - (
                coef_re[number] * back_im[number] - coef_im[number] * back_re[number]
            )
        factor = 1.0 / jnp.sqrt(squared + 1e-06)
        unit_q = mapped * factor
        unit_p = direction * factor
        alpha_re = proj_re * factor
        alpha_im = proj_im * factor
        solution = solution + scaled(unit_p, alpha_re, alpha_im, comp_count)
        residual = residual - scaled(unit_q, alpha_re, alpha_im, comp_count)
        basis_q.append(unit_q)
        basis_p.append(unit_p)
    return (
        solution.reshape(1, site_count, 2 * comp_count, rhs_count),
        residual.reshape(1, site_count, 2 * comp_count, rhs_count),
    )


MESH = pl.DeviceIdType.MESH


def flipped(number, mask, bits):
    total = 0
    for bit in range(bits):
        size = 1 << bit
        total = total + (((number // size) % 2 + (mask // size) % 2) % 2) * size
    return total


def swapped(value):
    return pltpu.roll(value, value.shape[-1] // 2, value.ndim - 1)


def lower_lanes(shape):
    return lax.broadcasted_iota(jnp.int32, shape, len(shape) - 1) < shape[-1] // 2


def turned(value):
    other = swapped(value)
    return jnp.where(lower_lanes(value.shape), -other, other)


def widened(rounded):
    return jnp.concatenate(
        [rounded, turned(rounded.astype(jnp.float32)).astype(jnp.bfloat16)], axis=0
    )


def times(factor, value):
    return factor[0] * value + factor[1] * turned(value)


def total_wait(region, sem):
    pltpu.make_async_copy(region, region, sem).wait()


def transposed(value, columns, comps):
    row = lax.broadcasted_iota(jnp.int32, value.shape, 0)
    chunk = lax.broadcasted_iota(jnp.int32, value.shape, 1) // comps
    width = value.shape[1]
    bits = columns.bit_length() - 1
    for bit in range(bits):
        size = 1 << bit
        moved = pltpu.roll(value, width - size * comps, 1)
        value = jnp.where((row // size) % 2 == 1, moved, value)
    for bit in range(bits):
        size = 1 << bit
        moved = pltpu.roll(value, size, 0)
        value = jnp.where((chunk // size) % 2 == 1, moved, value)
    for bit in range(bits):
        size = 1 << bit
        moved = pltpu.roll(value, width - size * comps, 1)
        value = jnp.where((row // size) % 2 == 1, moved, value)
    return value


def solve_kernel(
    count, sites, comps,
    mass_ref, proj_hbm, fine_hbm, links_hbm,
    sol_ref, res_ref,
    proj_ref, fine_ref, links_ref, near_ref, zlinks_ref, tlinks_ref,
    weights_in, rights_ref, part_keep, part_out, part_in, sum_out, hi_out, source_ref,
    first_round, first_z, first_t,
    wide_ref, round_ref, halo_ref, acc_ref, sol_half, res_half, basis_q, basis_p, stat_out, stat_in,
    local_sem, wsend, wrecv, psend, precv, ssend, srecv, tsend, trecv, zsend, zrecv,
    hsend, hrecv, gsend, grecv,
):
    me = lax.axis_index("ta")
    bits = count.bit_length() - 1
    core = me % 2
    chip = me // 2
    partner = chip * 2 + 1 - core
    chips = count // 2
    far = chips // 2
    turns = [(1 - 2 * ((me // (1 << bit)) % 2)) * (1 << bit) for bit in range(bits)]
    others = [me]
    for step in range(1, count):
        top = step.bit_length() - 1
        others.append(others[step - (1 << top)] + turns[top])
    null = comps // 2
    rhs = fine_ref.shape[2]
    columns = proj_ref.shape[1]
    width = columns * comps
    groups = comps // columns

    proj_copy = pltpu.make_async_copy(proj_hbm, proj_ref, local_sem.at[2])
    proj_copy.start()
    barrier = pltpu.get_barrier_semaphore()
    for other in others[:0:-1]:
        pl.semaphore_signal(barrier, inc=1, device_id={"ta": other}, device_id_type=MESH)
    fine_copy = pltpu.make_async_copy(fine_hbm, fine_ref, local_sem.at[0])
    fine_copy.start()
    links_copy = pltpu.make_async_copy(links_hbm, links_ref, local_sem.at[1])
    links_copy.start()
    proj_copy.wait()
    pl.semaphore_wait(barrier, count - 1)

    def weights_copy(other, origin):
        return pltpu.make_async_remote_copy(
            src_ref=proj_ref.at[other], dst_ref=weights_in.at[origin],
            send_sem=wsend.at[0], recv_sem=wrecv.at[origin],
            device_id={"ta": other}, device_id_type=MESH,
        )

    order = list(range(1, 4)) + list(range(count // 2, count)) + list(range(4, count // 2))
    for step in order:
        weights_copy(others[step], me).start()

    fine_copy.wait()

    def build_right(plane, carry):
        fine = fine_ref[plane].astype(jnp.float32).reshape(columns, 2, 2, null, rhs)
        turned_order = [fine[(columns - at) % columns] for at in range(columns)]
        for half in range(2):
            picked = [
                block[part, half] for block in turned_order for part in range(2)
            ]
            rights_ref[plane, :, half * rhs : (half + 1) * rhs] = jnp.concatenate(
                picked, axis=0
            ).astype(jnp.bfloat16)
        return carry

    lax.fori_loop(0, count, build_right, 0)

    links_copy.wait()
    for site in range(sites):
        near_ref[site] = links_ref[site, :, : 10 * comps]
        zlinks_ref[site] = links_ref[site, :, 10 * comps : 14 * comps]
        tlinks_ref[site] = links_ref[site, :, 14 * comps : 18 * comps]

    def restricted(plane, raw_ref):
        raw = raw_ref[plane].astype(jnp.float32)
        pieces = [
            transposed(raw[:, group * width : (group + 1) * width], columns, comps)
            for group in range(groups)
        ]
        upper = jnp.concatenate(pieces, axis=0)
        lane = lax.broadcasted_iota(jnp.int32, upper.shape, 1) % comps
        lower = jnp.where(
            lane < null, -pltpu.roll(upper, width - null, 1), pltpu.roll(upper, null, 1)
        )
        left = jnp.concatenate([upper, lower], axis=0).astype(jnp.bfloat16)
        total = jnp.dot(left, rights_ref[plane], preferred_element_type=jnp.float32)
        real = jnp.concatenate([total[:null, :rhs], total[null:comps, rhs:]], axis=0)
        imag = jnp.concatenate(
            [total[comps : comps + null, :rhs], total[comps + null :, rhs:]], axis=0
        )
        low = lower_lanes(real.shape)
        return jnp.stack(
            [jnp.where(low, real, swapped(imag)), jnp.where(low, swapped(real), imag)], axis=0
        )

    def part_copy(slot):
        return pltpu.make_async_remote_copy(
            src_ref=part_out.at[slot], dst_ref=part_in.at[slot],
            send_sem=psend.at[0], recv_sem=precv.at[slot],
            device_id={"ta": partner}, device_id_type=MESH,
        )

    def source_copy(slot, origin):
        return pltpu.make_async_remote_copy(
            src_ref=sum_out.at[slot], dst_ref=source_ref.at[origin],
            send_sem=ssend.at[0], recv_sem=srecv.at[origin],
            device_id={"ta": flipped(chip, slot, bits - 1) * 2 + core}, device_id_type=MESH,
        )

    def first_t_copy(slot):
        return pltpu.make_async_remote_copy(
            src_ref=hi_out.at[slot], dst_ref=first_t.at[chip],
            send_sem=tsend.at[0], recv_sem=trecv.at[0],
            device_id={"ta": (flipped(chip, slot, bits - 1) * 2 + core + count // 2) % count},
            device_id_type=MESH,
        )

    def pair(step):
        other = flipped(chip, step, bits - 1)
        away = other * 2 + 1 - core
        weights_copy(partner, away).wait_recv()
        part_out[step] = restricted(away, weights_in)
        part_copy(step).start()
        kept = other * 2 + core
        weights_copy(partner, kept).wait_recv()
        part_keep[step] = restricted(kept, weights_in)

    def finish(step):
        part_copy(step).wait_recv()
        total = part_keep[step] + part_in[step]
        rounded = total.astype(jnp.bfloat16)
        sum_out[step] = total
        source_copy(step, chip).start()

        @pl.when(step != far)
        def _():
            hi_out[step] = rounded
            first_t_copy(step).start()

        @pl.when(step == far)
        def _():
            first_t[chip] = rounded

    base = (me // LZ) * LZ
    z_at = me % LZ
    above = base + (z_at + 1) % LZ
    below = base + (z_at + LZ - 1) % LZ
    other_time = (me + LZ) % count
    targets = (other_time, above, below)
    lines = sites // LX

    def first_z_copy(which, site):
        return pltpu.make_async_remote_copy(
            src_ref=first_round.at[site], dst_ref=first_z.at[which, site],
            send_sem=zsend.at[0], recv_sem=zrecv.at[which],
            device_id={"ta": targets[1 + which]}, device_id_type=MESH,
        )

    def forward(site):
        first_round[site] = source_ref[site].astype(jnp.bfloat16)
        for which in range(2):
            first_z_copy(which, site).start()

    weights_copy(partner, partner).wait_recv()
    part_out[0] = restricted(partner, weights_in)
    part_copy(0).start()
    part_keep[0] = restricted(me, proj_ref)
    pair(1)
    part_copy(0).wait_recv()
    own = part_keep[0] + part_in[0]
    source_ref[chip] = own
    hi_out[0] = own.astype(jnp.bfloat16)
    first_t_copy(0).start()
    forward(chip)

    def pair_step(step, carry):
        pair(step)
        finish(step - 1)
        return carry

    lax.fori_loop(2, chips, pair_step, 0)
    finish(chips - 1)

    def forward_step(step, carry):
        site = flipped(chip, step, bits - 1)
        source_copy(0, site).wait_recv()
        forward(site)
        return carry

    lax.fori_loop(1, chips, forward_step, 0)

    mass = mass_ref[0]

    def place(site, dx, dy):
        return ((site // LX + dy) % lines) * LX + (site % LX + dx) % LX

    def halo_copy(it, half, which):
        return pltpu.make_async_remote_copy(
            src_ref=round_ref.at[it - 1, half], dst_ref=halo_ref.at[it - 1, half, which],
            send_sem=hsend.at[0], recv_sem=hrecv.at[it - 1, half, which],
            device_id={"ta": targets[which]}, device_id_type=MESH,
        )

    def stat_copy(it, half, other):
        return pltpu.make_async_remote_copy(
            src_ref=stat_out.at[it, half], dst_ref=stat_in.at[it, half, me],
            send_sem=gsend.at[0], recv_sem=grecv.at[it, half],
            device_id={"ta": other}, device_id_type=MESH,
        )

    def residual_at(it, half, site):
        return source_ref[site, half] if it == 0 else res_half[half, site]

    def rounded_at(it, half, site):
        return first_round[site, half] if it == 0 else round_ref[it - 1, half, site]

    def halo_at(it, half, which, site):
        if it > 0:
            return halo_ref[it - 1, half, which, site]
        return first_t[site, half] if which == 0 else first_z[which - 1, site, half]

    def send_halo(it, half):
        for site in range(sites):
            round_ref[it - 1, half, site] = res_half[half, site].astype(jnp.bfloat16)
        for which in range(3):
            halo_copy(it, half, which).start()

    def near_product(it, half):
        for site in range(sites):
            wide_ref[half, site] = widened(rounded_at(it, half, site))
        steps = ((0, 0), (1, 0), (-1, 0), (0, 1), (0, -1))
        for site in range(sites):
            right = jnp.concatenate(
                [wide_ref[half, place(site, dx, dy)] for dx, dy in steps], axis=0
            )
            acc_ref[half, site] = jnp.dot(
                near_ref[site], right, preferred_element_type=jnp.float32
            )

    def z_product(it, half, site):
        right = jnp.concatenate(
            [widened(halo_at(it, half, 2, site)), widened(halo_at(it, half, 1, site))], axis=0
        )
        return acc_ref[half, site] + jnp.dot(
            zlinks_ref[site], right, preferred_element_type=jnp.float32
        )

    def t_product(it, half, site):
        wide = widened(halo_at(it, half, 0, site))
        right = jnp.concatenate([wide, wide], axis=0)
        return acc_ref[half, site] + jnp.dot(
            tlinks_ref[site], right, preferred_element_type=jnp.float32
        )

    def far_product(it, half):
        if it == 0:
            if half == 0:
                total_wait(first_t.at[pl.ds(0, sites - 1)], trecv.at[0])
            first_part, last_part = t_product, z_product
        else:
            halo_copy(it, half, 2).wait_recv()
            halo_copy(it, half, 1).wait_recv()
            first_part, last_part = z_product, t_product
        for site in range(sites):
            acc_ref[half, site] = first_part(it, half, site)
        if it == 0:
            if half == 0:
                for which in range(2):
                    total_wait(first_z.at[which], zrecv.at[which])
        else:
            halo_copy(it, half, 0).wait_recv()
        sums = [0.0] * (3 + 2 * it)
        for site in range(sites):
            product = last_part(it, half, site)
            q = product + mass * rounded_at(it, half, site).astype(jnp.float32)
            acc_ref[half, site] = q
            r = residual_at(it, half, site)
            q_other = swapped(q)
            sums[0] += q * q
            sums[1] += q * r
            sums[2] += q * swapped(r)
            for j in range(it):
                b = basis_q[j, half, site]
                sums[3 + 2 * j] += b * q
                sums[4 + 2 * j] += b * q_other
        lines_of = [jnp.sum(value, axis=0, keepdims=True) for value in sums]
        lines_of += [jnp.zeros((8 - len(lines_of), rhs), jnp.float32)]
        stats = jnp.concatenate(lines_of, axis=0)
        moved = swapped(stats)
        low = lower_lanes(stats.shape)
        reals = stats + moved
        imags = jnp.where(low, stats - moved, moved - stats)
        packed = jnp.concatenate(
            [reals[0:1]]
            + [
                jnp.where(low[0:1], reals[at : at + 1], imags[at + 1 : at + 2])
                for at in (1, 3, 5)
            ],
            axis=0,
        )
        stat_out[it, half] = packed
        for other in others[:0:-1]:
            stat_copy(it, half, other).start()
        stat_in[it, half, me] = packed

    scalars = [([], [], [], []) for _ in range(2)]

    def update(it, half):
        total_wait(stat_in.at[it, half, pl.ds(0, count - 1)], grecv.at[it, half])
        total = jnp.sum(stat_in[it, half], axis=0)
        moved = swapped(total)
        low = lower_lanes(total.shape)
        reals = jnp.where(low, total, moved)
        imags = jnp.where(low, moved, total)
        backs, epsilons, overlaps, _ = scalars[half]
        squared, cross_re, cross_im = reals[0:1], reals[1:2], imags[1:2]
        coefs = [(reals[2 + j : 3 + j], imags[2 + j : 3 + j]) for j in range(it)]
        for j, (c_re, c_im) in enumerate(coefs):
            squared = squared - (c_re * c_re + c_im * c_im) * (1.0 + epsilons[j])
            cross_re = cross_re - (c_re * backs[j][0] + c_im * backs[j][1])
            cross_im = cross_im - (c_re * backs[j][1] - c_im * backs[j][0])
        if it == 2:
            (a_re, a_im), (b_re, b_im) = coefs
            pair_re, pair_im = a_re * b_re + a_im * b_im, a_re * b_im - a_im * b_re
            squared = squared + 2.0 * (pair_re * overlaps[0][0] - pair_im * overlaps[0][1])
        factor = 1.0 / jnp.sqrt(squared + 1e-06)
        alpha = (cross_re * factor, cross_im * factor)
        epsilon = 1e-06 * factor * factor
        if it == 1:
            over = (coefs[0][0] * epsilons[0] * factor, coefs[0][1] * epsilons[0] * factor)
            overlaps.append(over)
            backs[0] = (
                backs[0][0] - (alpha[0] * over[0] - alpha[1] * over[1]),
                backs[0][1] - (alpha[0] * over[1] + alpha[1] * over[0]),
            )
        backs.append((alpha[0] * epsilon, alpha[1] * epsilon))
        epsilons.append(epsilon)
        for site in range(sites):
            residual = residual_at(it, half, site)
            q = acc_ref[half, site]
            p = residual
            for j in range(it):
                q = q - times(coefs[j], basis_q[j, half, site])
                p = p - times(coefs[j], basis_p[j, half, site])
            q = q * factor
            p = p * factor
            if it < ITERS - 1:
                basis_q[it, half, site] = q
                basis_p[it, half, site] = p
            step = times(alpha, p)
            sol_half[half, site] = step if it == 0 else sol_half[half, site] + step
            res_half[half, site] = residual - times(alpha, q)

    for half in range(2):
        near_product(0, half)
    for it in range(ITERS):
        for half in range(2):
            far_product(it, half)
        for half in range(2):
            update(it, half)
            if it < ITERS - 1:
                send_halo(it + 1, half)
                near_product(it + 1, half)
    for from_ref, to_ref in ((sol_half, sol_ref), (res_half, res_ref)):
        for site in range(sites):
            first, second = from_ref[0, site], from_ref[1, site]
            low = lower_lanes(first.shape)
            to_ref[site, :comps] = jnp.where(low, first, swapped(second))
            to_ref[site, comps:] = jnp.where(low, swapped(first), second)

    total_wait(proj_ref.at[pl.ds(0, count - 1)], wsend.at[0])
    total_wait(part_out, psend.at[0])
    total_wait(sum_out.at[pl.ds(0, chips - 1)], ssend.at[0])
    total_wait(hi_out.at[pl.ds(0, chips - 1)], tsend.at[0])
    total_wait(first_z, zsend.at[0])
    total_wait(halo_ref, hsend.at[0])
    total_wait(stat_in.at[:, :, pl.ds(0, count - 1)], gsend.at[0])


def shards_kernel(fine_source, projectors, stencil_links, quark_mass):
    count = lax.axis_size("ta")
    planes, local_columns, _, _, null, rhs = fine_source.shape
    sites, comps = stencil_links.shape[1], stencil_links.shape[2]
    rows = local_columns * 4 * null
    fine = fine_source.reshape(planes, rows, rhs)
    proj = projectors.reshape(count, local_columns, 4 * null * null)
    width = local_columns * comps
    links = stencil_links.reshape(sites, comps, 18 * comps)
    chips = count // 2
    vector = (sites, 2 * comps, rhs)
    f32, bf16 = jnp.float32, jnp.bfloat16
    dma = pltpu.SemaphoreType.DMA
    vmem = pl.BlockSpec(memory_space=pltpu.VMEM)
    hbm = pl.BlockSpec(memory_space=pltpu.HBM)
    parts = (chips, 2, comps, rhs)
    half = (sites, comps, rhs)
    sol, res = pl.pallas_call(
        functools.partial(solve_kernel, count, sites, comps),
        out_shape=[pltpu.VMEM(vector, f32)] * 2,
        in_specs=[pl.BlockSpec(memory_space=pltpu.SMEM), hbm, hbm, hbm],
        out_specs=[vmem, vmem],
        scratch_shapes=[
            pltpu.VMEM(proj.shape, bf16),
            pltpu.VMEM(fine.shape, bf16),
            pltpu.VMEM(links.shape, bf16),
            pltpu.VMEM((sites, comps, 10 * comps), bf16),
            pltpu.VMEM((sites, comps, 4 * comps), bf16),
            pltpu.VMEM((sites, comps, 4 * comps), bf16),
            pltpu.VMEM(proj.shape, bf16),
            pltpu.VMEM((planes, width, 2 * rhs), bf16),
            pltpu.VMEM(parts, f32),
            pltpu.VMEM(parts, f32),
            pltpu.VMEM(parts, f32),
            pltpu.VMEM(parts, f32),
            pltpu.VMEM(parts, bf16),
            pltpu.VMEM((sites, 2, comps, rhs), f32),
            pltpu.VMEM((sites, 2, comps, rhs), bf16),
            pltpu.VMEM((2, sites, 2, comps, rhs), bf16),
            pltpu.VMEM((sites, 2, comps, rhs), bf16),
            pltpu.VMEM((2, sites, 2 * comps, rhs), bf16),
            pltpu.VMEM((ITERS - 1, 2, *half), bf16),
            pltpu.VMEM((ITERS - 1, 2, 3, *half), bf16),
            pltpu.VMEM((2, *half), f32),
            pltpu.VMEM((2, *half), f32),
            pltpu.VMEM((2, *half), f32),
            pltpu.VMEM((ITERS - 1, 2, *half), f32),
            pltpu.VMEM((ITERS - 1, 2, *half), f32),
            pltpu.VMEM((ITERS, 2, 4, rhs), f32),
            pltpu.VMEM((ITERS, 2, count, 4, rhs), f32),
            dma((3,)),
            dma((1,)),
            dma((count,)),
            dma((1,)),
            dma((chips,)),
            dma((1,)),
            dma((chips,)),
            dma((1,)),
            dma((1,)),
            dma((1,)),
            dma((2,)),
            dma((1,)),
            dma((ITERS - 1, 2, 3)),
            dma((1,)),
            dma((ITERS, 2)),
        ],
        compiler_params=pltpu.CompilerParams(
            collective_id=0, has_side_effects=True, vmem_limit_bytes=60 * 1024 * 1024
        ),
    )(quark_mass, proj, fine, links)
    return sol.reshape(1, *vector), res.reshape(1, *vector)


def shards(fine_source, projectors, stencil_links, quark_mass):
    count = lax.axis_size("ta")
    sites = stencil_links.shape[1]
    local_columns = fine_source.shape[1]
    block = projectors.shape[1] // sites
    fits = (
        count == 2 * LZ
        and count == 2 * sites
        and count & (count - 1) == 0
        and block == 2 * local_columns
        and stencil_links.shape[2] % local_columns == 0
        and fine_source.shape[0] == count
        and ITERS == 3
        and fine_source.shape[5] % 2 == 0
    )
    chosen = shards_kernel if fits else shards_general
    return chosen(fine_source, projectors, stencil_links, quark_mass)


def solution(mesh):
    return jax.shard_map(
        shards,
        mesh=mesh,
        in_specs=(
            P("cfg", "ta", None, None, None, None),
            P(("cfg", "ta"), None, None),
            P(("cfg", "ta"), None, None, None),
            P("cfg"),
        ),
        out_specs=(P(("cfg", "ta"), None, None, None), P(("cfg", "ta"), None, None, None)),
        check_vma=False,
    )
```

```python
import functools
import math

import jax
import jax.numpy as jnp
from jax import lax
from jax.experimental import pallas as pl
from jax.experimental.pallas import tpu as pltpu
from jax.sharding import PartitionSpec as P

LX = 4
LZ = 8
ITERS = 3


def from_behind(value, axis, steps):
    count = lax.axis_size(axis)
    pairs = [(source, (source + steps) % count) for source in range(count)]
    return lax.ppermute(value, axis, pairs)


def real_weights(proj_view):
    proj_re = proj_view[..., 0, :]
    proj_im = proj_view[..., 1, :]
    first_row = jnp.stack([proj_re, proj_im], axis=-4)
    second_row = jnp.stack([-proj_im, proj_re], axis=-4)
    return jnp.stack([first_row, second_row], axis=-5)


def inner_local(left, right, comp_count):
    left_re = left[:, :comp_count]
    left_im = left[:, comp_count:]
    right_re = right[:, :comp_count]
    right_im = right[:, comp_count:]
    return (
        jnp.sum(left_re * right_re + left_im * right_im, axis=(0, 1)),
        jnp.sum(left_re * right_im - left_im * right_re, axis=(0, 1)),
    )


def scaled(vector, factor_re, factor_im, comp_count):
    vector_re = vector[:, :comp_count]
    vector_im = vector[:, comp_count:]
    return jnp.concatenate(
        [
            factor_re * vector_re - factor_im * vector_im,
            factor_re * vector_im + factor_im * vector_re,
        ],
        axis=1,
    )


def shards_general(fine_source, projectors, stencil_links, quark_mass):
    comp_count = stencil_links.shape[2]
    null_count = comp_count // 2
    site_count = stencil_links.shape[1]
    column_count = projectors.shape[1]
    block_count = column_count // site_count
    fine_count = fine_source.shape[4]
    rhs_count = fine_source.shape[5]
    plane_count = fine_source.shape[0]
    moved_proj = lax.all_to_all(projectors, "ta", split_axis=1, concat_axis=0, tiled=True)
    local_columns = fine_source.shape[1]
    group_size = math.gcd(block_count, local_columns)
    groups = local_columns // group_size
    weights = real_weights(
        moved_proj.reshape(plane_count, groups, group_size, 2, null_count, 2, fine_count)
    )
    fine_local = fine_source.reshape(plane_count, groups, group_size, 2, 2, fine_count, rhs_count)
    partial_sums = jnp.einsum(
        "pmgdchvk,pmgchkr->pmdhvr", weights, fine_local, preferred_element_type=jnp.float32
    )
    partial_sums = partial_sums.reshape(plane_count, groups, 2 * comp_count, rhs_count)
    collected = lax.all_to_all(partial_sums, "ta", split_axis=0, concat_axis=1, tiled=True)
    source = jnp.sum(
        collected.reshape(site_count, block_count // group_size, 2 * comp_count, rhs_count), axis=1
    )
    link_view = stencil_links.reshape(site_count, comp_count, 9, 2, comp_count)
    link_re = link_view[:, :, :, 0, :]
    link_im = link_view[:, :, :, 1, :]
    upper_rows = jnp.stack([link_re, -link_im], axis=3)
    lower_rows = jnp.stack([link_im, link_re], axis=3)
    real_operator = jnp.stack([upper_rows, lower_rows], axis=1).reshape(
        site_count, 2 * comp_count, 18 * comp_count
    )
    mass_value = quark_mass[0]
    z_position = lax.axis_index("ta") % LZ
    line_count = site_count // LX

    def flatten_sites(shifted):
        return shifted.reshape(site_count, 2 * comp_count, rhs_count)

    solution = jnp.zeros_like(source)
    residual = source
    basis_q = []
    basis_p = []
    for iteration in range(ITERS):
        direction = residual
        rounded = residual.astype(jnp.bfloat16)
        plane_view = rounded.reshape(line_count, LX, 2 * comp_count, rhs_count)
        x_plus = flatten_sites(jnp.roll(plane_view, -1, axis=1))
        x_minus = flatten_sites(jnp.roll(plane_view, 1, axis=1))
        y_plus = flatten_sites(jnp.roll(plane_view, -1, axis=0))
        y_minus = flatten_sites(jnp.roll(plane_view, 1, axis=0))
        z_plus_near = from_behind(rounded, "ta", -1)
        z_minus_near = from_behind(rounded, "ta", 1)
        upper_pair = from_behind(jnp.stack([rounded, z_minus_near], axis=0), "ta", -LZ)
        lower_pair = from_behind(jnp.stack([rounded, z_plus_near], axis=0), "ta", LZ)
        t_plus = upper_pair[0]
        t_minus = lower_pair[0]
        z_plus = jnp.where(z_position == LZ - 1, lower_pair[1], z_plus_near)
        z_minus = jnp.where(z_position == 0, upper_pair[1], z_minus_near)
        stacked = jnp.stack(
            [rounded, x_plus, x_minus, y_plus, y_minus, z_plus, z_minus, t_plus, t_minus], axis=1
        )
        stacked = stacked.reshape(site_count, 18 * comp_count, rhs_count)
        product = jnp.einsum(
            "sij,sjr->sir", real_operator, stacked, preferred_element_type=jnp.float32
        )
        mapped = product + mass_value * rounded.astype(jnp.float32)
        square_loc = inner_local(mapped, mapped, comp_count)[0]
        cross_re, cross_im = inner_local(mapped, residual, comp_count)
        if iteration > 0:
            coef_pairs = [inner_local(earlier, mapped, comp_count) for earlier in basis_q]
            back_pairs = [inner_local(earlier, residual, comp_count) for earlier in basis_q]
            coef_re = jnp.stack([pair[0] for pair in coef_pairs])
            coef_im = jnp.stack([pair[1] for pair in coef_pairs])
            back_re = jnp.stack([pair[0] for pair in back_pairs])
            back_im = jnp.stack([pair[1] for pair in back_pairs])
        else:
            coef_re = jnp.zeros((1, rhs_count), jnp.float32)
            coef_im = jnp.zeros((1, rhs_count), jnp.float32)
            back_re = jnp.zeros((1, rhs_count), jnp.float32)
            back_im = jnp.zeros((1, rhs_count), jnp.float32)
        square_all, cross_re, cross_im, coef_re, coef_im, back_re, back_im = lax.psum(
            (square_loc, cross_re, cross_im, coef_re, coef_im, back_re, back_im), "ta"
        )
        squared = square_all
        proj_re = cross_re
        proj_im = cross_im
        for number in range(iteration):
            mapped = mapped - scaled(basis_q[number], coef_re[number], coef_im[number], comp_count)
            direction = direction - scaled(
                basis_p[number], coef_re[number], coef_im[number], comp_count
            )
            squared = squared - (
                coef_re[number] * coef_re[number] + coef_im[number] * coef_im[number]
            )
            proj_re = proj_re - (
                coef_re[number] * back_re[number] + coef_im[number] * back_im[number]
            )
            proj_im = proj_im - (
                coef_re[number] * back_im[number] - coef_im[number] * back_re[number]
            )
        factor = 1.0 / jnp.sqrt(squared + 1e-06)
        unit_q = mapped * factor
        unit_p = direction * factor
        alpha_re = proj_re * factor
        alpha_im = proj_im * factor
        solution = solution + scaled(unit_p, alpha_re, alpha_im, comp_count)
        residual = residual - scaled(unit_q, alpha_re, alpha_im, comp_count)
        basis_q.append(unit_q)
        basis_p.append(unit_p)
    return (
        solution.reshape(1, site_count, 2 * comp_count, rhs_count),
        residual.reshape(1, site_count, 2 * comp_count, rhs_count),
    )


MESH = pl.DeviceIdType.MESH


def flipped(number, mask, bits):
    total = 0
    for bit in range(bits):
        size = 1 << bit
        total = total + (((number // size) % 2 + (mask // size) % 2) % 2) * size
    return total


def swapped(value):
    return pltpu.roll(value, value.shape[-1] // 2, value.ndim - 1)


def lower_lanes(shape):
    return lax.broadcasted_iota(jnp.int32, shape, len(shape) - 1) < shape[-1] // 2


def turned(value):
    other = swapped(value)
    return jnp.where(lower_lanes(value.shape), -other, other)


def widened(rounded):
    return jnp.concatenate(
        [rounded, turned(rounded.astype(jnp.float32)).astype(jnp.bfloat16)], axis=0
    )


def times(factor, value):
    return factor[0] * value + factor[1] * turned(value)


def total_wait(region, sem):
    pltpu.make_async_copy(region, region, sem).wait()


def transposed(value, columns, comps):
    row = lax.broadcasted_iota(jnp.int32, value.shape, 0)
    chunk = lax.broadcasted_iota(jnp.int32, value.shape, 1) // comps
    width = value.shape[1]
    bits = columns.bit_length() - 1
    for bit in range(bits):
        size = 1 << bit
        moved = pltpu.roll(value, width - size * comps, 1)
        value = jnp.where((row // size) % 2 == 1, moved, value)
    for bit in range(bits):
        size = 1 << bit
        moved = pltpu.roll(value, size, 0)
        value = jnp.where((chunk // size) % 2 == 1, moved, value)
    for bit in range(bits):
        size = 1 << bit
        moved = pltpu.roll(value, width - size * comps, 1)
        value = jnp.where((row // size) % 2 == 1, moved, value)
    return value


CODE_SCALE = 2.0**12


def coded(rest):
    square = rest * rest * (CODE_SCALE * CODE_SCALE)
    fourth = square * square
    eighth = fourth * fourth
    return jnp.where(rest < 0.0, -eighth, eighth).astype(jnp.bfloat16)


def decoded(code):
    value = code.astype(jnp.float32)
    root = jnp.sqrt(jnp.sqrt(jnp.sqrt(jnp.abs(value)))) * (1.0 / CODE_SCALE)
    return jnp.where(value < 0.0, -root, root)


def solve_kernel(
    count, sites, comps,
    mass_ref, proj_hbm, fine_hbm, links_hbm,
    sol_ref, res_ref,
    proj_ref, fine_ref, links_ref, near_ref, zlinks_ref, tlinks_ref,
    weights_in, rights_ref, part_keep, part_out, part_in, hi_out, lo_out, lo_in, source_ref,
    first_round, first_z, first_t,
    wide_ref, round_ref, halo_ref, acc_ref, sol_half, res_half, basis_q, basis_p, stat_out, stat_in,
    local_sem, wsend, wrecv, psend, precv, ssend, srecv, tsend, trecv, lsend, lrecv, zsend, zrecv,
    hsend, hrecv, gsend, grecv,
):
    me = lax.axis_index("ta")
    bits = count.bit_length() - 1
    core = me % 2
    chip = me // 2
    partner = chip * 2 + 1 - core
    chips = count // 2
    far = chips // 2
    turns = [(1 - 2 * ((me // (1 << bit)) % 2)) * (1 << bit) for bit in range(bits)]
    others = [me]
    for step in range(1, count):
        top = step.bit_length() - 1
        others.append(others[step - (1 << top)] + turns[top])
    null = comps // 2
    rhs = fine_ref.shape[2]
    columns = proj_ref.shape[1]
    width = columns * comps
    groups = comps // columns

    proj_copy = pltpu.make_async_copy(proj_hbm, proj_ref, local_sem.at[2])
    proj_copy.start()
    barrier = pltpu.get_barrier_semaphore()
    for other in others[:0:-1]:
        pl.semaphore_signal(barrier, inc=1, device_id={"ta": other}, device_id_type=MESH)
    fine_copy = pltpu.make_async_copy(fine_hbm, fine_ref, local_sem.at[0])
    fine_copy.start()
    links_copy = pltpu.make_async_copy(links_hbm, links_ref, local_sem.at[1])
    links_copy.start()
    proj_copy.wait()
    pl.semaphore_wait(barrier, count - 1)

    def weights_copy(other, origin):
        return pltpu.make_async_remote_copy(
            src_ref=proj_ref.at[other], dst_ref=weights_in.at[origin],
            send_sem=wsend.at[0], recv_sem=wrecv.at[origin],
            device_id={"ta": other}, device_id_type=MESH,
        )

    quarter = me // (count // 4)
    outer = 1 - (quarter % 3 + 1) // 2
    for step in range(1, 4):
        weights_copy(others[step], me).start()
    for step in range(count // 2, count):
        crossed = step ^ (count // 4)
        weights_copy(outer * others[step] + (1 - outer) * others[crossed], me).start()
    for step in range(4, count // 2):
        weights_copy(others[step], me).start()

    fine_copy.wait()

    def build_right(plane, carry):
        fine = fine_ref[plane].astype(jnp.float32).reshape(columns, 2, 2, null, rhs)
        turned_order = [fine[(columns - at) % columns] for at in range(columns)]
        for half in range(2):
            picked = [
                block[part, half] for block in turned_order for part in range(2)
            ]
            rights_ref[plane, :, half * rhs : (half + 1) * rhs] = jnp.concatenate(
                picked, axis=0
            ).astype(jnp.bfloat16)
        return carry

    lax.fori_loop(0, count, build_right, 0)

    links_copy.wait()
    for site in range(sites):
        near_ref[site] = links_ref[site, :, : 10 * comps]
        zlinks_ref[site] = links_ref[site, :, 10 * comps : 14 * comps]
        tlinks_ref[site] = links_ref[site, :, 14 * comps : 18 * comps]

    def restricted(plane, raw_ref):
        raw = raw_ref[plane].astype(jnp.float32)
        pieces = [
            transposed(raw[:, group * width : (group + 1) * width], columns, comps)
            for group in range(groups)
        ]
        upper = jnp.concatenate(pieces, axis=0)
        lane = lax.broadcasted_iota(jnp.int32, upper.shape, 1) % comps
        lower = jnp.where(
            lane < null, -pltpu.roll(upper, width - null, 1), pltpu.roll(upper, null, 1)
        )
        left = jnp.concatenate([upper, lower], axis=0).astype(jnp.bfloat16)
        total = jnp.dot(left, rights_ref[plane], preferred_element_type=jnp.float32)
        real = jnp.concatenate([total[:null, :rhs], total[null:comps, rhs:]], axis=0)
        imag = jnp.concatenate(
            [total[comps : comps + null, :rhs], total[comps + null :, rhs:]], axis=0
        )
        low = lower_lanes(real.shape)
        return jnp.stack(
            [jnp.where(low, real, swapped(imag)), jnp.where(low, swapped(real), imag)], axis=0
        )

    def part_copy(slot):
        return pltpu.make_async_remote_copy(
            src_ref=part_out.at[slot], dst_ref=part_in.at[slot],
            send_sem=psend.at[0], recv_sem=precv.at[slot],
            device_id={"ta": partner}, device_id_type=MESH,
        )

    def source_copy(slot, origin, half):
        return pltpu.make_async_remote_copy(
            src_ref=hi_out.at[slot, half], dst_ref=first_round.at[half, origin],
            send_sem=ssend.at[0], recv_sem=srecv.at[half, origin],
            device_id={"ta": flipped(chip, slot, bits - 1) * 2 + core}, device_id_type=MESH,
        )

    def rest_copy(slot, half):
        return pltpu.make_async_remote_copy(
            src_ref=lo_out.at[slot, half], dst_ref=lo_in.at[half, chip],
            send_sem=lsend.at[0], recv_sem=lrecv.at[half],
            device_id={"ta": flipped(chip, slot, bits - 1) * 2 + core}, device_id_type=MESH,
        )

    def first_t_copy(slot, half):
        return pltpu.make_async_remote_copy(
            src_ref=hi_out.at[slot, half], dst_ref=first_t.at[half, chip],
            send_sem=tsend.at[0], recv_sem=trecv.at[half],
            device_id={"ta": (flipped(chip, slot, bits - 1) * 2 + core + count // 2) % count},
            device_id_type=MESH,
        )

    def send_high(step, half):
        source_copy(step, chip, half).start()

        @pl.when(step != far)
        def _():
            first_t_copy(step, half).start()

    def pair(step):
        other = flipped(chip, step, bits - 1)
        away = other * 2 + 1 - core
        kept = other * 2 + core
        weights_copy(partner, away).wait_recv()
        weights_copy(partner, kept).wait_recv()
        sent, held = restricted(away, weights_in), restricted(kept, weights_in)
        part_out[step] = sent
        part_keep[step] = held
        part_copy(step).start()

    def finish(step):
        part_copy(step).wait_recv()
        total = part_keep[step] + part_in[step]
        rounded = total.astype(jnp.bfloat16)
        hi_out[step] = rounded
        send_high(step, 0)

        @pl.when(step == far)
        def _():
            first_t[0, chip] = rounded[0]
            first_t[1, chip] = rounded[1]

        lo_out[step] = coded(total - rounded.astype(jnp.float32))

    base = (me // LZ) * LZ
    z_at = me % LZ
    above = base + (z_at + 1) % LZ
    below = base + (z_at + LZ - 1) % LZ
    other_time = (me + LZ) % count
    targets = (other_time, above, below)
    lines = sites // LX

    def first_z_copy(half, which, site):
        return pltpu.make_async_remote_copy(
            src_ref=first_round.at[half, site], dst_ref=first_z.at[half, which, site],
            send_sem=zsend.at[0], recv_sem=zrecv.at[half, which],
            device_id={"ta": targets[1 + which]}, device_id_type=MESH,
        )

    def forward(half, site):
        for which in range(2):
            first_z_copy(half, which, site).start()

    weights_copy(partner, partner).wait_recv()
    sent, held = restricted(partner, weights_in), restricted(me, proj_ref)
    part_out[0] = sent
    part_keep[0] = held
    part_copy(0).start()
    pair(1)
    part_copy(0).wait_recv()
    own = part_keep[0] + part_in[0]
    own_rounded = own.astype(jnp.bfloat16)
    hi_out[0] = own_rounded
    first_t_copy(0, 0).start()
    for half in range(2):
        source_ref[half, chip] = own[half]
        first_round[half, chip] = own_rounded[half]
    forward(0, chip)

    def arranged(at):
        group = at // 2
        later = outer * ((2 * group + 1) % 3 + 1) + (1 - outer) * (group % 3 + 1)
        return ((group + 2) // 3) * later * 2 + at % 2

    def pair_step(at, carry):
        pair(arranged(at))
        finish(arranged(at - 1))
        return carry

    lax.fori_loop(2, chips, pair_step, 0)
    finish(arranged(chips - 1))

    def rotated(at):
        return (at + far - 1) % (chips - 1) + 1

    def send_rest(half):
        def rest_step(at, carry):
            rest_copy(rotated(at), half).start()
            return carry

        lax.fori_loop(0, chips - 1, rest_step, 0)

    def send_second():
        def second_step(at, carry):
            send_high(rotated(at), 1)
            return carry

        first_t_copy(0, 1).start()
        forward(1, chip)
        lax.fori_loop(0, chips - 1, second_step, 0)

    def forward_all(half):
        def forward_step(at, carry):
            site = flipped(chip, arranged(at), bits - 1)
            source_copy(0, site, half).wait_recv()
            forward(half, site)
            return carry

        lax.fori_loop(1, chips, forward_step, 0)

    def complete_source(half):
        def complete_step(step, carry):
            site = flipped(chip, step, bits - 1)
            high = first_round[half, site].astype(jnp.float32)
            source_ref[half, site] = high + decoded(lo_in[half, site])
            return carry

        total_wait(lo_in.at[half, pl.ds(0, sites - 1)], lrecv.at[half])
        lax.fori_loop(1, chips, complete_step, 0)

    mass = mass_ref[0]

    def place(site, dx, dy):
        return ((site // LX + dy) % lines) * LX + (site % LX + dx) % LX

    def halo_copy(it, half, which):
        return pltpu.make_async_remote_copy(
            src_ref=round_ref.at[it - 1, half], dst_ref=halo_ref.at[it - 1, half, which],
            send_sem=hsend.at[0], recv_sem=hrecv.at[it - 1, half, which],
            device_id={"ta": targets[which]}, device_id_type=MESH,
        )

    def stat_copy(it, half, other):
        return pltpu.make_async_remote_copy(
            src_ref=stat_out.at[it, half], dst_ref=stat_in.at[it, half, me],
            send_sem=gsend.at[0], recv_sem=grecv.at[it, half],
            device_id={"ta": other}, device_id_type=MESH,
        )

    def residual_at(it, half, site):
        return source_ref[half, site] if it == 0 else res_half[half, site]

    def rounded_at(it, half, site):
        return first_round[half, site] if it == 0 else round_ref[it - 1, half, site]

    def halo_at(it, half, which, site):
        if it > 0:
            return halo_ref[it - 1, half, which, site]
        return first_t[half, site] if which == 0 else first_z[half, which - 1, site]

    def send_halo(it, half):
        for site in range(sites):
            round_ref[it - 1, half, site] = res_half[half, site].astype(jnp.bfloat16)
        @pl.when(outer == 0)
        def _():
            halo_copy(it, half, 0).start()

        for which in range(1, 3):
            halo_copy(it, half, which).start()

    def send_late_halo(it, half):
        @pl.when(outer == 1)
        def _():
            halo_copy(it, half, 0).start()

    def near_product(it, half):
        for site in range(sites):
            wide_ref[half, site] = widened(rounded_at(it, half, site))
        steps = ((0, 0), (1, 0), (-1, 0), (0, 1), (0, -1))
        for site in range(sites):
            right = jnp.concatenate(
                [wide_ref[half, place(site, dx, dy)] for dx, dy in steps], axis=0
            )
            acc_ref[half, site] = jnp.dot(
                near_ref[site], right, preferred_element_type=jnp.float32
            )

    def z_product(it, half, site):
        right = jnp.concatenate(
            [widened(halo_at(it, half, 2, site)), widened(halo_at(it, half, 1, site))], axis=0
        )
        return acc_ref[half, site] + jnp.dot(
            zlinks_ref[site], right, preferred_element_type=jnp.float32
        )

    def t_product(it, half, site):
        wide = widened(halo_at(it, half, 0, site))
        right = jnp.concatenate([wide, wide], axis=0)
        return acc_ref[half, site] + jnp.dot(
            tlinks_ref[site], right, preferred_element_type=jnp.float32
        )

    def full_product(it, half, site, product):
        return product + mass * rounded_at(it, half, site).astype(jnp.float32)

    def add_sums(it, half, site, q, sums):
        r = residual_at(it, half, site)
        q_other = swapped(q)
        sums[0] += q * q
        sums[1] += q * r
        sums[2] += q * swapped(r)
        for j in range(it):
            b = basis_q[j, half, site]
            sums[3 + 2 * j] += b * q
            sums[4 + 2 * j] += b * q_other

    def first_t_product(half):
        total_wait(first_t.at[half, pl.ds(0, sites - 1)], trecv.at[half])
        for site in range(sites):
            acc_ref[half, site] = t_product(0, half, site)

    def first_z_product(half):
        for which in range(2):
            total_wait(first_z.at[half, which], zrecv.at[half, which])
        sums = [0.0] * 3
        for site in range(sites):
            q = full_product(0, half, site, z_product(0, half, site))
            acc_ref[half, site] = q
            add_sums(0, half, site, q, sums)
        send_stats(0, half, sums)

    def far_product(it, half):
        halo_copy(it, half, 2).wait_recv()
        halo_copy(it, half, 1).wait_recv()
        for site in range(sites):
            acc_ref[half, site] = z_product(it, half, site)
        halo_copy(it, half, 0).wait_recv()
        sums = [0.0] * (3 + 2 * it)
        for site in range(sites):
            q = full_product(it, half, site, t_product(it, half, site))
            acc_ref[half, site] = q
            add_sums(it, half, site, q, sums)
        send_stats(it, half, sums)

    def send_stats(it, half, sums):
        lines_of = [jnp.sum(value, axis=0, keepdims=True) for value in sums]
        lines_of += [jnp.zeros((8 - len(lines_of), rhs), jnp.float32)]
        stats = jnp.concatenate(lines_of, axis=0)
        moved = swapped(stats)
        low = lower_lanes(stats.shape)
        reals = stats + moved
        imags = jnp.where(low, stats - moved, moved - stats)
        packed = jnp.concatenate(
            [reals[0:1]]
            + [
                jnp.where(low[0:1], reals[at : at + 1], imags[at + 1 : at + 2])
                for at in (1, 3, 5)
            ],
            axis=0,
        )
        stat_out[it, half] = packed
        for other in others[:0:-1]:
            stat_copy(it, half, other).start()
        stat_in[it, half, me] = packed

    scalars = [([], [], [], []) for _ in range(2)]

    def update(it, half):
        total_wait(stat_in.at[it, half, pl.ds(0, count - 1)], grecv.at[it, half])
        total = jnp.sum(stat_in[it, half], axis=0)
        moved = swapped(total)
        low = lower_lanes(total.shape)
        reals = jnp.where(low, total, moved)
        imags = jnp.where(low, moved, total)
        backs, epsilons, overlaps, _ = scalars[half]
        squared, cross_re, cross_im = reals[0:1], reals[1:2], imags[1:2]
        coefs = [(reals[2 + j : 3 + j], imags[2 + j : 3 + j]) for j in range(it)]
        for j, (c_re, c_im) in enumerate(coefs):
            squared = squared - (c_re * c_re + c_im * c_im) * (1.0 + epsilons[j])
            cross_re = cross_re - (c_re * backs[j][0] + c_im * backs[j][1])
            cross_im = cross_im - (c_re * backs[j][1] - c_im * backs[j][0])
        if it == 2:
            (a_re, a_im), (b_re, b_im) = coefs
            pair_re, pair_im = a_re * b_re + a_im * b_im, a_re * b_im - a_im * b_re
            squared = squared + 2.0 * (pair_re * overlaps[0][0] - pair_im * overlaps[0][1])
        factor = 1.0 / jnp.sqrt(squared + 1e-06)
        alpha = (cross_re * factor, cross_im * factor)
        epsilon = 1e-06 * factor * factor
        if it == 1:
            over = (coefs[0][0] * epsilons[0] * factor, coefs[0][1] * epsilons[0] * factor)
            overlaps.append(over)
            backs[0] = (
                backs[0][0] - (alpha[0] * over[0] - alpha[1] * over[1]),
                backs[0][1] - (alpha[0] * over[1] + alpha[1] * over[0]),
            )
        backs.append((alpha[0] * epsilon, alpha[1] * epsilon))
        epsilons.append(epsilon)
        for site in range(sites):
            residual = residual_at(it, half, site)
            q = acc_ref[half, site]
            p = residual
            for j in range(it):
                q = q - times(coefs[j], basis_q[j, half, site])
                p = p - times(coefs[j], basis_p[j, half, site])
            q = q * factor
            p = p * factor
            if it < ITERS - 1:
                basis_q[it, half, site] = q
                basis_p[it, half, site] = p
            step = times(alpha, p)
            sol_half[half, site] = step if it == 0 else sol_half[half, site] + step
            res_half[half, site] = residual - times(alpha, q)

    pl.when(outer == 0)(lambda: send_rest(0))
    forward_all(0)
    pl.when(outer == 1)(lambda: send_rest(0))
    @pl.when(outer == 0)
    def _():
        send_second()
        send_rest(1)

    near_product(0, 0)
    first_t_product(0)
    @pl.when(outer == 1)
    def _():
        send_second()
        send_rest(1)

    complete_source(0)
    forward_all(1)
    first_z_product(0)
    near_product(0, 1)
    first_t_product(1)
    complete_source(1)
    first_z_product(1)
    for it in range(ITERS):
        if it > 0:
            for half in range(2):
                far_product(it, half)
        for half in range(2):
            update(it, half)
            if it < ITERS - 1:
                send_halo(it + 1, half)
                near_product(it + 1, half)
                send_late_halo(it + 1, half)
    for from_ref, to_ref in ((sol_half, sol_ref), (res_half, res_ref)):
        for site in range(sites):
            first, second = from_ref[0, site], from_ref[1, site]
            low = lower_lanes(first.shape)
            to_ref[site, :comps] = jnp.where(low, first, swapped(second))
            to_ref[site, comps:] = jnp.where(low, swapped(first), second)

    total_wait(proj_ref.at[pl.ds(0, count - 1)], wsend.at[0])
    total_wait(part_out, psend.at[0])
    total_wait(hi_out.at[pl.ds(0, chips - 1)], ssend.at[0])
    total_wait(lo_out.at[pl.ds(0, chips - 1)], lsend.at[0])
    total_wait(hi_out.at[pl.ds(0, chips - 1)], tsend.at[0])
    total_wait(first_z, zsend.at[0])
    total_wait(halo_ref, hsend.at[0])
    total_wait(stat_in.at[:, :, pl.ds(0, count - 1)], gsend.at[0])


def shards_kernel(fine_source, projectors, stencil_links, quark_mass):
    count = lax.axis_size("ta")
    planes, local_columns, _, _, null, rhs = fine_source.shape
    sites, comps = stencil_links.shape[1], stencil_links.shape[2]
    rows = local_columns * 4 * null
    fine = fine_source.reshape(planes, rows, rhs)
    proj = projectors.reshape(count, local_columns, 4 * null * null)
    width = local_columns * comps
    links = stencil_links.reshape(sites, comps, 18 * comps)
    chips = count // 2
    vector = (sites, 2 * comps, rhs)
    f32, bf16 = jnp.float32, jnp.bfloat16
    dma = pltpu.SemaphoreType.DMA
    vmem = pl.BlockSpec(memory_space=pltpu.VMEM)
    hbm = pl.BlockSpec(memory_space=pltpu.HBM)
    parts = (chips, 2, comps, rhs)
    half = (sites, comps, rhs)
    sol, res = pl.pallas_call(
        functools.partial(solve_kernel, count, sites, comps),
        out_shape=[pltpu.VMEM(vector, f32)] * 2,
        in_specs=[pl.BlockSpec(memory_space=pltpu.SMEM), hbm, hbm, hbm],
        out_specs=[vmem, vmem],
        scratch_shapes=[
            pltpu.VMEM(proj.shape, bf16),
            pltpu.VMEM(fine.shape, bf16),
            pltpu.VMEM(links.shape, bf16),
            pltpu.VMEM((sites, comps, 10 * comps), bf16),
            pltpu.VMEM((sites, comps, 4 * comps), bf16),
            pltpu.VMEM((sites, comps, 4 * comps), bf16),
            pltpu.VMEM(proj.shape, bf16),
            pltpu.VMEM((planes, width, 2 * rhs), bf16),
            pltpu.VMEM(parts, f32),
            pltpu.VMEM(parts, f32),
            pltpu.VMEM(parts, f32),
            pltpu.VMEM(parts, bf16),
            pltpu.VMEM(parts, bf16),
            pltpu.VMEM((2, sites, comps, rhs), bf16),
            pltpu.VMEM((2, sites, comps, rhs), f32),
            pltpu.VMEM((2, sites, comps, rhs), bf16),
            pltpu.VMEM((2, 2, sites, comps, rhs), bf16),
            pltpu.VMEM((2, sites, comps, rhs), bf16),
            pltpu.VMEM((2, sites, 2 * comps, rhs), bf16),
            pltpu.VMEM((ITERS - 1, 2, *half), bf16),
            pltpu.VMEM((ITERS - 1, 2, 3, *half), bf16),
            pltpu.VMEM((2, *half), f32),
            pltpu.VMEM((2, *half), f32),
            pltpu.VMEM((2, *half), f32),
            pltpu.VMEM((ITERS - 1, 2, *half), f32),
            pltpu.VMEM((ITERS - 1, 2, *half), f32),
            pltpu.VMEM((ITERS, 2, 4, rhs), f32),
            pltpu.VMEM((ITERS, 2, count, 4, rhs), f32),
            dma((3,)),
            dma((1,)),
            dma((count,)),
            dma((1,)),
            dma((chips,)),
            dma((1,)),
            dma((2, chips)),
            dma((1,)),
            dma((2,)),
            dma((1,)),
            dma((2,)),
            dma((1,)),
            dma((2, 2)),
            dma((1,)),
            dma((ITERS - 1, 2, 3)),
            dma((1,)),
            dma((ITERS, 2)),
        ],
        compiler_params=pltpu.CompilerParams(
            collective_id=0, has_side_effects=True, vmem_limit_bytes=60 * 1024 * 1024
        ),
    )(quark_mass, proj, fine, links)
    return sol.reshape(1, *vector), res.reshape(1, *vector)


def shards(fine_source, projectors, stencil_links, quark_mass):
    count = lax.axis_size("ta")
    sites = stencil_links.shape[1]
    local_columns = fine_source.shape[1]
    block = projectors.shape[1] // sites
    fits = (
        count == 2 * LZ
        and count == 2 * sites
        and count & (count - 1) == 0
        and block == 2 * local_columns
        and stencil_links.shape[2] % local_columns == 0
        and fine_source.shape[0] == count
        and ITERS == 3
        and fine_source.shape[5] % 2 == 0
    )
    chosen = shards_kernel if fits else shards_general
    return chosen(fine_source, projectors, stencil_links, quark_mass)


def solution(mesh):
    return jax.shard_map(
        shards,
        mesh=mesh,
        in_specs=(
            P("cfg", "ta", None, None, None, None),
            P(("cfg", "ta"), None, None),
            P(("cfg", "ta"), None, None, None),
            P("cfg"),
        ),
        out_specs=(P(("cfg", "ta"), None, None, None), P(("cfg", "ta"), None, None, None)),
        check_vma=False,
    )
```

```python
import functools
import math

import jax
import jax.numpy as jnp
from jax import lax
from jax.experimental import pallas as pl
from jax.experimental.pallas import tpu as pltpu
from jax.sharding import PartitionSpec as P

LX = 4
LZ = 8
ITERS = 3


def from_behind(value, axis, steps):
    count = lax.axis_size(axis)
    pairs = [(source, (source + steps) % count) for source in range(count)]
    return lax.ppermute(value, axis, pairs)


def real_weights(proj_view):
    proj_re = proj_view[..., 0, :]
    proj_im = proj_view[..., 1, :]
    first_row = jnp.stack([proj_re, proj_im], axis=-4)
    second_row = jnp.stack([-proj_im, proj_re], axis=-4)
    return jnp.stack([first_row, second_row], axis=-5)


def inner_local(left, right, comp_count):
    left_re = left[:, :comp_count]
    left_im = left[:, comp_count:]
    right_re = right[:, :comp_count]
    right_im = right[:, comp_count:]
    return (
        jnp.sum(left_re * right_re + left_im * right_im, axis=(0, 1)),
        jnp.sum(left_re * right_im - left_im * right_re, axis=(0, 1)),
    )


def scaled(vector, factor_re, factor_im, comp_count):
    vector_re = vector[:, :comp_count]
    vector_im = vector[:, comp_count:]
    return jnp.concatenate(
        [
            factor_re * vector_re - factor_im * vector_im,
            factor_re * vector_im + factor_im * vector_re,
        ],
        axis=1,
    )


def shards_general(fine_source, projectors, stencil_links, quark_mass):
    comp_count = stencil_links.shape[2]
    null_count = comp_count // 2
    site_count = stencil_links.shape[1]
    column_count = projectors.shape[1]
    block_count = column_count // site_count
    fine_count = fine_source.shape[4]
    rhs_count = fine_source.shape[5]
    plane_count = fine_source.shape[0]
    moved_proj = lax.all_to_all(projectors, "ta", split_axis=1, concat_axis=0, tiled=True)
    local_columns = fine_source.shape[1]
    group_size = math.gcd(block_count, local_columns)
    groups = local_columns // group_size
    weights = real_weights(
        moved_proj.reshape(plane_count, groups, group_size, 2, null_count, 2, fine_count)
    )
    fine_local = fine_source.reshape(plane_count, groups, group_size, 2, 2, fine_count, rhs_count)
    partial_sums = jnp.einsum(
        "pmgdchvk,pmgchkr->pmdhvr", weights, fine_local, preferred_element_type=jnp.float32
    )
    partial_sums = partial_sums.reshape(plane_count, groups, 2 * comp_count, rhs_count)
    collected = lax.all_to_all(partial_sums, "ta", split_axis=0, concat_axis=1, tiled=True)
    source = jnp.sum(
        collected.reshape(site_count, block_count // group_size, 2 * comp_count, rhs_count), axis=1
    )
    link_view = stencil_links.reshape(site_count, comp_count, 9, 2, comp_count)
    link_re = link_view[:, :, :, 0, :]
    link_im = link_view[:, :, :, 1, :]
    upper_rows = jnp.stack([link_re, -link_im], axis=3)
    lower_rows = jnp.stack([link_im, link_re], axis=3)
    real_operator = jnp.stack([upper_rows, lower_rows], axis=1).reshape(
        site_count, 2 * comp_count, 18 * comp_count
    )
    mass_value = quark_mass[0]
    z_position = lax.axis_index("ta") % LZ
    line_count = site_count // LX

    def flatten_sites(shifted):
        return shifted.reshape(site_count, 2 * comp_count, rhs_count)

    solution = jnp.zeros_like(source)
    residual = source
    basis_q = []
    basis_p = []
    for iteration in range(ITERS):
        direction = residual
        rounded = residual.astype(jnp.bfloat16)
        plane_view = rounded.reshape(line_count, LX, 2 * comp_count, rhs_count)
        x_plus = flatten_sites(jnp.roll(plane_view, -1, axis=1))
        x_minus = flatten_sites(jnp.roll(plane_view, 1, axis=1))
        y_plus = flatten_sites(jnp.roll(plane_view, -1, axis=0))
        y_minus = flatten_sites(jnp.roll(plane_view, 1, axis=0))
        z_plus_near = from_behind(rounded, "ta", -1)
        z_minus_near = from_behind(rounded, "ta", 1)
        upper_pair = from_behind(jnp.stack([rounded, z_minus_near], axis=0), "ta", -LZ)
        lower_pair = from_behind(jnp.stack([rounded, z_plus_near], axis=0), "ta", LZ)
        t_plus = upper_pair[0]
        t_minus = lower_pair[0]
        z_plus = jnp.where(z_position == LZ - 1, lower_pair[1], z_plus_near)
        z_minus = jnp.where(z_position == 0, upper_pair[1], z_minus_near)
        stacked = jnp.stack(
            [rounded, x_plus, x_minus, y_plus, y_minus, z_plus, z_minus, t_plus, t_minus], axis=1
        )
        stacked = stacked.reshape(site_count, 18 * comp_count, rhs_count)
        product = jnp.einsum(
            "sij,sjr->sir", real_operator, stacked, preferred_element_type=jnp.float32
        )
        mapped = product + mass_value * rounded.astype(jnp.float32)
        square_loc = inner_local(mapped, mapped, comp_count)[0]
        cross_re, cross_im = inner_local(mapped, residual, comp_count)
        if iteration > 0:
            coef_pairs = [inner_local(earlier, mapped, comp_count) for earlier in basis_q]
            back_pairs = [inner_local(earlier, residual, comp_count) for earlier in basis_q]
            coef_re = jnp.stack([pair[0] for pair in coef_pairs])
            coef_im = jnp.stack([pair[1] for pair in coef_pairs])
            back_re = jnp.stack([pair[0] for pair in back_pairs])
            back_im = jnp.stack([pair[1] for pair in back_pairs])
        else:
            coef_re = jnp.zeros((1, rhs_count), jnp.float32)
            coef_im = jnp.zeros((1, rhs_count), jnp.float32)
            back_re = jnp.zeros((1, rhs_count), jnp.float32)
            back_im = jnp.zeros((1, rhs_count), jnp.float32)
        square_all, cross_re, cross_im, coef_re, coef_im, back_re, back_im = lax.psum(
            (square_loc, cross_re, cross_im, coef_re, coef_im, back_re, back_im), "ta"
        )
        squared = square_all
        proj_re = cross_re
        proj_im = cross_im
        for number in range(iteration):
            mapped = mapped - scaled(basis_q[number], coef_re[number], coef_im[number], comp_count)
            direction = direction - scaled(
                basis_p[number], coef_re[number], coef_im[number], comp_count
            )
            squared = squared - (
                coef_re[number] * coef_re[number] + coef_im[number] * coef_im[number]
            )
            proj_re = proj_re - (
                coef_re[number] * back_re[number] + coef_im[number] * back_im[number]
            )
            proj_im = proj_im - (
                coef_re[number] * back_im[number] - coef_im[number] * back_re[number]
            )
        factor = 1.0 / jnp.sqrt(squared + 1e-06)
        unit_q = mapped * factor
        unit_p = direction * factor
        alpha_re = proj_re * factor
        alpha_im = proj_im * factor
        solution = solution + scaled(unit_p, alpha_re, alpha_im, comp_count)
        residual = residual - scaled(unit_q, alpha_re, alpha_im, comp_count)
        basis_q.append(unit_q)
        basis_p.append(unit_p)
    return (
        solution.reshape(1, site_count, 2 * comp_count, rhs_count),
        residual.reshape(1, site_count, 2 * comp_count, rhs_count),
    )


MESH = pl.DeviceIdType.MESH


def flipped(number, mask, bits):
    total = 0
    for bit in range(bits):
        size = 1 << bit
        total = total + (((number // size) % 2 + (mask // size) % 2) % 2) * size
    return total


def swapped(value):
    return pltpu.roll(value, value.shape[-1] // 2, value.ndim - 1)


def lower_lanes(shape):
    return lax.broadcasted_iota(jnp.int32, shape, len(shape) - 1) < shape[-1] // 2


def turned(value):
    other = swapped(value)
    return jnp.where(lower_lanes(value.shape), -other, other)


def widened(rounded):
    return jnp.concatenate(
        [rounded, turned(rounded.astype(jnp.float32)).astype(jnp.bfloat16)], axis=0
    )


def times(factor, value):
    return factor[0] * value + factor[1] * turned(value)


def total_wait(region, sem):
    pltpu.make_async_copy(region, region, sem).wait()


def transposed(value, columns, comps):
    row = lax.broadcasted_iota(jnp.int32, value.shape, 0)
    chunk = lax.broadcasted_iota(jnp.int32, value.shape, 1) // comps
    width = value.shape[1]
    bits = columns.bit_length() - 1
    for bit in range(bits):
        size = 1 << bit
        moved = pltpu.roll(value, width - size * comps, 1)
        value = jnp.where((row // size) % 2 == 1, moved, value)
    for bit in range(bits):
        size = 1 << bit
        moved = pltpu.roll(value, size, 0)
        value = jnp.where((chunk // size) % 2 == 1, moved, value)
    for bit in range(bits):
        size = 1 << bit
        moved = pltpu.roll(value, width - size * comps, 1)
        value = jnp.where((row // size) % 2 == 1, moved, value)
    return value


CODE_SCALE = 2.0**12


def coded(rest):
    square = rest * rest * (CODE_SCALE * CODE_SCALE)
    fourth = square * square
    eighth = fourth * fourth
    return jnp.where(rest < 0.0, -eighth, eighth).astype(jnp.bfloat16)


def decoded(code):
    value = code.astype(jnp.float32)
    root = jnp.sqrt(jnp.sqrt(jnp.sqrt(jnp.abs(value)))) * (1.0 / CODE_SCALE)
    return jnp.where(value < 0.0, -root, root)


def solve_kernel(
    count, sites, comps,
    mass_ref, proj_hbm, fine_hbm, links_hbm,
    sol_ref, res_ref,
    proj_ref, fine_ref, links_ref, near_ref, zlinks_ref, tlinks_ref,
    weights_in, rights_ref, part_keep, part_out, part_in, hi_out, lo_out, lo_in, source_ref,
    first_round, first_z, first_t,
    wide_ref, round_ref, halo_ref, acc_ref, sol_half, res_half, basis_q, basis_p, stat_out, stat_in,
    local_sem, wsend, wrecv, psend, precv, ssend, srecv, tsend, trecv, lsend, lrecv, zsend, zrecv,
    hsend, hrecv, gsend, grecv,
):
    me = lax.axis_index("ta")
    bits = count.bit_length() - 1
    core = me % 2
    chip = me // 2
    partner = chip * 2 + 1 - core
    chips = count // 2
    far = chips // 2
    turns = [(1 - 2 * ((me // (1 << bit)) % 2)) * (1 << bit) for bit in range(bits)]
    others = [me]
    for step in range(1, count):
        top = step.bit_length() - 1
        others.append(others[step - (1 << top)] + turns[top])
    null = comps // 2
    rhs = fine_ref.shape[2]
    columns = proj_ref.shape[1]
    width = columns * comps
    groups = comps // columns

    proj_copy = pltpu.make_async_copy(proj_hbm, proj_ref, local_sem.at[2])
    proj_copy.start()
    barrier = pltpu.get_barrier_semaphore()
    for other in others[:0:-1]:
        pl.semaphore_signal(barrier, inc=1, device_id={"ta": other}, device_id_type=MESH)
    fine_copy = pltpu.make_async_copy(fine_hbm, fine_ref, local_sem.at[0])
    fine_copy.start()
    links_copy = pltpu.make_async_copy(links_hbm, links_ref, local_sem.at[1])
    links_copy.start()
    proj_copy.wait()
    pl.semaphore_wait(barrier, count - 1)

    def weights_copy(other, origin):
        return pltpu.make_async_remote_copy(
            src_ref=proj_ref.at[other], dst_ref=weights_in.at[origin],
            send_sem=wsend.at[0], recv_sem=wrecv.at[origin],
            device_id={"ta": other}, device_id_type=MESH,
        )

    quarter = me // (count // 4)
    outer = 1 - (quarter % 3 + 1) // 2
    for step in range(1, 4):
        weights_copy(others[step], me).start()
    for step in range(count // 2, count):
        crossed = step ^ (count // 4)
        weights_copy(outer * others[step] + (1 - outer) * others[crossed], me).start()
    for step in range(4, count // 2):
        weights_copy(others[step], me).start()

    fine_copy.wait()

    def build_right(plane, carry):
        fine = fine_ref[plane].astype(jnp.float32).reshape(columns, 2, 2, null, rhs)
        turned_order = [fine[(columns - at) % columns] for at in range(columns)]
        for half in range(2):
            picked = [
                block[part, half] for block in turned_order for part in range(2)
            ]
            rights_ref[plane, :, half * rhs : (half + 1) * rhs] = jnp.concatenate(
                picked, axis=0
            ).astype(jnp.bfloat16)
        return carry

    lax.fori_loop(0, count, build_right, 0)

    links_copy.wait()
    for site in range(sites):
        near_ref[site] = links_ref[site, :, : 10 * comps]
        zlinks_ref[site] = links_ref[site, :, 10 * comps : 14 * comps]
        tlinks_ref[site] = links_ref[site, :, 14 * comps : 18 * comps]

    def restricted(plane, raw_ref):
        raw = raw_ref[plane].astype(jnp.float32)
        pieces = [
            transposed(raw[:, group * width : (group + 1) * width], columns, comps)
            for group in range(groups)
        ]
        upper = jnp.concatenate(pieces, axis=0)
        lane = lax.broadcasted_iota(jnp.int32, upper.shape, 1) % comps
        lower = jnp.where(
            lane < null, -pltpu.roll(upper, width - null, 1), pltpu.roll(upper, null, 1)
        )
        left = jnp.concatenate([upper, lower], axis=0).astype(jnp.bfloat16)
        total = jnp.dot(left, rights_ref[plane], preferred_element_type=jnp.float32)
        real = jnp.concatenate([total[:null, :rhs], total[null:comps, rhs:]], axis=0)
        imag = jnp.concatenate(
            [total[comps : comps + null, :rhs], total[comps + null :, rhs:]], axis=0
        )
        low = lower_lanes(real.shape)
        return jnp.stack(
            [jnp.where(low, real, swapped(imag)), jnp.where(low, swapped(real), imag)], axis=0
        )

    def part_copy(slot):
        return pltpu.make_async_remote_copy(
            src_ref=part_out.at[slot], dst_ref=part_in.at[slot],
            send_sem=psend.at[0], recv_sem=precv.at[slot],
            device_id={"ta": partner}, device_id_type=MESH,
        )

    def source_copy(slot, origin):
        return pltpu.make_async_remote_copy(
            src_ref=hi_out.at[slot], dst_ref=first_round.at[origin],
            send_sem=ssend.at[0], recv_sem=srecv.at[origin],
            device_id={"ta": flipped(chip, slot, bits - 1) * 2 + core}, device_id_type=MESH,
        )

    def rest_copy(slot, half):
        return pltpu.make_async_remote_copy(
            src_ref=lo_out.at[slot, half], dst_ref=lo_in.at[half, chip],
            send_sem=lsend.at[0], recv_sem=lrecv.at[half],
            device_id={"ta": others[2 * slot]}, device_id_type=MESH,
        )

    def first_t_copy(slot, half):
        return pltpu.make_async_remote_copy(
            src_ref=hi_out.at[slot, half], dst_ref=first_t.at[half, chip],
            send_sem=tsend.at[0], recv_sem=trecv.at[half],
            device_id={"ta": others[2 * (slot ^ far)]}, device_id_type=MESH,
        )

    def pair(step):
        other = flipped(chip, step, bits - 1)
        away = other * 2 + 1 - core
        kept = other * 2 + core
        weights_copy(partner, away).wait_recv()
        weights_copy(partner, kept).wait_recv()
        sent, held = restricted(away, weights_in), restricted(kept, weights_in)
        part_out[step] = sent
        part_keep[step] = held
        part_copy(step).start()

    def finish(step):
        part_copy(step).wait_recv()
        total = part_keep[step] + part_in[step]
        rounded = total.astype(jnp.bfloat16)
        hi_out[step] = rounded
        source_copy(step, chip).start()
        lo_out[step] = coded(total - rounded.astype(jnp.float32))

    base = (me // LZ) * LZ
    z_at = me % LZ
    above = base + (z_at + 1) % LZ
    below = base + (z_at + LZ - 1) % LZ
    other_time = (me + LZ) % count
    targets = (other_time, above, below)
    lines = sites // LX

    def first_z_copy(which, site):
        return pltpu.make_async_remote_copy(
            src_ref=first_round.at[site], dst_ref=first_z.at[which, site],
            send_sem=zsend.at[0], recv_sem=zrecv.at[which],
            device_id={"ta": targets[1 + which]}, device_id_type=MESH,
        )

    def forward(site):
        for which in range(2):
            first_z_copy(which, site).start()

    weights_copy(partner, partner).wait_recv()
    sent, held = restricted(partner, weights_in), restricted(me, proj_ref)
    part_out[0] = sent
    part_keep[0] = held
    part_copy(0).start()
    pair(1)
    part_copy(0).wait_recv()
    own = part_keep[0] + part_in[0]
    own_rounded = own.astype(jnp.bfloat16)
    hi_out[0] = own_rounded
    first_round[chip] = own_rounded
    for half in range(2):
        source_ref[half, chip] = own[half]
    forward(chip)

    def arranged(at):
        group = at // 2
        later = outer * ((2 * group + 1) % 3 + 1) + (1 - outer) * (group % 3 + 1)
        return ((group + 2) // 3) * later * 2 + at % 2

    def pair_step(at, carry):
        pair(arranged(at))
        finish(arranged(at - 1))
        return carry

    lax.fori_loop(2, chips, pair_step, 0)
    finish(arranged(chips - 1))

    def send_after(half):
        first_t[half, chip] = hi_out[far, half]
        for step in range(chips - 1, -1, -1):
            if step != far:
                first_t_copy(step, half).start()

    def send_rest(half):
        for step in range(chips - 1, 0, -1):
            rest_copy(step, half).start()

    def forward_all():
        def forward_step(at, carry):
            site = flipped(chip, arranged(at), bits - 1)
            source_copy(0, site).wait_recv()
            forward(site)
            return carry

        lax.fori_loop(1, chips, forward_step, 0)

    def complete_source(half):
        def complete_step(step, carry):
            site = flipped(chip, step, bits - 1)
            high = first_round[site, half].astype(jnp.float32)
            source_ref[half, site] = high + decoded(lo_in[half, site])
            return carry

        total_wait(lo_in.at[half, pl.ds(0, sites - 1)], lrecv.at[half])
        lax.fori_loop(1, chips, complete_step, 0)

    mass = mass_ref[0]

    def place(site, dx, dy):
        return ((site // LX + dy) % lines) * LX + (site % LX + dx) % LX

    pieces = 2
    span = sites // pieces

    def z_copy(it, half, which):
        return pltpu.make_async_remote_copy(
            src_ref=round_ref.at[it - 1, half], dst_ref=halo_ref.at[it - 1, half, which],
            send_sem=hsend.at[0], recv_sem=hrecv.at[half, which - 1],
            device_id={"ta": targets[which]}, device_id_type=MESH,
        )

    def t_copy(it, half, piece):
        part = pl.ds(piece * span, span)
        return pltpu.make_async_remote_copy(
            src_ref=round_ref.at[it - 1, half, part], dst_ref=halo_ref.at[it - 1, half, 0, part],
            send_sem=hsend.at[0], recv_sem=hrecv.at[half, 2 + piece],
            device_id={"ta": other_time}, device_id_type=MESH,
        )

    def send_t(it, half):
        for piece in range(pieces):
            t_copy(it, half, piece).start()

    def stat_copy(it, half, other):
        return pltpu.make_async_remote_copy(
            src_ref=stat_out.at[it, half], dst_ref=stat_in.at[it, half, me],
            send_sem=gsend.at[0], recv_sem=grecv.at[it, half],
            device_id={"ta": other}, device_id_type=MESH,
        )

    def residual_at(it, half, site):
        return source_ref[half, site] if it == 0 else res_half[half, site]

    def rounded_at(it, half, site):
        return first_round[site, half] if it == 0 else round_ref[it - 1, half, site]

    def halo_at(it, half, which, site):
        if it > 0:
            return halo_ref[it - 1, half, which, site]
        return first_t[half, site] if which == 0 else first_z[which - 1, site, half]

    def send_halo(it, half):
        for site in range(sites):
            round_ref[it - 1, half, site] = res_half[half, site].astype(jnp.bfloat16)
        pl.when(outer == 0)(lambda: send_t(it, half))
        for which in range(1, 3):
            z_copy(it, half, which).start()

    def send_late_halo(it, half):
        pl.when(outer == 1)(lambda: send_t(it, half))

    def near_product(it, half):
        for site in range(sites):
            wide_ref[half, site] = widened(rounded_at(it, half, site))
        steps = ((0, 0), (1, 0), (-1, 0), (0, 1), (0, -1))
        for site in range(sites):
            right = jnp.concatenate(
                [wide_ref[half, place(site, dx, dy)] for dx, dy in steps], axis=0
            )
            acc_ref[half, site] = jnp.dot(
                near_ref[site], right, preferred_element_type=jnp.float32
            )

    def z_product(it, half, site):
        right = jnp.concatenate(
            [widened(halo_at(it, half, 2, site)), widened(halo_at(it, half, 1, site))], axis=0
        )
        return acc_ref[half, site] + jnp.dot(
            zlinks_ref[site], right, preferred_element_type=jnp.float32
        )

    def t_product(it, half, site):
        wide = widened(halo_at(it, half, 0, site))
        right = jnp.concatenate([wide, wide], axis=0)
        return acc_ref[half, site] + jnp.dot(
            tlinks_ref[site], right, preferred_element_type=jnp.float32
        )

    def full_product(it, half, site, product):
        return product + mass * rounded_at(it, half, site).astype(jnp.float32)

    def add_sums(it, half, site, q, sums):
        r = residual_at(it, half, site)
        q_other = swapped(q)
        sums[0] += q * q
        sums[1] += q * r
        sums[2] += q * swapped(r)
        for j in range(it):
            b = basis_q[j, half, site]
            sums[3 + 2 * j] += b * q
            sums[4 + 2 * j] += b * q_other

    def first_t_product(half):
        total_wait(first_t.at[half, pl.ds(0, sites - 1)], trecv.at[half])
        for site in range(sites):
            acc_ref[half, site] = t_product(0, half, site)

    def first_z_product(half):
        if half == 0:
            for which in range(2):
                total_wait(first_z.at[which], zrecv.at[which])
        sums = [0.0] * 3
        for site in range(sites):
            q = full_product(0, half, site, z_product(0, half, site))
            acc_ref[half, site] = q
            add_sums(0, half, site, q, sums)
        send_stats(0, half, sums)

    def far_product(it, half):
        for which in (2, 1):
            z_copy(it, half, which).wait_recv()
        for site in range(sites):
            product = z_product(it, half, site)
            acc_ref[half, site] = full_product(it, half, site, product)
        sums = [0.0] * (3 + 2 * it)
        for site in range(sites):
            if site % span == 0:
                t_copy(it, half, site // span).wait_recv()
            q = t_product(it, half, site)
            acc_ref[half, site] = q
            add_sums(it, half, site, q, sums)
        send_stats(it, half, sums)

    def send_stats(it, half, sums):
        lines_of = [jnp.sum(value, axis=0, keepdims=True) for value in sums]
        lines_of += [jnp.zeros((8 - len(lines_of), rhs), jnp.float32)]
        stats = jnp.concatenate(lines_of, axis=0)
        moved = swapped(stats)
        low = lower_lanes(stats.shape)
        reals = stats + moved
        imags = jnp.where(low, stats - moved, moved - stats)
        packed = jnp.concatenate(
            [reals[0:1]]
            + [
                jnp.where(low[0:1], reals[at : at + 1], imags[at + 1 : at + 2])
                for at in (1, 3, 5)
            ],
            axis=0,
        )
        stat_out[it, half] = packed
        for other in others[:0:-1]:
            stat_copy(it, half, other).start()
        stat_in[it, half, me] = packed

    scalars = [([], [], [], []) for _ in range(2)]

    def update(it, half):
        total_wait(stat_in.at[it, half, pl.ds(0, count - 1)], grecv.at[it, half])
        total = jnp.sum(stat_in[it, half], axis=0)
        moved = swapped(total)
        low = lower_lanes(total.shape)
        reals = jnp.where(low, total, moved)
        imags = jnp.where(low, moved, total)
        backs, epsilons, overlaps, _ = scalars[half]
        squared, cross_re, cross_im = reals[0:1], reals[1:2], imags[1:2]
        coefs = [(reals[2 + j : 3 + j], imags[2 + j : 3 + j]) for j in range(it)]
        for j, (c_re, c_im) in enumerate(coefs):
            squared = squared - (c_re * c_re + c_im * c_im) * (1.0 + epsilons[j])
            cross_re = cross_re - (c_re * backs[j][0] + c_im * backs[j][1])
            cross_im = cross_im - (c_re * backs[j][1] - c_im * backs[j][0])
        if it == 2:
            (a_re, a_im), (b_re, b_im) = coefs
            pair_re, pair_im = a_re * b_re + a_im * b_im, a_re * b_im - a_im * b_re
            squared = squared + 2.0 * (pair_re * overlaps[0][0] - pair_im * overlaps[0][1])
        factor = 1.0 / jnp.sqrt(squared + 1e-06)
        alpha = (cross_re * factor, cross_im * factor)
        epsilon = 1e-06 * factor * factor
        if it == 1:
            over = (coefs[0][0] * epsilons[0] * factor, coefs[0][1] * epsilons[0] * factor)
            overlaps.append(over)
            backs[0] = (
                backs[0][0] - (alpha[0] * over[0] - alpha[1] * over[1]),
                backs[0][1] - (alpha[0] * over[1] + alpha[1] * over[0]),
            )
        backs.append((alpha[0] * epsilon, alpha[1] * epsilon))
        epsilons.append(epsilon)
        for site in range(sites):
            residual = residual_at(it, half, site)
            q = acc_ref[half, site]
            p = residual
            for j in range(it):
                q = q - times(coefs[j], basis_q[j, half, site])
                p = p - times(coefs[j], basis_p[j, half, site])
            q = q * factor
            p = p * factor
            if it < ITERS - 1:
                basis_q[it, half, site] = q
                basis_p[it, half, site] = p
            step = times(alpha, p)
            new_sol = step if it == 0 else sol_half[half, site] + step
            new_res = residual - times(alpha, q)
            if it < ITERS - 1 or half == 0:
                sol_half[half, site] = new_sol
                res_half[half, site] = new_res
            else:
                unpack(sol_ref, site, sol_half[0, site], new_sol)
                unpack(res_ref, site, res_half[0, site], new_res)

    def unpack(to_ref, site, first, second):
        low = lower_lanes(first.shape)
        to_ref[site, :comps] = jnp.where(low, first, swapped(second))
        to_ref[site, comps:] = jnp.where(low, swapped(first), second)

    send_after(0)
    pl.when(outer == 0)(lambda: send_rest(0))
    forward_all()
    pl.when(outer == 1)(lambda: send_rest(0))
    near_product(0, 0)
    near_product(0, 1)
    first_t_product(0)
    send_after(1)
    send_rest(1)
    complete_source(0)
    first_z_product(0)
    first_t_product(1)
    complete_source(1)
    first_z_product(1)
    for it in range(ITERS):
        if it > 0:
            for half in range(2):
                far_product(it, half)
        for half in range(2):
            update(it, half)
            if it < ITERS - 1:
                send_halo(it + 1, half)
                near_product(it + 1, half)
                send_late_halo(it + 1, half)
    total_wait(proj_ref.at[pl.ds(0, count - 1)], wsend.at[0])
    total_wait(part_out, psend.at[0])
    total_wait(hi_out.at[pl.ds(0, chips - 1)], ssend.at[0])
    total_wait(lo_out.at[pl.ds(0, chips - 1)], lsend.at[0])
    total_wait(hi_out.at[pl.ds(0, chips - 1)], tsend.at[0])
    total_wait(first_z, zsend.at[0])
    total_wait(halo_ref, hsend.at[0])
    total_wait(stat_in.at[:, :, pl.ds(0, count - 1)], gsend.at[0])


def store_kernel(sol_ref, res_ref, sol_hbm, res_hbm, sems):
    copies = [
        pltpu.make_async_copy(from_ref, to_ref, sems.at[at])
        for at, (from_ref, to_ref) in enumerate(((sol_ref, sol_hbm), (res_ref, res_hbm)))
    ]
    for copy in copies:
        copy.start()
    for copy in copies:
        copy.wait()


def stored(sol, res):
    vmem = pl.BlockSpec(memory_space=pltpu.VMEM)
    hbm = pl.BlockSpec(memory_space=pltpu.HBM)
    return pl.pallas_call(
        store_kernel,
        out_shape=[jax.ShapeDtypeStruct(value.shape, value.dtype) for value in (sol, res)],
        in_specs=[vmem, vmem],
        out_specs=[hbm, hbm],
        scratch_shapes=[pltpu.SemaphoreType.DMA((2,))],
        compiler_params=pltpu.CompilerParams(vmem_limit_bytes=1024 * 1024),
    )(sol, res)


def shards_kernel(fine_source, projectors, stencil_links, quark_mass):
    count = lax.axis_size("ta")
    planes, local_columns, _, _, null, rhs = fine_source.shape
    sites, comps = stencil_links.shape[1], stencil_links.shape[2]
    rows = local_columns * 4 * null
    fine = fine_source.reshape(planes, rows, rhs)
    proj = projectors.reshape(count, local_columns, 4 * null * null)
    width = local_columns * comps
    links = stencil_links.reshape(sites, comps, 18 * comps)
    chips = count // 2
    vector = (sites, 2 * comps, rhs)
    f32, bf16 = jnp.float32, jnp.bfloat16
    dma = pltpu.SemaphoreType.DMA
    vmem = pl.BlockSpec(memory_space=pltpu.VMEM)
    hbm = pl.BlockSpec(memory_space=pltpu.HBM)
    parts = (chips, 2, comps, rhs)
    half = (sites, comps, rhs)
    sol, res = pl.pallas_call(
        functools.partial(solve_kernel, count, sites, comps),
        out_shape=[pltpu.VMEM(vector, f32)] * 2,
        in_specs=[pl.BlockSpec(memory_space=pltpu.SMEM), hbm, hbm, hbm],
        out_specs=[vmem, vmem],
        scratch_shapes=[
            pltpu.VMEM(proj.shape, bf16),
            pltpu.VMEM(fine.shape, bf16),
            pltpu.VMEM(links.shape, bf16),
            pltpu.VMEM((sites, comps, 10 * comps), bf16),
            pltpu.VMEM((sites, comps, 4 * comps), bf16),
            pltpu.VMEM((sites, comps, 4 * comps), bf16),
            pltpu.VMEM(proj.shape, bf16),
            pltpu.VMEM((planes, width, 2 * rhs), bf16),
            pltpu.VMEM(parts, f32),
            pltpu.VMEM(parts, f32),
            pltpu.VMEM(parts, f32),
            pltpu.VMEM(parts, bf16),
            pltpu.VMEM(parts, bf16),
            pltpu.VMEM((2, sites, comps, rhs), bf16),
            pltpu.VMEM((2, sites, comps, rhs), f32),
            pltpu.VMEM((sites, 2, comps, rhs), bf16),
            pltpu.VMEM((2, sites, 2, comps, rhs), bf16),
            pltpu.VMEM((2, sites, comps, rhs), bf16),
            pltpu.VMEM((2, sites, 2 * comps, rhs), bf16),
            pltpu.VMEM((ITERS - 1, 2, *half), bf16),
            pltpu.VMEM((ITERS - 1, 2, 3, *half), bf16),
            pltpu.VMEM((2, *half), f32),
            pltpu.VMEM((2, *half), f32),
            pltpu.VMEM((2, *half), f32),
            pltpu.VMEM((ITERS - 1, 2, *half), f32),
            pltpu.VMEM((ITERS - 1, 2, *half), f32),
            pltpu.VMEM((ITERS, 2, 4, rhs), f32),
            pltpu.VMEM((ITERS, 2, count, 4, rhs), f32),
            dma((3,)),
            dma((1,)),
            dma((count,)),
            dma((1,)),
            dma((chips,)),
            dma((1,)),
            dma((chips,)),
            dma((1,)),
            dma((2,)),
            dma((1,)),
            dma((2,)),
            dma((1,)),
            dma((2,)),
            dma((1,)),
            dma((2, 4)),
            dma((1,)),
            dma((ITERS, 2)),
        ],
        compiler_params=pltpu.CompilerParams(
            collective_id=0, has_side_effects=True, vmem_limit_bytes=60 * 1024 * 1024
        ),
    )(quark_mass, proj, fine, links)
    sol, res = stored(sol, res)
    return sol.reshape(1, *vector), res.reshape(1, *vector)


def shards(fine_source, projectors, stencil_links, quark_mass):
    count = lax.axis_size("ta")
    sites = stencil_links.shape[1]
    local_columns = fine_source.shape[1]
    block = projectors.shape[1] // sites
    fits = (
        count == 2 * LZ
        and count == 2 * sites
        and count & (count - 1) == 0
        and block == 2 * local_columns
        and stencil_links.shape[2] % local_columns == 0
        and fine_source.shape[0] == count
        and ITERS == 3
        and fine_source.shape[5] % 2 == 0
    )
    chosen = shards_kernel if fits else shards_general
    return chosen(fine_source, projectors, stencil_links, quark_mass)


def solution(mesh):
    return jax.shard_map(
        shards,
        mesh=mesh,
        in_specs=(
            P("cfg", "ta", None, None, None, None),
            P(("cfg", "ta"), None, None),
            P(("cfg", "ta"), None, None, None),
            P("cfg"),
        ),
        out_specs=(P(("cfg", "ta"), None, None, None), P(("cfg", "ta"), None, None, None)),
        check_vma=False,
    )
```

```python
import functools
import math

import jax
import jax.numpy as jnp
from jax import lax
from jax.experimental import pallas as pl
from jax.experimental.pallas import tpu as pltpu
from jax.sharding import PartitionSpec as P

LX = 4
LZ = 8
ITERS = 3


def from_behind(value, axis, steps):
    count = lax.axis_size(axis)
    pairs = [(source, (source + steps) % count) for source in range(count)]
    return lax.ppermute(value, axis, pairs)


def real_weights(proj_view):
    proj_re = proj_view[..., 0, :]
    proj_im = proj_view[..., 1, :]
    first_row = jnp.stack([proj_re, proj_im], axis=-4)
    second_row = jnp.stack([-proj_im, proj_re], axis=-4)
    return jnp.stack([first_row, second_row], axis=-5)


def inner_local(left, right, comp_count):
    left_re = left[:, :comp_count]
    left_im = left[:, comp_count:]
    right_re = right[:, :comp_count]
    right_im = right[:, comp_count:]
    return (
        jnp.sum(left_re * right_re + left_im * right_im, axis=(0, 1)),
        jnp.sum(left_re * right_im - left_im * right_re, axis=(0, 1)),
    )


def scaled(vector, factor_re, factor_im, comp_count):
    vector_re = vector[:, :comp_count]
    vector_im = vector[:, comp_count:]
    return jnp.concatenate(
        [
            factor_re * vector_re - factor_im * vector_im,
            factor_re * vector_im + factor_im * vector_re,
        ],
        axis=1,
    )


def shards_general(fine_source, projectors, stencil_links, quark_mass):
    comp_count = stencil_links.shape[2]
    null_count = comp_count // 2
    site_count = stencil_links.shape[1]
    column_count = projectors.shape[1]
    block_count = column_count // site_count
    fine_count = fine_source.shape[4]
    rhs_count = fine_source.shape[5]
    plane_count = fine_source.shape[0]
    moved_proj = lax.all_to_all(projectors, "ta", split_axis=1, concat_axis=0, tiled=True)
    local_columns = fine_source.shape[1]
    group_size = math.gcd(block_count, local_columns)
    groups = local_columns // group_size
    weights = real_weights(
        moved_proj.reshape(plane_count, groups, group_size, 2, null_count, 2, fine_count)
    )
    fine_local = fine_source.reshape(plane_count, groups, group_size, 2, 2, fine_count, rhs_count)
    partial_sums = jnp.einsum(
        "pmgdchvk,pmgchkr->pmdhvr", weights, fine_local, preferred_element_type=jnp.float32
    )
    partial_sums = partial_sums.reshape(plane_count, groups, 2 * comp_count, rhs_count)
    collected = lax.all_to_all(partial_sums, "ta", split_axis=0, concat_axis=1, tiled=True)
    source = jnp.sum(
        collected.reshape(site_count, block_count // group_size, 2 * comp_count, rhs_count), axis=1
    )
    link_view = stencil_links.reshape(site_count, comp_count, 9, 2, comp_count)
    link_re = link_view[:, :, :, 0, :]
    link_im = link_view[:, :, :, 1, :]
    upper_rows = jnp.stack([link_re, -link_im], axis=3)
    lower_rows = jnp.stack([link_im, link_re], axis=3)
    real_operator = jnp.stack([upper_rows, lower_rows], axis=1).reshape(
        site_count, 2 * comp_count, 18 * comp_count
    )
    mass_value = quark_mass[0]
    z_position = lax.axis_index("ta") % LZ
    line_count = site_count // LX

    def flatten_sites(shifted):
        return shifted.reshape(site_count, 2 * comp_count, rhs_count)

    solution = jnp.zeros_like(source)
    residual = source
    basis_q = []
    basis_p = []
    for iteration in range(ITERS):
        direction = residual
        rounded = residual.astype(jnp.bfloat16)
        plane_view = rounded.reshape(line_count, LX, 2 * comp_count, rhs_count)
        x_plus = flatten_sites(jnp.roll(plane_view, -1, axis=1))
        x_minus = flatten_sites(jnp.roll(plane_view, 1, axis=1))
        y_plus = flatten_sites(jnp.roll(plane_view, -1, axis=0))
        y_minus = flatten_sites(jnp.roll(plane_view, 1, axis=0))
        z_plus_near = from_behind(rounded, "ta", -1)
        z_minus_near = from_behind(rounded, "ta", 1)
        upper_pair = from_behind(jnp.stack([rounded, z_minus_near], axis=0), "ta", -LZ)
        lower_pair = from_behind(jnp.stack([rounded, z_plus_near], axis=0), "ta", LZ)
        t_plus = upper_pair[0]
        t_minus = lower_pair[0]
        z_plus = jnp.where(z_position == LZ - 1, lower_pair[1], z_plus_near)
        z_minus = jnp.where(z_position == 0, upper_pair[1], z_minus_near)
        stacked = jnp.stack(
            [rounded, x_plus, x_minus, y_plus, y_minus, z_plus, z_minus, t_plus, t_minus], axis=1
        )
        stacked = stacked.reshape(site_count, 18 * comp_count, rhs_count)
        product = jnp.einsum(
            "sij,sjr->sir", real_operator, stacked, preferred_element_type=jnp.float32
        )
        mapped = product + mass_value * rounded.astype(jnp.float32)
        square_loc = inner_local(mapped, mapped, comp_count)[0]
        cross_re, cross_im = inner_local(mapped, residual, comp_count)
        if iteration > 0:
            coef_pairs = [inner_local(earlier, mapped, comp_count) for earlier in basis_q]
            back_pairs = [inner_local(earlier, residual, comp_count) for earlier in basis_q]
            coef_re = jnp.stack([pair[0] for pair in coef_pairs])
            coef_im = jnp.stack([pair[1] for pair in coef_pairs])
            back_re = jnp.stack([pair[0] for pair in back_pairs])
            back_im = jnp.stack([pair[1] for pair in back_pairs])
        else:
            coef_re = jnp.zeros((1, rhs_count), jnp.float32)
            coef_im = jnp.zeros((1, rhs_count), jnp.float32)
            back_re = jnp.zeros((1, rhs_count), jnp.float32)
            back_im = jnp.zeros((1, rhs_count), jnp.float32)
        square_all, cross_re, cross_im, coef_re, coef_im, back_re, back_im = lax.psum(
            (square_loc, cross_re, cross_im, coef_re, coef_im, back_re, back_im), "ta"
        )
        squared = square_all
        proj_re = cross_re
        proj_im = cross_im
        for number in range(iteration):
            mapped = mapped - scaled(basis_q[number], coef_re[number], coef_im[number], comp_count)
            direction = direction - scaled(
                basis_p[number], coef_re[number], coef_im[number], comp_count
            )
            squared = squared - (
                coef_re[number] * coef_re[number] + coef_im[number] * coef_im[number]
            )
            proj_re = proj_re - (
                coef_re[number] * back_re[number] + coef_im[number] * back_im[number]
            )
            proj_im = proj_im - (
                coef_re[number] * back_im[number] - coef_im[number] * back_re[number]
            )
        factor = 1.0 / jnp.sqrt(squared + 1e-06)
        unit_q = mapped * factor
        unit_p = direction * factor
        alpha_re = proj_re * factor
        alpha_im = proj_im * factor
        solution = solution + scaled(unit_p, alpha_re, alpha_im, comp_count)
        residual = residual - scaled(unit_q, alpha_re, alpha_im, comp_count)
        basis_q.append(unit_q)
        basis_p.append(unit_p)
    return (
        solution.reshape(1, site_count, 2 * comp_count, rhs_count),
        residual.reshape(1, site_count, 2 * comp_count, rhs_count),
    )


MESH = pl.DeviceIdType.MESH


def flipped(number, mask, bits):
    total = 0
    for bit in range(bits):
        size = 1 << bit
        total = total + (((number // size) % 2 + (mask // size) % 2) % 2) * size
    return total


def swapped(value):
    return pltpu.roll(value, value.shape[-1] // 2, value.ndim - 1)


def lower_lanes(shape):
    return lax.broadcasted_iota(jnp.int32, shape, len(shape) - 1) < shape[-1] // 2


def turned(value):
    other = swapped(value)
    return jnp.where(lower_lanes(value.shape), -other, other)


def widened(rounded):
    return jnp.concatenate(
        [rounded, turned(rounded.astype(jnp.float32)).astype(jnp.bfloat16)], axis=0
    )


def times(factor, value):
    return factor[0] * value + factor[1] * turned(value)


def total_wait(region, sem):
    pltpu.make_async_copy(region, region, sem).wait()


def transposed(value, columns, comps):
    row = lax.broadcasted_iota(jnp.int32, value.shape, 0)
    chunk = lax.broadcasted_iota(jnp.int32, value.shape, 1) // comps
    width = value.shape[1]
    bits = columns.bit_length() - 1
    for bit in range(bits):
        size = 1 << bit
        moved = pltpu.roll(value, width - size * comps, 1)
        value = jnp.where((row // size) % 2 == 1, moved, value)
    for bit in range(bits):
        size = 1 << bit
        moved = pltpu.roll(value, size, 0)
        value = jnp.where((chunk // size) % 2 == 1, moved, value)
    for bit in range(bits):
        size = 1 << bit
        moved = pltpu.roll(value, width - size * comps, 1)
        value = jnp.where((row // size) % 2 == 1, moved, value)
    return value


CODE_SCALE = 2.0**12


def coded(rest):
    square = rest * rest * (CODE_SCALE * CODE_SCALE)
    fourth = square * square
    eighth = fourth * fourth
    return jnp.where(rest < 0.0, -eighth, eighth).astype(jnp.bfloat16)


def decoded(code):
    value = code.astype(jnp.float32)
    root = jnp.sqrt(jnp.sqrt(jnp.sqrt(jnp.abs(value)))) * (1.0 / CODE_SCALE)
    return jnp.where(value < 0.0, -root, root)


def solve_kernel(
    count, sites, comps,
    mass_ref, proj_hbm, fine_hbm, links_hbm,
    sol_ref, res_ref,
    proj_ref, fine_ref, links_ref, near_ref, zlinks_ref, tlinks_ref,
    weights_in, rights_ref, part_keep, part_out, part_in, hi_out, lo_out, lo_in, source_ref,
    first_round, first_z, first_t,
    wide_ref, round_ref, halo_ref, acc_ref, acc_turned, sol_half, res_half, res_turned,
    basis_q, basis_p, turned_q, turned_p, stat_out, stat_in,
    local_sem, wsend, wrecv, psend, precv, ssend, srecv, tsend, trecv, lsend, lrecv, zsend, zrecv,
    hsend, hrecv, gsend, grecv,
):
    me = lax.axis_index("ta")
    bits = count.bit_length() - 1
    core = me % 2
    chip = me // 2
    partner = chip * 2 + 1 - core
    chips = count // 2
    far = chips // 2
    turns = [(1 - 2 * ((me // (1 << bit)) % 2)) * (1 << bit) for bit in range(bits)]
    others = [me]
    for step in range(1, count):
        top = step.bit_length() - 1
        others.append(others[step - (1 << top)] + turns[top])
    null = comps // 2
    rhs = fine_ref.shape[2]
    columns = proj_ref.shape[1]
    width = columns * comps
    groups = comps // columns

    proj_copy = pltpu.make_async_copy(proj_hbm, proj_ref, local_sem.at[2])
    proj_copy.start()
    barrier = pltpu.get_barrier_semaphore()
    for other in others[:0:-1]:
        pl.semaphore_signal(barrier, inc=1, device_id={"ta": other}, device_id_type=MESH)
    fine_copy = pltpu.make_async_copy(fine_hbm, fine_ref, local_sem.at[0])
    fine_copy.start()
    links_copy = pltpu.make_async_copy(links_hbm, links_ref, local_sem.at[1])
    links_copy.start()
    proj_copy.wait()
    pl.semaphore_wait(barrier, count - 1)

    def weights_copy(other, origin):
        return pltpu.make_async_remote_copy(
            src_ref=proj_ref.at[other], dst_ref=weights_in.at[origin],
            send_sem=wsend.at[0], recv_sem=wrecv.at[origin],
            device_id={"ta": other}, device_id_type=MESH,
        )

    quarter = me // (count // 4)
    outer = 1 - (quarter % 3 + 1) // 2
    for step in range(1, 4):
        weights_copy(others[step], me).start()
    for step in range(count // 2, count):
        crossed = step ^ (count // 4)
        weights_copy(outer * others[step] + (1 - outer) * others[crossed], me).start()
    for step in range(4, count // 2):
        weights_copy(others[step], me).start()

    fine_copy.wait()

    def build_right(plane, carry):
        fine = fine_ref[plane].astype(jnp.float32).reshape(columns, 2, 2, null, rhs)
        turned_order = [fine[(columns - at) % columns] for at in range(columns)]
        for half in range(2):
            picked = [
                block[part, half] for block in turned_order for part in range(2)
            ]
            rights_ref[plane, :, half * rhs : (half + 1) * rhs] = jnp.concatenate(
                picked, axis=0
            ).astype(jnp.bfloat16)
        return carry

    lax.fori_loop(0, count, build_right, 0)

    links_copy.wait()
    for site in range(sites):
        near_ref[site] = links_ref[site, :, : 10 * comps]
        zlinks_ref[site] = links_ref[site, :, 10 * comps : 14 * comps]
        tlinks_ref[site] = links_ref[site, :, 14 * comps : 18 * comps]

    def restricted(plane, raw_ref):
        raw = raw_ref[plane].astype(jnp.float32)
        pieces = [
            transposed(raw[:, group * width : (group + 1) * width], columns, comps)
            for group in range(groups)
        ]
        upper = jnp.concatenate(pieces, axis=0)
        lane = lax.broadcasted_iota(jnp.int32, upper.shape, 1) % comps
        lower = jnp.where(
            lane < null, -pltpu.roll(upper, width - null, 1), pltpu.roll(upper, null, 1)
        )
        left = jnp.concatenate([upper, lower], axis=0).astype(jnp.bfloat16)
        total = jnp.dot(left, rights_ref[plane], preferred_element_type=jnp.float32)
        real = jnp.concatenate([total[:null, :rhs], total[null:comps, rhs:]], axis=0)
        imag = jnp.concatenate(
            [total[comps : comps + null, :rhs], total[comps + null :, rhs:]], axis=0
        )
        low = lower_lanes(real.shape)
        return jnp.stack(
            [jnp.where(low, real, swapped(imag)), jnp.where(low, swapped(real), imag)], axis=0
        )

    def part_copy(slot):
        return pltpu.make_async_remote_copy(
            src_ref=part_out.at[slot], dst_ref=part_in.at[slot],
            send_sem=psend.at[0], recv_sem=precv.at[slot],
            device_id={"ta": partner}, device_id_type=MESH,
        )

    def source_copy(slot, origin):
        return pltpu.make_async_remote_copy(
            src_ref=hi_out.at[slot], dst_ref=first_round.at[origin],
            send_sem=ssend.at[0], recv_sem=srecv.at[origin],
            device_id={"ta": flipped(chip, slot, bits - 1) * 2 + core}, device_id_type=MESH,
        )

    def rest_copy(slot, half):
        return pltpu.make_async_remote_copy(
            src_ref=lo_out.at[slot, half], dst_ref=lo_in.at[half, chip],
            send_sem=lsend.at[0], recv_sem=lrecv.at[half],
            device_id={"ta": others[2 * slot]}, device_id_type=MESH,
        )

    def first_t_copy(slot, half):
        return pltpu.make_async_remote_copy(
            src_ref=hi_out.at[slot, half], dst_ref=first_t.at[half, chip],
            send_sem=tsend.at[0], recv_sem=trecv.at[half],
            device_id={"ta": others[2 * (slot ^ far)]}, device_id_type=MESH,
        )

    def pair(step):
        other = flipped(chip, step, bits - 1)
        away = other * 2 + 1 - core
        kept = other * 2 + core
        weights_copy(partner, away).wait_recv()
        weights_copy(partner, kept).wait_recv()
        sent, held = restricted(away, weights_in), restricted(kept, weights_in)
        part_out[step] = sent
        part_keep[step] = held
        part_copy(step).start()

    def finish(step):
        part_copy(step).wait_recv()
        total = part_keep[step] + part_in[step]
        rounded = total.astype(jnp.bfloat16)
        hi_out[step] = rounded
        source_copy(step, chip).start()
        lo_out[step] = coded(total - rounded.astype(jnp.float32))

    base = (me // LZ) * LZ
    z_at = me % LZ
    above = base + (z_at + 1) % LZ
    below = base + (z_at + LZ - 1) % LZ
    other_time = (me + LZ) % count
    targets = (other_time, above, below)
    lines = sites // LX

    def first_z_copy(half, which, site):
        return pltpu.make_async_remote_copy(
            src_ref=first_round.at[site, half], dst_ref=first_z.at[half, which, site],
            send_sem=zsend.at[0], recv_sem=zrecv.at[half, which],
            device_id={"ta": targets[1 + which]}, device_id_type=MESH,
        )

    def forward(half, site):
        for which in range(2):
            first_z_copy(half, which, site).start()

    weights_copy(partner, partner).wait_recv()
    sent, held = restricted(partner, weights_in), restricted(me, proj_ref)
    part_out[0] = sent
    part_keep[0] = held
    part_copy(0).start()
    pair(1)
    part_copy(0).wait_recv()
    own = part_keep[0] + part_in[0]
    own_rounded = own.astype(jnp.bfloat16)
    hi_out[0] = own_rounded
    first_round[chip] = own_rounded
    own_rest = coded(own - own_rounded.astype(jnp.float32))
    for half in range(2):
        lo_in[half, chip] = own_rest[half]
    forward(0, chip)

    def arranged(at):
        group = at // 2
        later = outer * ((2 * group + 1) % 3 + 1) + (1 - outer) * (group % 3 + 1)
        return ((group + 2) // 3) * later * 2 + at % 2

    def pair_step(at, carry):
        pair(arranged(at))
        finish(arranged(at - 1))
        return carry

    lax.fori_loop(2, chips, pair_step, 0)
    finish(arranged(chips - 1))

    def send_after(half):
        first_t[half, chip] = hi_out[far, half]
        for step in range(chips - 1, -1, -1):
            if step != far:
                first_t_copy(step, half).start()

    def send_rest(half):
        for step in range(chips - 1, 0, -1):
            rest_copy(step, half).start()

    def forward_all():
        def forward_step(at, carry):
            site = flipped(chip, arranged(at), bits - 1)
            source_copy(0, site).wait_recv()
            forward(0, site)
            return carry

        lax.fori_loop(1, chips, forward_step, 0)

    mass = mass_ref[0]

    def place(site, dx, dy):
        return ((site // LX + dy) % lines) * LX + (site % LX + dx) % LX

    pieces = 4
    span = sites // pieces

    def z_copy(it, half, which):
        return pltpu.make_async_remote_copy(
            src_ref=round_ref.at[it - 1, half], dst_ref=halo_ref.at[it - 1, half, which],
            send_sem=hsend.at[0], recv_sem=hrecv.at[half, which - 1],
            device_id={"ta": targets[which]}, device_id_type=MESH,
        )

    def t_copy(it, half, piece):
        part = pl.ds(piece * span, span)
        return pltpu.make_async_remote_copy(
            src_ref=round_ref.at[it - 1, half, part], dst_ref=halo_ref.at[it - 1, half, 0, part],
            send_sem=hsend.at[0], recv_sem=hrecv.at[half, 2 + piece],
            device_id={"ta": other_time}, device_id_type=MESH,
        )

    def send_t(it, half):
        for piece in range(pieces):
            t_copy(it, half, piece).start()

    def stat_copy(it, half, other):
        return pltpu.make_async_remote_copy(
            src_ref=stat_out.at[it, half], dst_ref=stat_in.at[it, half, me],
            send_sem=gsend.at[0], recv_sem=grecv.at[it, half],
            device_id={"ta": other}, device_id_type=MESH,
        )

    def residual_at(it, half, site):
        return source_ref[half, site] if it == 0 else res_half[it - 1, half, site]

    def rounded_at(it, half, site):
        return first_round[site, half] if it == 0 else round_ref[it - 1, half, site]

    def halo_at(it, half, which, site):
        if it > 0:
            return halo_ref[it - 1, half, which, site]
        return first_t[half, site] if which == 0 else first_z[half, which - 1, site]

    def send_late_halo(it, half):
        pl.when(outer == 1)(lambda: send_t(it, half))

    def near_product(it, half):
        for site in range(sites):
            wide_ref[half, site] = widened(rounded_at(it, half, site))
        steps = ((0, 0), (1, 0), (-1, 0), (0, 1), (0, -1))
        for site in range(sites):
            right = jnp.concatenate(
                [wide_ref[half, place(site, dx, dy)] for dx, dy in steps], axis=0
            )
            acc_ref[it % 2, half, site] = jnp.dot(
                near_ref[site], right, preferred_element_type=jnp.float32
            )

    def z_product(it, half, site):
        right = jnp.concatenate(
            [widened(halo_at(it, half, 2, site)), widened(halo_at(it, half, 1, site))], axis=0
        )
        return acc_ref[it % 2, half, site] + jnp.dot(
            zlinks_ref[site], right, preferred_element_type=jnp.float32
        )

    def t_product(it, half, site):
        wide = widened(halo_at(it, half, 0, site))
        right = jnp.concatenate([wide, wide], axis=0)
        return acc_ref[it % 2, half, site] + jnp.dot(
            tlinks_ref[site], right, preferred_element_type=jnp.float32
        )

    def full_product(it, half, site, product):
        return product + mass * rounded_at(it, half, site).astype(jnp.float32)

    def add_sums(it, half, site, q, sums):
        sums[0] += q * q
        sums[1] += q * residual_at(it, half, site)
        sums[2] += q * res_turned[half, site]
        for j in range(it):
            sums[3 + 2 * j] += basis_q[j, half, site] * q
            sums[4 + 2 * j] += turned_q[j, half, site] * q

    def first_t_product(half):
        total_wait(first_t.at[half, pl.ds(0, sites - 1)], trecv.at[half])
        for site in range(sites):
            acc_ref[0, half, site] = t_product(0, half, site)

    def first_z_product(half):
        for which in range(2):
            total_wait(first_z.at[half, which], zrecv.at[half, which])
        for site in range(sites):
            product = z_product(0, half, site)
            acc_ref[0, half, site] = full_product(0, half, site, product)

    def first_stats(half):
        total_wait(lo_in.at[half, pl.ds(0, sites - 1)], lrecv.at[half])
        sums = [0.0] * 3
        for site in range(sites):
            high = first_round[site, half].astype(jnp.float32)
            whole = high + decoded(lo_in[half, site])
            source_ref[half, site] = whole
            res_turned[half, site] = turned(whole)
            add_sums(0, half, site, acc_ref[0, half, site], sums)
        send_stats(0, half, sums)

    def far_product(it, half):
        for which in (2, 1):
            z_copy(it, half, which).wait_recv()
        for site in range(sites):
            product = z_product(it, half, site)
            acc_ref[it % 2, half, site] = full_product(it, half, site, product)
        sums = [0.0] * (3 + 2 * it)
        for site in range(sites):
            if site % span == 0:
                t_copy(it, half, site // span).wait_recv()
            q = t_product(it, half, site)
            acc_ref[it % 2, half, site] = q
            add_sums(it, half, site, q, sums)
        send_stats(it, half, sums)

    def send_stats(it, half, sums):
        lines_of = [jnp.sum(value, axis=0, keepdims=True) for value in sums]
        lines_of += [jnp.zeros((8 - len(lines_of), rhs), jnp.float32)]
        stats = jnp.concatenate(lines_of, axis=0)
        stats = stats + swapped(stats)
        low = lower_lanes((1, rhs))
        rows = [stats[at : at + 1] for at in range(7)]
        packed = jnp.concatenate(
            [rows[0], jnp.where(low, rows[1], -rows[2])]
            + [jnp.where(low, rows[at], rows[at + 1]) for at in (3, 5)],
            axis=0,
        )
        stat_out[it, half] = packed
        for other in others[:0:-1]:
            stat_copy(it, half, other).start()
        stat_in[it, half, me] = packed
        for site in range(sites):
            acc_turned[half, site] = turned(acc_ref[it % 2, half, site])

    scalars = [([], [], [], []) for _ in range(2)]

    def update(it, half):
        total_wait(stat_in.at[it, half, pl.ds(0, count - 1)], grecv.at[it, half])
        total = jnp.sum(stat_in[it, half], axis=0)
        moved = swapped(total)
        low = lower_lanes(total.shape)
        reals = jnp.where(low, total, moved)
        imags = jnp.where(low, moved, total)
        backs, epsilons, overlaps, _ = scalars[half]
        squared, cross_re, cross_im = reals[0:1], reals[1:2], imags[1:2]
        coefs = [(reals[2 + j : 3 + j], imags[2 + j : 3 + j]) for j in range(it)]
        for j, (c_re, c_im) in enumerate(coefs):
            squared = squared - (c_re * c_re + c_im * c_im) * (1.0 + epsilons[j])
            cross_re = cross_re - (c_re * backs[j][0] + c_im * backs[j][1])
            cross_im = cross_im - (c_re * backs[j][1] - c_im * backs[j][0])
        if it == 2:
            (a_re, a_im), (b_re, b_im) = coefs
            pair_re, pair_im = a_re * b_re + a_im * b_im, a_re * b_im - a_im * b_re
            squared = squared + 2.0 * (pair_re * overlaps[0][0] - pair_im * overlaps[0][1])
        factor = 1.0 / jnp.sqrt(squared + 1e-06)
        alpha = (cross_re * factor, cross_im * factor)
        epsilon = 1e-06 * factor * factor
        if it == 1:
            over = (coefs[0][0] * epsilons[0] * factor, coefs[0][1] * epsilons[0] * factor)
            overlaps.append(over)
            backs[0] = (
                backs[0][0] - (alpha[0] * over[0] - alpha[1] * over[1]),
                backs[0][1] - (alpha[0] * over[1] + alpha[1] * over[0]),
            )
        backs.append((alpha[0] * epsilon, alpha[1] * epsilon))
        epsilons.append(epsilon)
        gamma = (alpha[0] * factor, alpha[1] * factor)
        betas = [
            (gamma[0] * c_re - gamma[1] * c_im, gamma[0] * c_im + gamma[1] * c_re)
            for c_re, c_im in coefs
        ]
        for site in range(sites):
            change = gamma[0] * acc_ref[it % 2, half, site] + gamma[1] * acc_turned[half, site]
            for j, beta in enumerate(betas):
                change -= beta[0] * basis_q[j, half, site] + beta[1] * turned_q[j, half, site]
            new_res = residual_at(it, half, site) - change
            if it < ITERS - 1:
                res_half[it, half, site] = new_res
                round_ref[it, half, site] = new_res.astype(jnp.bfloat16)
                if site % span == span - 1:
                    pl.when(outer == 0)(lambda: t_copy(it + 1, half, site // span).start())
            elif half == 0:
                res_half[it, half, site] = new_res
            else:
                unpack(res_ref, site, res_half[it, 0, site], new_res)
        if it < ITERS - 1:
            for which in range(1, 3):
                z_copy(it + 1, half, which).start()

        def remaining():
            for site in range(sites):
                residual = residual_at(it, half, site)
                step = gamma[0] * residual + gamma[1] * res_turned[half, site]
                for j, beta in enumerate(betas):
                    step -= beta[0] * basis_p[j, half, site] + beta[1] * turned_p[j, half, site]
                new_sol = step if it == 0 else sol_half[half, site] + step
                if it == ITERS - 1 and half == 1:
                    unpack(sol_ref, site, sol_half[0, site], new_sol)
                else:
                    sol_half[half, site] = new_sol
                if it < ITERS - 1:
                    q = acc_ref[it % 2, half, site]
                    p = residual
                    for j, (c_re, c_im) in enumerate(coefs):
                        q -= c_re * basis_q[j, half, site] + c_im * turned_q[j, half, site]
                        p -= c_re * basis_p[j, half, site] + c_im * turned_p[j, half, site]
                    q = q * factor
                    p = p * factor
                    basis_q[it, half, site] = q
                    basis_p[it, half, site] = p
                    turned_q[it, half, site] = turned(q)
                    turned_p[it, half, site] = turned(p)
                    res_turned[half, site] = turned(res_half[it, half, site])

        return remaining

    def unpack(to_ref, site, first, second):
        low = lower_lanes(first.shape)
        to_ref[site, :comps] = jnp.where(low, first, swapped(second))
        to_ref[site, comps:] = jnp.where(low, swapped(first), second)

    send_after(0)
    pl.when(outer == 0)(lambda: send_rest(0))
    forward_all()
    pl.when(outer == 1)(lambda: send_rest(0))
    near_product(0, 0)
    near_product(0, 1)
    first_t_product(0)
    for site in range(sites):
        forward(1, site)
    send_after(1)
    send_rest(1)
    first_z_product(0)
    first_stats(0)
    first_t_product(1)
    first_z_product(1)
    first_stats(1)
    for it in range(ITERS):
        if it > 0:
            for half in range(2):
                far_product(it, half)
        for half in range(2):
            remaining = update(it, half)
            if it < ITERS - 1:
                near_product(it + 1, half)
            remaining()
            if it < ITERS - 1:
                send_late_halo(it + 1, half)

    total_wait(proj_ref.at[pl.ds(0, count - 1)], wsend.at[0])
    total_wait(part_out, psend.at[0])
    total_wait(hi_out.at[pl.ds(0, chips - 1)], ssend.at[0])
    total_wait(lo_out.at[pl.ds(0, chips - 1)], lsend.at[0])
    total_wait(hi_out.at[pl.ds(0, chips - 1)], tsend.at[0])
    total_wait(first_z, zsend.at[0])
    total_wait(halo_ref, hsend.at[0])
    total_wait(stat_in.at[:, :, pl.ds(0, count - 1)], gsend.at[0])


def store_kernel(sol_ref, res_ref, sol_hbm, res_hbm, sems):
    copies = [
        pltpu.make_async_copy(from_ref, to_ref, sems.at[at])
        for at, (from_ref, to_ref) in enumerate(((sol_ref, sol_hbm), (res_ref, res_hbm)))
    ]
    for copy in copies:
        copy.start()
    for copy in copies:
        copy.wait()


def stored(sol, res):
    vmem = pl.BlockSpec(memory_space=pltpu.VMEM)
    hbm = pl.BlockSpec(memory_space=pltpu.HBM)
    return pl.pallas_call(
        store_kernel,
        out_shape=[jax.ShapeDtypeStruct(value.shape, value.dtype) for value in (sol, res)],
        in_specs=[vmem, vmem],
        out_specs=[hbm, hbm],
        scratch_shapes=[pltpu.SemaphoreType.DMA((2,))],
        compiler_params=pltpu.CompilerParams(vmem_limit_bytes=1024 * 1024),
    )(sol, res)


def shards_kernel(fine_source, projectors, stencil_links, quark_mass):
    count = lax.axis_size("ta")
    planes, local_columns, _, _, null, rhs = fine_source.shape
    sites, comps = stencil_links.shape[1], stencil_links.shape[2]
    rows = local_columns * 4 * null
    fine = fine_source.reshape(planes, rows, rhs)
    proj = projectors.reshape(count, local_columns, 4 * null * null)
    width = local_columns * comps
    links = stencil_links.reshape(sites, comps, 18 * comps)
    chips = count // 2
    vector = (sites, 2 * comps, rhs)
    f32, bf16 = jnp.float32, jnp.bfloat16
    dma = pltpu.SemaphoreType.DMA
    vmem = pl.BlockSpec(memory_space=pltpu.VMEM)
    hbm = pl.BlockSpec(memory_space=pltpu.HBM)
    parts = (chips, 2, comps, rhs)
    half = (sites, comps, rhs)
    sol, res = pl.pallas_call(
        functools.partial(solve_kernel, count, sites, comps),
        out_shape=[pltpu.VMEM(vector, f32)] * 2,
        in_specs=[pl.BlockSpec(memory_space=pltpu.SMEM), hbm, hbm, hbm],
        out_specs=[vmem, vmem],
        scratch_shapes=[
            pltpu.VMEM(proj.shape, bf16),
            pltpu.VMEM(fine.shape, bf16),
            pltpu.VMEM(links.shape, bf16),
            pltpu.VMEM((sites, comps, 10 * comps), bf16),
            pltpu.VMEM((sites, comps, 4 * comps), bf16),
            pltpu.VMEM((sites, comps, 4 * comps), bf16),
            pltpu.VMEM(proj.shape, bf16),
            pltpu.VMEM((planes, width, 2 * rhs), bf16),
            pltpu.VMEM(parts, f32),
            pltpu.VMEM(parts, f32),
            pltpu.VMEM(parts, f32),
            pltpu.VMEM(parts, bf16),
            pltpu.VMEM(parts, bf16),
            pltpu.VMEM((2, sites, comps, rhs), bf16),
            pltpu.VMEM((2, sites, comps, rhs), f32),
            pltpu.VMEM((sites, 2, comps, rhs), bf16),
            pltpu.VMEM((2, 2, sites, comps, rhs), bf16),
            pltpu.VMEM((2, sites, comps, rhs), bf16),
            pltpu.VMEM((2, sites, 2 * comps, rhs), bf16),
            pltpu.VMEM((ITERS - 1, 2, *half), bf16),
            pltpu.VMEM((ITERS - 1, 2, 3, *half), bf16),
            pltpu.VMEM((2, 2, *half), f32),
            pltpu.VMEM((2, *half), f32),
            pltpu.VMEM((2, *half), f32),
            pltpu.VMEM((ITERS, 2, *half), f32),
            pltpu.VMEM((2, *half), f32),
            pltpu.VMEM((ITERS - 1, 2, *half), f32),
            pltpu.VMEM((ITERS - 1, 2, *half), f32),
            pltpu.VMEM((ITERS - 1, 2, *half), f32),
            pltpu.VMEM((ITERS - 1, 2, *half), f32),
            pltpu.VMEM((ITERS, 2, 4, rhs), f32),
            pltpu.VMEM((ITERS, 2, count, 4, rhs), f32),
            dma((3,)),
            dma((1,)),
            dma((count,)),
            dma((1,)),
            dma((chips,)),
            dma((1,)),
            dma((chips,)),
            dma((1,)),
            dma((2,)),
            dma((1,)),
            dma((2,)),
            dma((1,)),
            dma((2, 2)),
            dma((1,)),
            dma((2, 6)),
            dma((1,)),
            dma((ITERS, 2)),
        ],
        compiler_params=pltpu.CompilerParams(
            collective_id=0, has_side_effects=True, vmem_limit_bytes=60 * 1024 * 1024
        ),
    )(quark_mass, proj, fine, links)
    sol, res = stored(sol, res)
    return sol.reshape(1, *vector), res.reshape(1, *vector)


def shards(fine_source, projectors, stencil_links, quark_mass):
    count = lax.axis_size("ta")
    sites = stencil_links.shape[1]
    local_columns = fine_source.shape[1]
    block = projectors.shape[1] // sites
    fits = (
        count == 2 * LZ
        and count == 2 * sites
        and count & (count - 1) == 0
        and block == 2 * local_columns
        and stencil_links.shape[2] % local_columns == 0
        and fine_source.shape[0] == count
        and ITERS == 3
        and fine_source.shape[5] % 2 == 0
    )
    chosen = shards_kernel if fits else shards_general
    return chosen(fine_source, projectors, stencil_links, quark_mass)


def solution(mesh):
    return jax.shard_map(
        shards,
        mesh=mesh,
        in_specs=(
            P("cfg", "ta", None, None, None, None),
            P(("cfg", "ta"), None, None),
            P(("cfg", "ta"), None, None, None),
            P("cfg"),
        ),
        out_specs=(P(("cfg", "ta"), None, None, None), P(("cfg", "ta"), None, None, None)),
        check_vma=False,
    )
```

```python
import functools
import math

import jax
import jax.numpy as jnp
from jax import lax
from jax.experimental import pallas as pl
from jax.experimental.pallas import tpu as pltpu
from jax.sharding import PartitionSpec as P

LX = 4
LZ = 8
ITERS = 3


def from_behind(value, axis, steps):
    count = lax.axis_size(axis)
    pairs = [(source, (source + steps) % count) for source in range(count)]
    return lax.ppermute(value, axis, pairs)


def real_weights(proj_view):
    proj_re = proj_view[..., 0, :]
    proj_im = proj_view[..., 1, :]
    first_row = jnp.stack([proj_re, proj_im], axis=-4)
    second_row = jnp.stack([-proj_im, proj_re], axis=-4)
    return jnp.stack([first_row, second_row], axis=-5)


def inner_local(left, right, comp_count):
    left_re = left[:, :comp_count]
    left_im = left[:, comp_count:]
    right_re = right[:, :comp_count]
    right_im = right[:, comp_count:]
    return (
        jnp.sum(left_re * right_re + left_im * right_im, axis=(0, 1)),
        jnp.sum(left_re * right_im - left_im * right_re, axis=(0, 1)),
    )


def scaled(vector, factor_re, factor_im, comp_count):
    vector_re = vector[:, :comp_count]
    vector_im = vector[:, comp_count:]
    return jnp.concatenate(
        [
            factor_re * vector_re - factor_im * vector_im,
            factor_re * vector_im + factor_im * vector_re,
        ],
        axis=1,
    )


def shards_general(fine_source, projectors, stencil_links, quark_mass):
    comp_count = stencil_links.shape[2]
    null_count = comp_count // 2
    site_count = stencil_links.shape[1]
    column_count = projectors.shape[1]
    block_count = column_count // site_count
    fine_count = fine_source.shape[4]
    rhs_count = fine_source.shape[5]
    plane_count = fine_source.shape[0]
    moved_proj = lax.all_to_all(projectors, "ta", split_axis=1, concat_axis=0, tiled=True)
    local_columns = fine_source.shape[1]
    group_size = math.gcd(block_count, local_columns)
    groups = local_columns // group_size
    weights = real_weights(
        moved_proj.reshape(plane_count, groups, group_size, 2, null_count, 2, fine_count)
    )
    fine_local = fine_source.reshape(plane_count, groups, group_size, 2, 2, fine_count, rhs_count)
    partial_sums = jnp.einsum(
        "pmgdchvk,pmgchkr->pmdhvr", weights, fine_local, preferred_element_type=jnp.float32
    )
    partial_sums = partial_sums.reshape(plane_count, groups, 2 * comp_count, rhs_count)
    collected = lax.all_to_all(partial_sums, "ta", split_axis=0, concat_axis=1, tiled=True)
    source = jnp.sum(
        collected.reshape(site_count, block_count // group_size, 2 * comp_count, rhs_count), axis=1
    )
    link_view = stencil_links.reshape(site_count, comp_count, 9, 2, comp_count)
    link_re = link_view[:, :, :, 0, :]
    link_im = link_view[:, :, :, 1, :]
    upper_rows = jnp.stack([link_re, -link_im], axis=3)
    lower_rows = jnp.stack([link_im, link_re], axis=3)
    real_operator = jnp.stack([upper_rows, lower_rows], axis=1).reshape(
        site_count, 2 * comp_count, 18 * comp_count
    )
    mass_value = quark_mass[0]
    z_position = lax.axis_index("ta") % LZ
    line_count = site_count // LX

    def flatten_sites(shifted):
        return shifted.reshape(site_count, 2 * comp_count, rhs_count)

    solution = jnp.zeros_like(source)
    residual = source
    basis_q = []
    basis_p = []
    for iteration in range(ITERS):
        direction = residual
        rounded = residual.astype(jnp.bfloat16)
        plane_view = rounded.reshape(line_count, LX, 2 * comp_count, rhs_count)
        x_plus = flatten_sites(jnp.roll(plane_view, -1, axis=1))
        x_minus = flatten_sites(jnp.roll(plane_view, 1, axis=1))
        y_plus = flatten_sites(jnp.roll(plane_view, -1, axis=0))
        y_minus = flatten_sites(jnp.roll(plane_view, 1, axis=0))
        z_plus_near = from_behind(rounded, "ta", -1)
        z_minus_near = from_behind(rounded, "ta", 1)
        upper_pair = from_behind(jnp.stack([rounded, z_minus_near], axis=0), "ta", -LZ)
        lower_pair = from_behind(jnp.stack([rounded, z_plus_near], axis=0), "ta", LZ)
        t_plus = upper_pair[0]
        t_minus = lower_pair[0]
        z_plus = jnp.where(z_position == LZ - 1, lower_pair[1], z_plus_near)
        z_minus = jnp.where(z_position == 0, upper_pair[1], z_minus_near)
        stacked = jnp.stack(
            [rounded, x_plus, x_minus, y_plus, y_minus, z_plus, z_minus, t_plus, t_minus], axis=1
        )
        stacked = stacked.reshape(site_count, 18 * comp_count, rhs_count)
        product = jnp.einsum(
            "sij,sjr->sir", real_operator, stacked, preferred_element_type=jnp.float32
        )
        mapped = product + mass_value * rounded.astype(jnp.float32)
        square_loc = inner_local(mapped, mapped, comp_count)[0]
        cross_re, cross_im = inner_local(mapped, residual, comp_count)
        if iteration > 0:
            coef_pairs = [inner_local(earlier, mapped, comp_count) for earlier in basis_q]
            back_pairs = [inner_local(earlier, residual, comp_count) for earlier in basis_q]
            coef_re = jnp.stack([pair[0] for pair in coef_pairs])
            coef_im = jnp.stack([pair[1] for pair in coef_pairs])
            back_re = jnp.stack([pair[0] for pair in back_pairs])
            back_im = jnp.stack([pair[1] for pair in back_pairs])
        else:
            coef_re = jnp.zeros((1, rhs_count), jnp.float32)
            coef_im = jnp.zeros((1, rhs_count), jnp.float32)
            back_re = jnp.zeros((1, rhs_count), jnp.float32)
            back_im = jnp.zeros((1, rhs_count), jnp.float32)
        square_all, cross_re, cross_im, coef_re, coef_im, back_re, back_im = lax.psum(
            (square_loc, cross_re, cross_im, coef_re, coef_im, back_re, back_im), "ta"
        )
        squared = square_all
        proj_re = cross_re
        proj_im = cross_im
        for number in range(iteration):
            mapped = mapped - scaled(basis_q[number], coef_re[number], coef_im[number], comp_count)
            direction = direction - scaled(
                basis_p[number], coef_re[number], coef_im[number], comp_count
            )
            squared = squared - (
                coef_re[number] * coef_re[number] + coef_im[number] * coef_im[number]
            )
            proj_re = proj_re - (
                coef_re[number] * back_re[number] + coef_im[number] * back_im[number]
            )
            proj_im = proj_im - (
                coef_re[number] * back_im[number] - coef_im[number] * back_re[number]
            )
        factor = 1.0 / jnp.sqrt(squared + 1e-06)
        unit_q = mapped * factor
        unit_p = direction * factor
        alpha_re = proj_re * factor
        alpha_im = proj_im * factor
        solution = solution + scaled(unit_p, alpha_re, alpha_im, comp_count)
        residual = residual - scaled(unit_q, alpha_re, alpha_im, comp_count)
        basis_q.append(unit_q)
        basis_p.append(unit_p)
    return (
        solution.reshape(1, site_count, 2 * comp_count, rhs_count),
        residual.reshape(1, site_count, 2 * comp_count, rhs_count),
    )


MESH = pl.DeviceIdType.MESH


def flipped(number, mask, bits):
    total = 0
    for bit in range(bits):
        size = 1 << bit
        total = total + (((number // size) % 2 + (mask // size) % 2) % 2) * size
    return total


def swapped(value):
    return pltpu.roll(value, value.shape[-1] // 2, value.ndim - 1)


def lower_lanes(shape):
    return lax.broadcasted_iota(jnp.int32, shape, len(shape) - 1) < shape[-1] // 2


def turned(value):
    other = swapped(value)
    return jnp.where(lower_lanes(value.shape), -other, other)


def widened(rounded):
    return jnp.concatenate(
        [rounded, turned(rounded.astype(jnp.float32)).astype(jnp.bfloat16)], axis=0
    )


def times(factor, value):
    return factor[0] * value + factor[1] * turned(value)


def total_wait(region, sem):
    pltpu.make_async_copy(region, region, sem).wait()


def transposed(value, columns, comps):
    row = lax.broadcasted_iota(jnp.int32, value.shape, 0)
    chunk = lax.broadcasted_iota(jnp.int32, value.shape, 1) // comps
    width = value.shape[1]
    bits = columns.bit_length() - 1
    for bit in range(bits):
        size = 1 << bit
        moved = pltpu.roll(value, width - size * comps, 1)
        value = jnp.where((row // size) % 2 == 1, moved, value)
    for bit in range(bits):
        size = 1 << bit
        moved = pltpu.roll(value, size, 0)
        value = jnp.where((chunk // size) % 2 == 1, moved, value)
    for bit in range(bits):
        size = 1 << bit
        moved = pltpu.roll(value, width - size * comps, 1)
        value = jnp.where((row // size) % 2 == 1, moved, value)
    return value


CODE_SCALE = 2.0**12


def coded(rest):
    square = rest * rest * (CODE_SCALE * CODE_SCALE)
    fourth = square * square
    eighth = fourth * fourth
    return jnp.where(rest < 0.0, -eighth, eighth).astype(jnp.bfloat16)


def decoded(code):
    value = code.astype(jnp.float32)
    root = jnp.sqrt(jnp.sqrt(jnp.sqrt(jnp.abs(value)))) * (1.0 / CODE_SCALE)
    return jnp.where(value < 0.0, -root, root)


def solve_kernel(
    count, sites, comps,
    mass_ref, proj_hbm, fine_hbm, links_hbm,
    sol_ref, res_ref,
    proj_ref, fine_ref, links_ref, near_ref, zlinks_ref, tlinks_ref,
    weights_in, rights_ref, part_keep, part_out, part_in, hi_out, lo_out, lo_in, source_ref,
    first_round, first_z, first_t,
    wide_ref, round_ref, halo_ref, acc_ref, acc_turned, sol_half, res_half, res_turned,
    basis_q, basis_p, turned_q, turned_p, stat_out, stat_in,
    local_sem, wsend, wrecv, psend, precv, ssend, srecv, tsend, trecv, lsend, lrecv, zsend, zrecv,
    hsend, hrecv, gsend, grecv,
):
    me = lax.axis_index("ta")
    bits = count.bit_length() - 1
    core = me % 2
    chip = me // 2
    partner = chip * 2 + 1 - core
    chips = count // 2
    far = chips // 2
    turns = [(1 - 2 * ((me // (1 << bit)) % 2)) * (1 << bit) for bit in range(bits)]
    others = [me]
    for step in range(1, count):
        top = step.bit_length() - 1
        others.append(others[step - (1 << top)] + turns[top])
    null = comps // 2
    rhs = fine_ref.shape[2]
    columns = proj_ref.shape[1]
    width = columns * comps
    groups = comps // columns

    proj_copy = pltpu.make_async_copy(proj_hbm, proj_ref, local_sem.at[2])
    proj_copy.start()
    barrier = pltpu.get_barrier_semaphore()
    for other in others[:0:-1]:
        pl.semaphore_signal(barrier, inc=1, device_id={"ta": other}, device_id_type=MESH)
    fine_copy = pltpu.make_async_copy(fine_hbm, fine_ref, local_sem.at[0])
    fine_copy.start()
    links_copy = pltpu.make_async_copy(links_hbm, links_ref, local_sem.at[1])
    links_copy.start()
    proj_copy.wait()
    pl.semaphore_wait(barrier, count - 1)

    def weights_copy(other, origin):
        return pltpu.make_async_remote_copy(
            src_ref=proj_ref.at[other], dst_ref=weights_in.at[origin],
            send_sem=wsend.at[0], recv_sem=wrecv.at[origin // 2],
            device_id={"ta": other}, device_id_type=MESH,
        )

    quarter = me // (count // 4)
    outer = 1 - (quarter % 3 + 1) // 2
    for step in range(1, 4):
        weights_copy(others[step], me).start()
    for step in range(count // 2, count):
        crossed = step ^ (count // 4)
        weights_copy(outer * others[step] + (1 - outer) * others[crossed], me).start()
    for step in range(4, count // 2):
        weights_copy(others[step], me).start()

    fine_copy.wait()

    def build_right(plane, carry):
        fine = fine_ref[plane].astype(jnp.float32).reshape(columns, 2, 2, null, rhs)
        turned_order = [fine[(columns - at) % columns] for at in range(columns)]
        for half in range(2):
            picked = [
                block[part, half] for block in turned_order for part in range(2)
            ]
            rights_ref[plane, :, half * rhs : (half + 1) * rhs] = jnp.concatenate(
                picked, axis=0
            ).astype(jnp.bfloat16)
        return carry

    lax.fori_loop(0, count, build_right, 0)

    links_copy.wait()
    for site in range(sites):
        near_ref[site] = links_ref[site, :, : 10 * comps]
        zlinks_ref[site] = links_ref[site, :, 10 * comps : 14 * comps]
        tlinks_ref[site] = links_ref[site, :, 14 * comps : 18 * comps]

    def restricted(plane, raw_ref):
        raw = raw_ref[plane].astype(jnp.float32)
        pieces = [
            transposed(raw[:, group * width : (group + 1) * width], columns, comps)
            for group in range(groups)
        ]
        upper = jnp.concatenate(pieces, axis=0)
        lane = lax.broadcasted_iota(jnp.int32, upper.shape, 1) % comps
        lower = jnp.where(
            lane < null, -pltpu.roll(upper, width - null, 1), pltpu.roll(upper, null, 1)
        )
        left = jnp.concatenate([upper, lower], axis=0).astype(jnp.bfloat16)
        total = jnp.dot(left, rights_ref[plane], preferred_element_type=jnp.float32)
        real = jnp.concatenate([total[:null, :rhs], total[null:comps, rhs:]], axis=0)
        imag = jnp.concatenate(
            [total[comps : comps + null, :rhs], total[comps + null :, rhs:]], axis=0
        )
        low = lower_lanes(real.shape)
        return jnp.stack(
            [jnp.where(low, real, swapped(imag)), jnp.where(low, swapped(real), imag)], axis=0
        )

    def part_copy(slot):
        return pltpu.make_async_remote_copy(
            src_ref=part_out.at[slot], dst_ref=part_in.at[slot],
            send_sem=psend.at[0], recv_sem=precv.at[slot],
            device_id={"ta": partner}, device_id_type=MESH,
        )

    def source_copy(slot, origin):
        return pltpu.make_async_remote_copy(
            src_ref=hi_out.at[slot], dst_ref=first_round.at[origin],
            send_sem=ssend.at[0], recv_sem=srecv.at[origin],
            device_id={"ta": flipped(chip, slot, bits - 1) * 2 + core}, device_id_type=MESH,
        )

    def rest_copy(slot, half):
        return pltpu.make_async_remote_copy(
            src_ref=lo_out.at[slot, half], dst_ref=lo_in.at[half, chip],
            send_sem=lsend.at[0], recv_sem=lrecv.at[half],
            device_id={"ta": others[2 * slot]}, device_id_type=MESH,
        )

    def first_t_copy(slot, half):
        return pltpu.make_async_remote_copy(
            src_ref=hi_out.at[slot, half], dst_ref=first_t.at[half, chip],
            send_sem=tsend.at[0], recv_sem=trecv.at[half],
            device_id={"ta": others[2 * (slot ^ far)]}, device_id_type=MESH,
        )

    def pair(step):
        other = flipped(chip, step, bits - 1)
        away = other * 2 + 1 - core
        kept = other * 2 + core
        total_wait(weights_in.at[pl.ds(other * 2, 2)], wrecv.at[other])
        sent, held = restricted(away, weights_in), restricted(kept, weights_in)
        part_out[step] = sent
        part_keep[step] = held
        part_copy(step).start()

    def finish(step):
        part_copy(step).wait_recv()
        total = part_keep[step] + part_in[step]
        rounded = total.astype(jnp.bfloat16)
        hi_out[step] = rounded
        source_copy(step, chip).start()
        lo_out[step] = coded(total - rounded.astype(jnp.float32))

    base = (me // LZ) * LZ
    z_at = me % LZ
    above = base + (z_at + 1) % LZ
    below = base + (z_at + LZ - 1) % LZ
    other_time = (me + LZ) % count
    targets = (other_time, above, below)
    lines = sites // LX

    def first_z_copy(half, which, site):
        return pltpu.make_async_remote_copy(
            src_ref=first_round.at[site, half], dst_ref=first_z.at[half, which, site],
            send_sem=zsend.at[0], recv_sem=zrecv.at[half, which],
            device_id={"ta": targets[1 + which]}, device_id_type=MESH,
        )

    def forward(half, site):
        for which in range(2):
            first_z_copy(half, which, site).start()

    weights_copy(partner, partner).wait_recv()
    sent, held = restricted(partner, weights_in), restricted(me, proj_ref)
    part_out[0] = sent
    part_keep[0] = held
    part_copy(0).start()
    pair(1)
    part_copy(0).wait_recv()
    own = part_keep[0] + part_in[0]
    own_rounded = own.astype(jnp.bfloat16)
    hi_out[0] = own_rounded
    first_round[chip] = own_rounded
    own_rest = coded(own - own_rounded.astype(jnp.float32))
    for half in range(2):
        lo_in[half, chip] = own_rest[half]
    forward(0, chip)

    def arranged(at):
        group = at // 2
        later = outer * ((2 * group + 1) % 3 + 1) + (1 - outer) * (group % 3 + 1)
        return ((group + 2) // 3) * later * 2 + at % 2

    def pair_step(at, carry):
        pair(arranged(at))
        finish(arranged(at - 1))
        return carry

    lax.fori_loop(2, chips, pair_step, 0)
    finish(arranged(chips - 1))

    def send_after(half):
        first_t[half, chip] = hi_out[far, half]
        for step in range(chips - 1, -1, -1):
            if step != far:
                first_t_copy(step, half).start()

    def send_rest(half):
        for step in range(chips - 1, 0, -1):
            rest_copy(step, half).start()

    def forward_all():
        def forward_step(at, carry):
            site = flipped(chip, arranged(at), bits - 1)
            source_copy(0, site).wait_recv()
            forward(0, site)
            return carry

        lax.fori_loop(1, chips, forward_step, 0)

    mass = mass_ref[0]

    def place(site, dx, dy):
        return ((site // LX + dy) % lines) * LX + (site % LX + dx) % LX

    pieces = 2
    span = sites // pieces

    def z_copy(it, half, which):
        return pltpu.make_async_remote_copy(
            src_ref=round_ref.at[it - 1, half], dst_ref=halo_ref.at[it - 1, half, which],
            send_sem=hsend.at[0], recv_sem=hrecv.at[half, which - 1],
            device_id={"ta": targets[which]}, device_id_type=MESH,
        )

    def t_copy(it, half, piece):
        part = pl.ds(piece * span, span)
        return pltpu.make_async_remote_copy(
            src_ref=round_ref.at[it - 1, half, part], dst_ref=halo_ref.at[it - 1, half, 0, part],
            send_sem=hsend.at[0], recv_sem=hrecv.at[half, 2 + piece],
            device_id={"ta": other_time}, device_id_type=MESH,
        )

    def send_t(it, half):
        for piece in range(pieces):
            t_copy(it, half, piece).start()

    def stat_copy(it, half, other):
        return pltpu.make_async_remote_copy(
            src_ref=stat_out.at[it, half], dst_ref=stat_in.at[it, half, me],
            send_sem=gsend.at[0], recv_sem=grecv.at[it, half],
            device_id={"ta": other}, device_id_type=MESH,
        )

    def residual_at(it, half, site):
        return source_ref[half, site] if it == 0 else res_half[it - 1, half, site]

    def rounded_at(it, half, site):
        return first_round[site, half] if it == 0 else round_ref[it - 1, half, site]

    def halo_at(it, half, which, site):
        if it > 0:
            return halo_ref[it - 1, half, which, site]
        return first_t[half, site] if which == 0 else first_z[half, which - 1, site]

    def send_late_halo(it, half):
        pl.when(outer == 1)(lambda: send_t(it, half))

    def near_product(it, half):
        for site in range(sites):
            wide_ref[half, site] = widened(rounded_at(it, half, site))
        steps = ((0, 0), (1, 0), (-1, 0), (0, 1), (0, -1))
        for site in range(sites):
            right = jnp.concatenate(
                [wide_ref[half, place(site, dx, dy)] for dx, dy in steps], axis=0
            )
            acc_ref[it % 2, half, site] = jnp.dot(
                near_ref[site], right, preferred_element_type=jnp.float32
            )

    def z_product(it, half, site):
        right = jnp.concatenate(
            [widened(halo_at(it, half, 2, site)), widened(halo_at(it, half, 1, site))], axis=0
        )
        return acc_ref[it % 2, half, site] + jnp.dot(
            zlinks_ref[site], right, preferred_element_type=jnp.float32
        )

    def t_product(it, half, site):
        wide = widened(halo_at(it, half, 0, site))
        right = jnp.concatenate([wide, wide], axis=0)
        return acc_ref[it % 2, half, site] + jnp.dot(
            tlinks_ref[site], right, preferred_element_type=jnp.float32
        )

    def full_product(it, half, site, product):
        return product + mass * rounded_at(it, half, site).astype(jnp.float32)

    def add_sums(it, half, site, q, sums):
        sums[0] += q * q
        sums[1] += q * residual_at(it, half, site)
        sums[2] += q * res_turned[half, site]
        for j in range(it):
            sums[3 + 2 * j] += basis_q[j, half, site] * q
            sums[4 + 2 * j] += turned_q[j, half, site] * q

    def first_t_product(half):
        total_wait(first_t.at[half, pl.ds(0, sites - 1)], trecv.at[half])
        for site in range(sites):
            acc_ref[0, half, site] = t_product(0, half, site)

    def first_z_product(half):
        for which in range(2):
            total_wait(first_z.at[half, which], zrecv.at[half, which])
        for site in range(sites):
            product = z_product(0, half, site)
            acc_ref[0, half, site] = full_product(0, half, site, product)

    def first_stats(half):
        total_wait(lo_in.at[half, pl.ds(0, sites - 1)], lrecv.at[half])
        sums = [0.0] * 3
        for site in range(sites):
            high = first_round[site, half].astype(jnp.float32)
            whole = high + decoded(lo_in[half, site])
            source_ref[half, site] = whole
            res_turned[half, site] = turned(whole)
            add_sums(0, half, site, acc_ref[0, half, site], sums)
        send_stats(0, half, sums)

    def far_product(it, half):
        for which in (2, 1):
            z_copy(it, half, which).wait_recv()
        for site in range(sites):
            product = z_product(it, half, site)
            acc_ref[it % 2, half, site] = full_product(it, half, site, product)
        sums = [0.0] * (3 + 2 * it)
        for site in range(sites):
            if site % span == 0:
                t_copy(it, half, site // span).wait_recv()
            q = t_product(it, half, site)
            acc_ref[it % 2, half, site] = q
            add_sums(it, half, site, q, sums)
        send_stats(it, half, sums)

    def send_stats(it, half, sums):
        lines_of = [jnp.sum(value, axis=0, keepdims=True) for value in sums]
        lines_of += [jnp.zeros((8 - len(lines_of), rhs), jnp.float32)]
        stats = jnp.concatenate(lines_of, axis=0)
        stats = stats + swapped(stats)
        low = lower_lanes((1, rhs))
        rows = [stats[at : at + 1] for at in range(7)]
        packed = jnp.concatenate(
            [rows[0], jnp.where(low, rows[1], -rows[2])]
            + [jnp.where(low, rows[at], rows[at + 1]) for at in (3, 5)],
            axis=0,
        )
        stat_out[it, half] = packed
        for other in others[:0:-1]:
            stat_copy(it, half, other).start()
        stat_in[it, half, me] = packed
        for site in range(sites):
            acc_turned[half, site] = turned(acc_ref[it % 2, half, site])

    scalars = [([], [], [], []) for _ in range(2)]

    def update(it, half):
        total_wait(stat_in.at[it, half, pl.ds(0, count - 1)], grecv.at[it, half])
        total = jnp.sum(stat_in[it, half], axis=0)
        moved = swapped(total)
        low = lower_lanes(total.shape)
        reals = jnp.where(low, total, moved)
        imags = jnp.where(low, moved, total)
        backs, epsilons, overlaps, _ = scalars[half]
        squared, cross_re, cross_im = reals[0:1], reals[1:2], imags[1:2]
        coefs = [(reals[2 + j : 3 + j], imags[2 + j : 3 + j]) for j in range(it)]
        for j, (c_re, c_im) in enumerate(coefs):
            squared = squared - (c_re * c_re + c_im * c_im) * (1.0 + epsilons[j])
            cross_re = cross_re - (c_re * backs[j][0] + c_im * backs[j][1])
            cross_im = cross_im - (c_re * backs[j][1] - c_im * backs[j][0])
        if it == 2:
            (a_re, a_im), (b_re, b_im) = coefs
            pair_re, pair_im = a_re * b_re + a_im * b_im, a_re * b_im - a_im * b_re
            squared = squared + 2.0 * (pair_re * overlaps[0][0] - pair_im * overlaps[0][1])
        factor = 1.0 / jnp.sqrt(squared + 1e-06)
        alpha = (cross_re * factor, cross_im * factor)
        epsilon = 1e-06 * factor * factor
        if it == 1:
            over = (coefs[0][0] * epsilons[0] * factor, coefs[0][1] * epsilons[0] * factor)
            overlaps.append(over)
            backs[0] = (
                backs[0][0] - (alpha[0] * over[0] - alpha[1] * over[1]),
                backs[0][1] - (alpha[0] * over[1] + alpha[1] * over[0]),
            )
        backs.append((alpha[0] * epsilon, alpha[1] * epsilon))
        epsilons.append(epsilon)
        gamma = (alpha[0] * factor, alpha[1] * factor)
        betas = [
            (gamma[0] * c_re - gamma[1] * c_im, gamma[0] * c_im + gamma[1] * c_re)
            for c_re, c_im in coefs
        ]
        for site in range(sites):
            change = gamma[0] * acc_ref[it % 2, half, site] + gamma[1] * acc_turned[half, site]
            for j, beta in enumerate(betas):
                change -= beta[0] * basis_q[j, half, site] + beta[1] * turned_q[j, half, site]
            new_res = residual_at(it, half, site) - change
            if it < ITERS - 1:
                res_half[it, half, site] = new_res
                round_ref[it, half, site] = new_res.astype(jnp.bfloat16)
                if site % span == span - 1:
                    pl.when(outer == 0)(lambda: t_copy(it + 1, half, site // span).start())
            elif half == 0:
                res_half[it, half, site] = new_res
            else:
                unpack(res_ref, site, res_half[it, 0, site], new_res)
        if it < ITERS - 1:
            for which in range(1, 3):
                z_copy(it + 1, half, which).start()

        def remaining():
            for site in range(sites):
                residual = residual_at(it, half, site)
                step = gamma[0] * residual + gamma[1] * res_turned[half, site]
                for j, beta in enumerate(betas):
                    step -= beta[0] * basis_p[j, half, site] + beta[1] * turned_p[j, half, site]
                new_sol = step if it == 0 else sol_half[half, site] + step
                if it == ITERS - 1 and half == 1:
                    unpack(sol_ref, site, sol_half[0, site], new_sol)
                else:
                    sol_half[half, site] = new_sol
                if it < ITERS - 1:
                    q = acc_ref[it % 2, half, site]
                    p = residual
                    for j, (c_re, c_im) in enumerate(coefs):
                        q -= c_re * basis_q[j, half, site] + c_im * turned_q[j, half, site]
                        p -= c_re * basis_p[j, half, site] + c_im * turned_p[j, half, site]
                    q = q * factor
                    p = p * factor
                    basis_q[it, half, site] = q
                    basis_p[it, half, site] = p
                    turned_q[it, half, site] = turned(q)
                    turned_p[it, half, site] = turned(p)
                    res_turned[half, site] = turned(res_half[it, half, site])

        return remaining

    def unpack(to_ref, site, first, second):
        low = lower_lanes(first.shape)
        to_ref[site, :comps] = jnp.where(low, first, swapped(second))
        to_ref[site, comps:] = jnp.where(low, swapped(first), second)

    send_after(0)
    pl.when(outer == 0)(lambda: send_rest(0))
    forward_all()
    pl.when(outer == 1)(lambda: send_rest(0))
    near_product(0, 0)
    near_product(0, 1)
    for site in range(sites):
        forward(1, site)
    send_after(1)
    first_t_product(0)
    send_rest(1)
    first_z_product(0)
    first_stats(0)
    first_t_product(1)
    first_z_product(1)
    first_stats(1)
    for it in range(ITERS):
        if it > 0:
            for half in range(2):
                far_product(it, half)
        for half in range(2):
            remaining = update(it, half)
            if it < ITERS - 1:
                near_product(it + 1, half)
            remaining()
            if it < ITERS - 1:
                send_late_halo(it + 1, half)

    total_wait(proj_ref.at[pl.ds(0, count - 1)], wsend.at[0])
    total_wait(part_out, psend.at[0])
    total_wait(hi_out.at[pl.ds(0, chips - 1)], ssend.at[0])
    total_wait(lo_out.at[pl.ds(0, chips - 1)], lsend.at[0])
    total_wait(hi_out.at[pl.ds(0, chips - 1)], tsend.at[0])
    total_wait(first_z, zsend.at[0])
    total_wait(halo_ref, hsend.at[0])
    total_wait(stat_in.at[:, :, pl.ds(0, count - 1)], gsend.at[0])


def store_kernel(sol_ref, res_ref, sol_hbm, res_hbm, sems):
    copies = [
        pltpu.make_async_copy(from_ref, to_ref, sems.at[at])
        for at, (from_ref, to_ref) in enumerate(((sol_ref, sol_hbm), (res_ref, res_hbm)))
    ]
    for copy in copies:
        copy.start()
    for copy in copies:
        copy.wait()


def stored(sol, res):
    vmem = pl.BlockSpec(memory_space=pltpu.VMEM)
    hbm = pl.BlockSpec(memory_space=pltpu.HBM)
    return pl.pallas_call(
        store_kernel,
        out_shape=[jax.ShapeDtypeStruct(value.shape, value.dtype) for value in (sol, res)],
        in_specs=[vmem, vmem],
        out_specs=[hbm, hbm],
        scratch_shapes=[pltpu.SemaphoreType.DMA((2,))],
        compiler_params=pltpu.CompilerParams(vmem_limit_bytes=1024 * 1024),
    )(sol, res)


def shards_kernel(fine_source, projectors, stencil_links, quark_mass):
    count = lax.axis_size("ta")
    planes, local_columns, _, _, null, rhs = fine_source.shape
    sites, comps = stencil_links.shape[1], stencil_links.shape[2]
    rows = local_columns * 4 * null
    fine = fine_source.reshape(planes, rows, rhs)
    proj = projectors.reshape(count, local_columns, 4 * null * null)
    width = local_columns * comps
    links = stencil_links.reshape(sites, comps, 18 * comps)
    chips = count // 2
    vector = (sites, 2 * comps, rhs)
    f32, bf16 = jnp.float32, jnp.bfloat16
    dma = pltpu.SemaphoreType.DMA
    vmem = pl.BlockSpec(memory_space=pltpu.VMEM)
    hbm = pl.BlockSpec(memory_space=pltpu.HBM)
    parts = (chips, 2, comps, rhs)
    half = (sites, comps, rhs)
    sol, res = pl.pallas_call(
        functools.partial(solve_kernel, count, sites, comps),
        out_shape=[pltpu.VMEM(vector, f32)] * 2,
        in_specs=[pl.BlockSpec(memory_space=pltpu.SMEM), hbm, hbm, hbm],
        out_specs=[vmem, vmem],
        scratch_shapes=[
            pltpu.VMEM(proj.shape, bf16),
            pltpu.VMEM(fine.shape, bf16),
            pltpu.VMEM(links.shape, bf16),
            pltpu.VMEM((sites, comps, 10 * comps), bf16),
            pltpu.VMEM((sites, comps, 4 * comps), bf16),
            pltpu.VMEM((sites, comps, 4 * comps), bf16),
            pltpu.VMEM(proj.shape, bf16),
            pltpu.VMEM((planes, width, 2 * rhs), bf16),
            pltpu.VMEM(parts, f32),
            pltpu.VMEM(parts, f32),
            pltpu.VMEM(parts, f32),
            pltpu.VMEM(parts, bf16),
            pltpu.VMEM(parts, bf16),
            pltpu.VMEM((2, sites, comps, rhs), bf16),
            pltpu.VMEM((2, sites, comps, rhs), f32),
            pltpu.VMEM((sites, 2, comps, rhs), bf16),
            pltpu.VMEM((2, 2, sites, comps, rhs), bf16),
            pltpu.VMEM((2, sites, comps, rhs), bf16),
            pltpu.VMEM((2, sites, 2 * comps, rhs), bf16),
            pltpu.VMEM((ITERS - 1, 2, *half), bf16),
            pltpu.VMEM((ITERS - 1, 2, 3, *half), bf16),
            pltpu.VMEM((2, 2, *half), f32),
            pltpu.VMEM((2, *half), f32),
            pltpu.VMEM((2, *half), f32),
            pltpu.VMEM((ITERS, 2, *half), f32),
            pltpu.VMEM((2, *half), f32),
            pltpu.VMEM((ITERS - 1, 2, *half), f32),
            pltpu.VMEM((ITERS - 1, 2, *half), f32),
            pltpu.VMEM((ITERS - 1, 2, *half), f32),
            pltpu.VMEM((ITERS - 1, 2, *half), f32),
            pltpu.VMEM((ITERS, 2, 4, rhs), f32),
            pltpu.VMEM((ITERS, 2, count, 4, rhs), f32),
            dma((3,)),
            dma((1,)),
            dma((chips,)),
            dma((1,)),
            dma((chips,)),
            dma((1,)),
            dma((chips,)),
            dma((1,)),
            dma((2,)),
            dma((1,)),
            dma((2,)),
            dma((1,)),
            dma((2, 2)),
            dma((1,)),
            dma((2, 4)),
            dma((1,)),
            dma((ITERS, 2)),
        ],
        compiler_params=pltpu.CompilerParams(
            collective_id=0, has_side_effects=True, vmem_limit_bytes=60 * 1024 * 1024
        ),
    )(quark_mass, proj, fine, links)
    sol, res = stored(sol, res)
    return sol.reshape(1, *vector), res.reshape(1, *vector)


def shards(fine_source, projectors, stencil_links, quark_mass):
    count = lax.axis_size("ta")
    sites = stencil_links.shape[1]
    local_columns = fine_source.shape[1]
    block = projectors.shape[1] // sites
    fits = (
        count == 2 * LZ
        and count == 2 * sites
        and count & (count - 1) == 0
        and block == 2 * local_columns
        and stencil_links.shape[2] % local_columns == 0
        and fine_source.shape[0] == count
        and ITERS == 3
        and fine_source.shape[5] % 2 == 0
    )
    chosen = shards_kernel if fits else shards_general
    return chosen(fine_source, projectors, stencil_links, quark_mass)


def solution(mesh):
    return jax.shard_map(
        shards,
        mesh=mesh,
        in_specs=(
            P("cfg", "ta", None, None, None, None),
            P(("cfg", "ta"), None, None),
            P(("cfg", "ta"), None, None, None),
            P("cfg"),
        ),
        out_specs=(P(("cfg", "ta"), None, None, None), P(("cfg", "ta"), None, None, None)),
        check_vma=False,
    )
```

```python
import functools
import math

import jax
import jax.numpy as jnp
from jax import lax
from jax.experimental import pallas as pl
from jax.experimental.pallas import tpu as pltpu
from jax.sharding import PartitionSpec as P

LX = 4
LZ = 8
ITERS = 3


def from_behind(value, axis, steps):
    count = lax.axis_size(axis)
    pairs = [(source, (source + steps) % count) for source in range(count)]
    return lax.ppermute(value, axis, pairs)


def real_weights(proj_view):
    proj_re = proj_view[..., 0, :]
    proj_im = proj_view[..., 1, :]
    first_row = jnp.stack([proj_re, proj_im], axis=-4)
    second_row = jnp.stack([-proj_im, proj_re], axis=-4)
    return jnp.stack([first_row, second_row], axis=-5)


def inner_local(left, right, comp_count):
    left_re = left[:, :comp_count]
    left_im = left[:, comp_count:]
    right_re = right[:, :comp_count]
    right_im = right[:, comp_count:]
    return (
        jnp.sum(left_re * right_re + left_im * right_im, axis=(0, 1)),
        jnp.sum(left_re * right_im - left_im * right_re, axis=(0, 1)),
    )


def scaled(vector, factor_re, factor_im, comp_count):
    vector_re = vector[:, :comp_count]
    vector_im = vector[:, comp_count:]
    return jnp.concatenate(
        [
            factor_re * vector_re - factor_im * vector_im,
            factor_re * vector_im + factor_im * vector_re,
        ],
        axis=1,
    )


def shards_general(fine_source, projectors, stencil_links, quark_mass):
    comp_count = stencil_links.shape[2]
    null_count = comp_count // 2
    site_count = stencil_links.shape[1]
    column_count = projectors.shape[1]
    block_count = column_count // site_count
    fine_count = fine_source.shape[4]
    rhs_count = fine_source.shape[5]
    plane_count = fine_source.shape[0]
    moved_proj = lax.all_to_all(projectors, "ta", split_axis=1, concat_axis=0, tiled=True)
    local_columns = fine_source.shape[1]
    group_size = math.gcd(block_count, local_columns)
    groups = local_columns // group_size
    weights = real_weights(
        moved_proj.reshape(plane_count, groups, group_size, 2, null_count, 2, fine_count)
    )
    fine_local = fine_source.reshape(plane_count, groups, group_size, 2, 2, fine_count, rhs_count)
    partial_sums = jnp.einsum(
        "pmgdchvk,pmgchkr->pmdhvr", weights, fine_local, preferred_element_type=jnp.float32
    )
    partial_sums = partial_sums.reshape(plane_count, groups, 2 * comp_count, rhs_count)
    collected = lax.all_to_all(partial_sums, "ta", split_axis=0, concat_axis=1, tiled=True)
    source = jnp.sum(
        collected.reshape(site_count, block_count // group_size, 2 * comp_count, rhs_count), axis=1
    )
    link_view = stencil_links.reshape(site_count, comp_count, 9, 2, comp_count)
    link_re = link_view[:, :, :, 0, :]
    link_im = link_view[:, :, :, 1, :]
    upper_rows = jnp.stack([link_re, -link_im], axis=3)
    lower_rows = jnp.stack([link_im, link_re], axis=3)
    real_operator = jnp.stack([upper_rows, lower_rows], axis=1).reshape(
        site_count, 2 * comp_count, 18 * comp_count
    )
    mass_value = quark_mass[0]
    z_position = lax.axis_index("ta") % LZ
    line_count = site_count // LX

    def flatten_sites(shifted):
        return shifted.reshape(site_count, 2 * comp_count, rhs_count)

    solution = jnp.zeros_like(source)
    residual = source
    basis_q = []
    basis_p = []
    for iteration in range(ITERS):
        direction = residual
        rounded = residual.astype(jnp.bfloat16)
        plane_view = rounded.reshape(line_count, LX, 2 * comp_count, rhs_count)
        x_plus = flatten_sites(jnp.roll(plane_view, -1, axis=1))
        x_minus = flatten_sites(jnp.roll(plane_view, 1, axis=1))
        y_plus = flatten_sites(jnp.roll(plane_view, -1, axis=0))
        y_minus = flatten_sites(jnp.roll(plane_view, 1, axis=0))
        z_plus_near = from_behind(rounded, "ta", -1)
        z_minus_near = from_behind(rounded, "ta", 1)
        upper_pair = from_behind(jnp.stack([rounded, z_minus_near], axis=0), "ta", -LZ)
        lower_pair = from_behind(jnp.stack([rounded, z_plus_near], axis=0), "ta", LZ)
        t_plus = upper_pair[0]
        t_minus = lower_pair[0]
        z_plus = jnp.where(z_position == LZ - 1, lower_pair[1], z_plus_near)
        z_minus = jnp.where(z_position == 0, upper_pair[1], z_minus_near)
        stacked = jnp.stack(
            [rounded, x_plus, x_minus, y_plus, y_minus, z_plus, z_minus, t_plus, t_minus], axis=1
        )
        stacked = stacked.reshape(site_count, 18 * comp_count, rhs_count)
        product = jnp.einsum(
            "sij,sjr->sir", real_operator, stacked, preferred_element_type=jnp.float32
        )
        mapped = product + mass_value * rounded.astype(jnp.float32)
        square_loc = inner_local(mapped, mapped, comp_count)[0]
        cross_re, cross_im = inner_local(mapped, residual, comp_count)
        if iteration > 0:
            coef_pairs = [inner_local(earlier, mapped, comp_count) for earlier in basis_q]
            back_pairs = [inner_local(earlier, residual, comp_count) for earlier in basis_q]
            coef_re = jnp.stack([pair[0] for pair in coef_pairs])
            coef_im = jnp.stack([pair[1] for pair in coef_pairs])
            back_re = jnp.stack([pair[0] for pair in back_pairs])
            back_im = jnp.stack([pair[1] for pair in back_pairs])
        else:
            coef_re = jnp.zeros((1, rhs_count), jnp.float32)
            coef_im = jnp.zeros((1, rhs_count), jnp.float32)
            back_re = jnp.zeros((1, rhs_count), jnp.float32)
            back_im = jnp.zeros((1, rhs_count), jnp.float32)
        square_all, cross_re, cross_im, coef_re, coef_im, back_re, back_im = lax.psum(
            (square_loc, cross_re, cross_im, coef_re, coef_im, back_re, back_im), "ta"
        )
        squared = square_all
        proj_re = cross_re
        proj_im = cross_im
        for number in range(iteration):
            mapped = mapped - scaled(basis_q[number], coef_re[number], coef_im[number], comp_count)
            direction = direction - scaled(
                basis_p[number], coef_re[number], coef_im[number], comp_count
            )
            squared = squared - (
                coef_re[number] * coef_re[number] + coef_im[number] * coef_im[number]
            )
            proj_re = proj_re - (
                coef_re[number] * back_re[number] + coef_im[number] * back_im[number]
            )
            proj_im = proj_im - (
                coef_re[number] * back_im[number] - coef_im[number] * back_re[number]
            )
        factor = 1.0 / jnp.sqrt(squared + 1e-06)
        unit_q = mapped * factor
        unit_p = direction * factor
        alpha_re = proj_re * factor
        alpha_im = proj_im * factor
        solution = solution + scaled(unit_p, alpha_re, alpha_im, comp_count)
        residual = residual - scaled(unit_q, alpha_re, alpha_im, comp_count)
        basis_q.append(unit_q)
        basis_p.append(unit_p)
    return (
        solution.reshape(1, site_count, 2 * comp_count, rhs_count),
        residual.reshape(1, site_count, 2 * comp_count, rhs_count),
    )


MESH = pl.DeviceIdType.MESH


def flipped(number, mask, bits):
    total = 0
    for bit in range(bits):
        size = 1 << bit
        total = total + (((number // size) % 2 + (mask // size) % 2) % 2) * size
    return total


def swapped(value):
    return pltpu.roll(value, value.shape[-1] // 2, value.ndim - 1)


def lower_lanes(shape):
    return lax.broadcasted_iota(jnp.int32, shape, len(shape) - 1) < shape[-1] // 2


def turned(value):
    other = swapped(value)
    return jnp.where(lower_lanes(value.shape), -other, other)


def widened(rounded):
    return jnp.concatenate(
        [rounded, turned(rounded.astype(jnp.float32)).astype(jnp.bfloat16)], axis=0
    )


def times(factor, value):
    return factor[0] * value + factor[1] * turned(value)


def total_wait(region, sem):
    pltpu.make_async_copy(region, region, sem).wait()


def transposed(value, columns, comps):
    row = lax.broadcasted_iota(jnp.int32, value.shape, 0)
    chunk = lax.broadcasted_iota(jnp.int32, value.shape, 1) // comps
    width = value.shape[1]
    bits = columns.bit_length() - 1
    for bit in range(bits):
        size = 1 << bit
        moved = pltpu.roll(value, width - size * comps, 1)
        value = jnp.where((row // size) % 2 == 1, moved, value)
    for bit in range(bits):
        size = 1 << bit
        moved = pltpu.roll(value, size, 0)
        value = jnp.where((chunk // size) % 2 == 1, moved, value)
    for bit in range(bits):
        size = 1 << bit
        moved = pltpu.roll(value, width - size * comps, 1)
        value = jnp.where((row // size) % 2 == 1, moved, value)
    return value


CODE_SCALE = 2.0**12


def coded(rest):
    square = rest * rest * (CODE_SCALE * CODE_SCALE)
    fourth = square * square
    eighth = fourth * fourth
    return jnp.where(rest < 0.0, -eighth, eighth).astype(jnp.bfloat16)


def decoded(code):
    value = code.astype(jnp.float32)
    size = jnp.abs(value)
    fourth = lax.rsqrt(lax.rsqrt(size))
    root = fourth * lax.rsqrt(fourth) * (1.0 / CODE_SCALE)
    root = jnp.where(size >= 2.0**-126, root, 0.0)
    return jnp.where(value < 0.0, -root, root)


def solve_kernel(
    count, sites, comps,
    mass_ref, proj_hbm, fine_hbm, links_hbm,
    sol_ref, res_ref,
    proj_ref, fine_ref, links_ref, near_ref, zlinks_ref, tlinks_ref,
    weights_in, rights_ref, part_keep, part_out, part_in, hi_out, lo_out, lo_in, source_ref,
    first_round, first_z, first_t,
    wide_ref, round_ref, halo_ref, acc_ref, acc_turned, sol_half, res_half, res_turned,
    basis_q, basis_p, turned_q, turned_p, stat_out, stat_in,
    local_sem, wsend, wrecv, psend, precv, ssend, srecv, tsend, trecv, lsend, lrecv, zsend, zrecv,
    hsend, hrecv, gsend, grecv,
):
    me = lax.axis_index("ta")
    bits = count.bit_length() - 1
    core = me % 2
    chip = me // 2
    partner = chip * 2 + 1 - core
    chips = count // 2
    far = chips // 2
    turns = [(1 - 2 * ((me // (1 << bit)) % 2)) * (1 << bit) for bit in range(bits)]
    others = [me]
    for step in range(1, count):
        top = step.bit_length() - 1
        others.append(others[step - (1 << top)] + turns[top])
    null = comps // 2
    rhs = fine_ref.shape[2]
    columns = proj_ref.shape[1]
    width = columns * comps
    groups = comps // columns

    proj_copy = pltpu.make_async_copy(proj_hbm, proj_ref, local_sem.at[2])
    proj_copy.start()
    barrier = pltpu.get_barrier_semaphore()
    for other in others[:0:-1]:
        pl.semaphore_signal(barrier, inc=1, device_id={"ta": other}, device_id_type=MESH)
    fine_copy = pltpu.make_async_copy(fine_hbm, fine_ref, local_sem.at[0])
    fine_copy.start()
    links_copy = pltpu.make_async_copy(links_hbm, links_ref, local_sem.at[1])
    links_copy.start()
    proj_copy.wait()
    pl.semaphore_wait(barrier, count - 1)

    def weights_copy(other, origin):
        return pltpu.make_async_remote_copy(
            src_ref=proj_ref.at[other], dst_ref=weights_in.at[origin],
            send_sem=wsend.at[0], recv_sem=wrecv.at[origin // 2],
            device_id={"ta": other}, device_id_type=MESH,
        )

    quarter = me // (count // 4)
    outer = 1 - (quarter % 3 + 1) // 2
    for step in range(1, 4):
        weights_copy(others[step], me).start()
    for step in range(count // 2, count):
        crossed = step ^ (count // 4)
        weights_copy(outer * others[step] + (1 - outer) * others[crossed], me).start()
    for step in range(4, count // 2):
        weights_copy(others[step], me).start()

    fine_copy.wait()

    def build_right(plane, carry):
        fine = fine_ref[plane].astype(jnp.float32).reshape(columns, 2, 2, null, rhs)
        turned_order = [fine[(columns - at) % columns] for at in range(columns)]
        for half in range(2):
            picked = [
                block[part, half] for block in turned_order for part in range(2)
            ]
            rights_ref[plane, :, half * rhs : (half + 1) * rhs] = jnp.concatenate(
                picked, axis=0
            ).astype(jnp.bfloat16)
        return carry

    lax.fori_loop(0, count, build_right, 0)

    links_copy.wait()
    for site in range(sites):
        near_ref[site] = links_ref[site, :, : 10 * comps]
        zlinks_ref[site] = links_ref[site, :, 10 * comps : 14 * comps]
        tlinks_ref[site] = links_ref[site, :, 14 * comps : 18 * comps]

    def restricted(plane, raw_ref):
        raw = raw_ref[plane].astype(jnp.float32)
        pieces = [
            transposed(raw[:, group * width : (group + 1) * width], columns, comps)
            for group in range(groups)
        ]
        upper = jnp.concatenate(pieces, axis=0)
        lane = lax.broadcasted_iota(jnp.int32, upper.shape, 1) % comps
        lower = jnp.where(
            lane < null, -pltpu.roll(upper, width - null, 1), pltpu.roll(upper, null, 1)
        )
        left = jnp.concatenate([upper, lower], axis=0).astype(jnp.bfloat16)
        total = jnp.dot(left, rights_ref[plane], preferred_element_type=jnp.float32)
        real = jnp.concatenate([total[:null, :rhs], total[null:comps, rhs:]], axis=0)
        imag = jnp.concatenate(
            [total[comps : comps + null, :rhs], total[comps + null :, rhs:]], axis=0
        )
        low = lower_lanes(real.shape)
        return jnp.stack(
            [jnp.where(low, real, swapped(imag)), jnp.where(low, swapped(real), imag)], axis=0
        )

    def part_copy(slot):
        return pltpu.make_async_remote_copy(
            src_ref=part_out.at[slot], dst_ref=part_in.at[slot],
            send_sem=psend.at[0], recv_sem=precv.at[slot],
            device_id={"ta": partner}, device_id_type=MESH,
        )

    def source_copy(slot, origin):
        return pltpu.make_async_remote_copy(
            src_ref=hi_out.at[slot], dst_ref=first_round.at[origin],
            send_sem=ssend.at[0], recv_sem=srecv.at[origin],
            device_id={"ta": flipped(chip, slot, bits - 1) * 2 + core}, device_id_type=MESH,
        )

    def rest_copy(slot, half):
        return pltpu.make_async_remote_copy(
            src_ref=lo_out.at[slot, half], dst_ref=lo_in.at[half, chip],
            send_sem=lsend.at[0], recv_sem=lrecv.at[half],
            device_id={"ta": others[2 * slot]}, device_id_type=MESH,
        )

    def first_t_copy(slot, half):
        return pltpu.make_async_remote_copy(
            src_ref=hi_out.at[slot, half], dst_ref=first_t.at[half, chip],
            send_sem=tsend.at[0], recv_sem=trecv.at[half],
            device_id={"ta": others[2 * (slot ^ far)]}, device_id_type=MESH,
        )

    def pair(step):
        other = flipped(chip, step, bits - 1)
        away = other * 2 + 1 - core
        kept = other * 2 + core
        total_wait(weights_in.at[pl.ds(other * 2, 2)], wrecv.at[other])
        sent, held = restricted(away, weights_in), restricted(kept, weights_in)
        part_out[step] = sent
        part_keep[step] = held
        part_copy(step).start()

    def finish(step):
        part_copy(step).wait_recv()
        total = part_keep[step] + part_in[step]
        rounded = total.astype(jnp.bfloat16)
        hi_out[step] = rounded
        source_copy(step, chip).start()
        lo_out[step] = coded(total - rounded.astype(jnp.float32))

    base = (me // LZ) * LZ
    z_at = me % LZ
    above = base + (z_at + 1) % LZ
    below = base + (z_at + LZ - 1) % LZ
    other_time = (me + LZ) % count
    targets = (other_time, above, below)
    lines = sites // LX

    def first_z_copy(half, which, site):
        return pltpu.make_async_remote_copy(
            src_ref=first_round.at[site, half], dst_ref=first_z.at[half, which, site],
            send_sem=zsend.at[0], recv_sem=zrecv.at[half, which],
            device_id={"ta": targets[1 + which]}, device_id_type=MESH,
        )

    def forward(half, site):
        for which in range(2):
            first_z_copy(half, which, site).start()

    weights_copy(partner, partner).wait_recv()
    sent, held = restricted(partner, weights_in), restricted(me, proj_ref)
    part_out[0] = sent
    part_keep[0] = held
    part_copy(0).start()
    pair(1)
    part_copy(0).wait_recv()
    own = part_keep[0] + part_in[0]
    own_rounded = own.astype(jnp.bfloat16)
    hi_out[0] = own_rounded
    first_round[chip] = own_rounded
    own_rest = coded(own - own_rounded.astype(jnp.float32))
    for half in range(2):
        lo_in[half, chip] = own_rest[half]
    forward(0, chip)

    def arranged(at):
        group = at // 2
        later = outer * ((2 * group + 1) % 3 + 1) + (1 - outer) * (group % 3 + 1)
        return ((group + 2) // 3) * later * 2 + at % 2

    def pair_step(at, carry):
        pair(arranged(at))
        finish(arranged(at - 1))
        return carry

    lax.fori_loop(2, chips, pair_step, 0)
    finish(arranged(chips - 1))

    def send_after(half):
        first_t[half, chip] = hi_out[far, half]
        for step in range(chips - 1, -1, -1):
            if step != far:
                first_t_copy(step, half).start()

    def send_rest(half):
        for step in range(chips - 1, 0, -1):
            rest_copy(step, half).start()

    def forward_all():
        def forward_step(at, carry):
            site = flipped(chip, arranged(at), bits - 1)
            source_copy(0, site).wait_recv()
            forward(0, site)
            return carry

        lax.fori_loop(1, chips, forward_step, 0)

    mass = mass_ref[0]

    def place(site, dx, dy):
        return ((site // LX + dy) % lines) * LX + (site % LX + dx) % LX

    pieces = 2
    span = sites // pieces

    def z_copy(it, half, which):
        return pltpu.make_async_remote_copy(
            src_ref=round_ref.at[it - 1, half], dst_ref=halo_ref.at[it - 1, half, which],
            send_sem=hsend.at[0], recv_sem=hrecv.at[half, which - 1],
            device_id={"ta": targets[which]}, device_id_type=MESH,
        )

    def t_copy(it, half, piece):
        part = pl.ds(piece * span, span)
        return pltpu.make_async_remote_copy(
            src_ref=round_ref.at[it - 1, half, part], dst_ref=halo_ref.at[it - 1, half, 0, part],
            send_sem=hsend.at[0], recv_sem=hrecv.at[half, 2 + piece],
            device_id={"ta": other_time}, device_id_type=MESH,
        )

    def send_t(it, half):
        for piece in range(pieces):
            t_copy(it, half, piece).start()

    def stat_copy(it, half, other):
        return pltpu.make_async_remote_copy(
            src_ref=stat_out.at[it, half], dst_ref=stat_in.at[it, half, me],
            send_sem=gsend.at[0], recv_sem=grecv.at[it, half],
            device_id={"ta": other}, device_id_type=MESH,
        )

    def residual_at(it, half, site):
        return source_ref[half, site] if it == 0 else res_half[it - 1, half, site]

    def rounded_at(it, half, site):
        return first_round[site, half] if it == 0 else round_ref[it - 1, half, site]

    def halo_at(it, half, which, site):
        if it > 0:
            return halo_ref[it - 1, half, which, site]
        return first_t[half, site] if which == 0 else first_z[half, which - 1, site]

    def send_late_halo(it, half):
        pl.when(outer == 1)(lambda: send_t(it, half))

    def near_product(it, half):
        for site in range(sites):
            wide_ref[half, site] = widened(rounded_at(it, half, site))
        steps = ((0, 0), (1, 0), (-1, 0), (0, 1), (0, -1))
        for site in range(sites):
            right = jnp.concatenate(
                [wide_ref[half, place(site, dx, dy)] for dx, dy in steps], axis=0
            )
            acc_ref[it % 2, half, site] = jnp.dot(
                near_ref[site], right, preferred_element_type=jnp.float32
            )

    def z_product(it, half, site):
        right = jnp.concatenate(
            [widened(halo_at(it, half, 2, site)), widened(halo_at(it, half, 1, site))], axis=0
        )
        return acc_ref[it % 2, half, site] + jnp.dot(
            zlinks_ref[site], right, preferred_element_type=jnp.float32
        )

    def t_product(it, half, site):
        wide = widened(halo_at(it, half, 0, site))
        right = jnp.concatenate([wide, wide], axis=0)
        return acc_ref[it % 2, half, site] + jnp.dot(
            tlinks_ref[site], right, preferred_element_type=jnp.float32
        )

    def full_product(it, half, site, product):
        return product + mass * rounded_at(it, half, site).astype(jnp.float32)

    def add_sums(it, half, site, q, sums):
        sums[0] += q * q
        sums[1] += q * residual_at(it, half, site)
        sums[2] += q * res_turned[half, site]
        for j in range(it):
            sums[3 + 2 * j] += basis_q[j, half, site] * q
            sums[4 + 2 * j] += turned_q[j, half, site] * q

    def first_t_product(half):
        total_wait(first_t.at[half, pl.ds(0, sites - 1)], trecv.at[half])
        for site in range(sites):
            acc_ref[0, half, site] = t_product(0, half, site)

    def first_z_product(half):
        for which in range(2):
            total_wait(first_z.at[half, which], zrecv.at[half, which])
        for site in range(sites):
            product = z_product(0, half, site)
            acc_ref[0, half, site] = full_product(0, half, site, product)

    def first_stats(half):
        total_wait(lo_in.at[half, pl.ds(0, sites - 1)], lrecv.at[half])
        sums = [0.0] * 3
        for site in range(sites):
            high = first_round[site, half].astype(jnp.float32)
            whole = high + decoded(lo_in[half, site])
            source_ref[half, site] = whole
            res_turned[half, site] = turned(whole)
            add_sums(0, half, site, acc_ref[0, half, site], sums)
        send_stats(0, half, sums)

    def far_product(it, half):
        for which in (2, 1):
            z_copy(it, half, which).wait_recv()
        for site in range(sites):
            product = z_product(it, half, site)
            acc_ref[it % 2, half, site] = full_product(it, half, site, product)
        sums = [0.0] * (3 + 2 * it)
        for site in range(sites):
            if site % span == 0:
                t_copy(it, half, site // span).wait_recv()
            q = t_product(it, half, site)
            acc_ref[it % 2, half, site] = q
            add_sums(it, half, site, q, sums)
        send_stats(it, half, sums)

    def send_stats(it, half, sums):
        lines_of = [jnp.sum(value, axis=0, keepdims=True) for value in sums]
        lines_of += [jnp.zeros((8 - len(lines_of), rhs), jnp.float32)]
        stats = jnp.concatenate(lines_of, axis=0)
        stats = stats + swapped(stats)
        low = lower_lanes((1, rhs))
        rows = [stats[at : at + 1] for at in range(7)]
        packed = jnp.concatenate(
            [rows[0], jnp.where(low, rows[1], -rows[2])]
            + [jnp.where(low, rows[at], rows[at + 1]) for at in (3, 5)],
            axis=0,
        )
        stat_out[it, half] = packed
        for other in others[:0:-1]:
            stat_copy(it, half, other).start()
        stat_in[it, half, me] = packed
        for site in range(sites):
            acc_turned[half, site] = turned(acc_ref[it % 2, half, site])

    scalars = [([], [], [], []) for _ in range(2)]

    def update(it, half):
        total_wait(stat_in.at[it, half, pl.ds(0, count - 1)], grecv.at[it, half])
        total = jnp.sum(stat_in[it, half], axis=0)
        moved = swapped(total)
        low = lower_lanes(total.shape)
        reals = jnp.where(low, total, moved)
        imags = jnp.where(low, moved, total)
        backs, epsilons, overlaps, _ = scalars[half]
        squared, cross_re, cross_im = reals[0:1], reals[1:2], imags[1:2]
        coefs = [(reals[2 + j : 3 + j], imags[2 + j : 3 + j]) for j in range(it)]
        for j, (c_re, c_im) in enumerate(coefs):
            squared = squared - (c_re * c_re + c_im * c_im) * (1.0 + epsilons[j])
            cross_re = cross_re - (c_re * backs[j][0] + c_im * backs[j][1])
            cross_im = cross_im - (c_re * backs[j][1] - c_im * backs[j][0])
        if it == 2:
            (a_re, a_im), (b_re, b_im) = coefs
            pair_re, pair_im = a_re * b_re + a_im * b_im, a_re * b_im - a_im * b_re
            squared = squared + 2.0 * (pair_re * overlaps[0][0] - pair_im * overlaps[0][1])
        factor = 1.0 / jnp.sqrt(squared + 1e-06)
        alpha = (cross_re * factor, cross_im * factor)
        epsilon = 1e-06 * factor * factor
        if it == 1:
            over = (coefs[0][0] * epsilons[0] * factor, coefs[0][1] * epsilons[0] * factor)
            overlaps.append(over)
            backs[0] = (
                backs[0][0] - (alpha[0] * over[0] - alpha[1] * over[1]),
                backs[0][1] - (alpha[0] * over[1] + alpha[1] * over[0]),
            )
        backs.append((alpha[0] * epsilon, alpha[1] * epsilon))
        epsilons.append(epsilon)
        gamma = (alpha[0] * factor, alpha[1] * factor)
        betas = [
            (gamma[0] * c_re - gamma[1] * c_im, gamma[0] * c_im + gamma[1] * c_re)
            for c_re, c_im in coefs
        ]
        for site in range(sites):
            change = gamma[0] * acc_ref[it % 2, half, site] + gamma[1] * acc_turned[half, site]
            for j, beta in enumerate(betas):
                change -= beta[0] * basis_q[j, half, site] + beta[1] * turned_q[j, half, site]
            new_res = residual_at(it, half, site) - change
            if it < ITERS - 1:
                res_half[it, half, site] = new_res
                round_ref[it, half, site] = new_res.astype(jnp.bfloat16)
                if site % span == span - 1:
                    pl.when(outer == 0)(lambda: t_copy(it + 1, half, site // span).start())
            elif half == 0:
                res_half[it, half, site] = new_res
            else:
                unpack(res_ref, site, res_half[it, 0, site], new_res)
        if it < ITERS - 1:
            for which in range(1, 3):
                z_copy(it + 1, half, which).start()

        def remaining():
            for site in range(sites):
                residual = residual_at(it, half, site)
                step = gamma[0] * residual + gamma[1] * res_turned[half, site]
                for j, beta in enumerate(betas):
                    step -= beta[0] * basis_p[j, half, site] + beta[1] * turned_p[j, half, site]
                new_sol = step if it == 0 else sol_half[half, site] + step
                if it == ITERS - 1 and half == 1:
                    unpack(sol_ref, site, sol_half[0, site], new_sol)
                else:
                    sol_half[half, site] = new_sol
                if it < ITERS - 1:
                    q = acc_ref[it % 2, half, site]
                    p = residual
                    for j, (c_re, c_im) in enumerate(coefs):
                        q -= c_re * basis_q[j, half, site] + c_im * turned_q[j, half, site]
                        p -= c_re * basis_p[j, half, site] + c_im * turned_p[j, half, site]
                    q = q * factor
                    p = p * factor
                    basis_q[it, half, site] = q
                    basis_p[it, half, site] = p
                    turned_q[it, half, site] = turned(q)
                    turned_p[it, half, site] = turned(p)
                    res_turned[half, site] = turned(res_half[it, half, site])

        return remaining

    def unpack(to_ref, site, first, second):
        low = lower_lanes(first.shape)
        to_ref[site, :comps] = jnp.where(low, first, swapped(second))
        to_ref[site, comps:] = jnp.where(low, swapped(first), second)

    send_after(0)
    pl.when(outer == 0)(lambda: send_rest(0))
    forward_all()
    pl.when(outer == 1)(lambda: send_rest(0))
    near_product(0, 0)
    near_product(0, 1)
    for site in range(sites):
        forward(1, site)
    send_after(1)
    first_t_product(0)
    send_rest(1)
    first_z_product(0)
    first_stats(0)
    first_t_product(1)
    first_z_product(1)
    first_stats(1)
    for it in range(ITERS):
        if it > 0:
            for half in range(2):
                far_product(it, half)
        for half in range(2):
            remaining = update(it, half)
            if it < ITERS - 1:
                near_product(it + 1, half)
            remaining()
            if it < ITERS - 1:
                send_late_halo(it + 1, half)

    total_wait(proj_ref.at[pl.ds(0, count - 1)], wsend.at[0])
    total_wait(part_out, psend.at[0])
    total_wait(hi_out.at[pl.ds(0, chips - 1)], ssend.at[0])
    total_wait(lo_out.at[pl.ds(0, chips - 1)], lsend.at[0])
    total_wait(hi_out.at[pl.ds(0, chips - 1)], tsend.at[0])
    total_wait(first_z, zsend.at[0])
    total_wait(halo_ref, hsend.at[0])
    total_wait(stat_in.at[:, :, pl.ds(0, count - 1)], gsend.at[0])


def store_kernel(sol_ref, res_ref, sol_hbm, res_hbm, sems):
    copies = [
        pltpu.make_async_copy(from_ref, to_ref, sems.at[at])
        for at, (from_ref, to_ref) in enumerate(((sol_ref, sol_hbm), (res_ref, res_hbm)))
    ]
    for copy in copies:
        copy.start()
    for copy in copies:
        copy.wait()


def stored(sol, res):
    vmem = pl.BlockSpec(memory_space=pltpu.VMEM)
    hbm = pl.BlockSpec(memory_space=pltpu.HBM)
    return pl.pallas_call(
        store_kernel,
        out_shape=[jax.ShapeDtypeStruct(value.shape, value.dtype) for value in (sol, res)],
        in_specs=[vmem, vmem],
        out_specs=[hbm, hbm],
        scratch_shapes=[pltpu.SemaphoreType.DMA((2,))],
        compiler_params=pltpu.CompilerParams(vmem_limit_bytes=1024 * 1024),
    )(sol, res)


def shards_kernel(fine_source, projectors, stencil_links, quark_mass):
    count = lax.axis_size("ta")
    planes, local_columns, _, _, null, rhs = fine_source.shape
    sites, comps = stencil_links.shape[1], stencil_links.shape[2]
    rows = local_columns * 4 * null
    fine = fine_source.reshape(planes, rows, rhs)
    proj = projectors.reshape(count, local_columns, 4 * null * null)
    width = local_columns * comps
    links = stencil_links.reshape(sites, comps, 18 * comps)
    chips = count // 2
    vector = (sites, 2 * comps, rhs)
    f32, bf16 = jnp.float32, jnp.bfloat16
    dma = pltpu.SemaphoreType.DMA
    vmem = pl.BlockSpec(memory_space=pltpu.VMEM)
    hbm = pl.BlockSpec(memory_space=pltpu.HBM)
    parts = (chips, 2, comps, rhs)
    half = (sites, comps, rhs)
    sol, res = pl.pallas_call(
        functools.partial(solve_kernel, count, sites, comps),
        out_shape=[pltpu.VMEM(vector, f32)] * 2,
        in_specs=[pl.BlockSpec(memory_space=pltpu.SMEM), hbm, hbm, hbm],
        out_specs=[vmem, vmem],
        scratch_shapes=[
            pltpu.VMEM(proj.shape, bf16),
            pltpu.VMEM(fine.shape, bf16),
            pltpu.VMEM(links.shape, bf16),
            pltpu.VMEM((sites, comps, 10 * comps), bf16),
            pltpu.VMEM((sites, comps, 4 * comps), bf16),
            pltpu.VMEM((sites, comps, 4 * comps), bf16),
            pltpu.VMEM(proj.shape, bf16),
            pltpu.VMEM((planes, width, 2 * rhs), bf16),
            pltpu.VMEM(parts, f32),
            pltpu.VMEM(parts, f32),
            pltpu.VMEM(parts, f32),
            pltpu.VMEM(parts, bf16),
            pltpu.VMEM(parts, bf16),
            pltpu.VMEM((2, sites, comps, rhs), bf16),
            pltpu.VMEM((2, sites, comps, rhs), f32),
            pltpu.VMEM((sites, 2, comps, rhs), bf16),
            pltpu.VMEM((2, 2, sites, comps, rhs), bf16),
            pltpu.VMEM((2, sites, comps, rhs), bf16),
            pltpu.VMEM((2, sites, 2 * comps, rhs), bf16),
            pltpu.VMEM((ITERS - 1, 2, *half), bf16),
            pltpu.VMEM((ITERS - 1, 2, 3, *half), bf16),
            pltpu.VMEM((2, 2, *half), f32),
            pltpu.VMEM((2, *half), f32),
            pltpu.VMEM((2, *half), f32),
            pltpu.VMEM((ITERS, 2, *half), f32),
            pltpu.VMEM((2, *half), f32),
            pltpu.VMEM((ITERS - 1, 2, *half), f32),
            pltpu.VMEM((ITERS - 1, 2, *half), f32),
            pltpu.VMEM((ITERS - 1, 2, *half), f32),
            pltpu.VMEM((ITERS - 1, 2, *half), f32),
            pltpu.VMEM((ITERS, 2, 4, rhs), f32),
            pltpu.VMEM((ITERS, 2, count, 4, rhs), f32),
            dma((3,)),
            dma((1,)),
            dma((chips,)),
            dma((1,)),
            dma((chips,)),
            dma((1,)),
            dma((chips,)),
            dma((1,)),
            dma((2,)),
            dma((1,)),
            dma((2,)),
            dma((1,)),
            dma((2, 2)),
            dma((1,)),
            dma((2, 4)),
            dma((1,)),
            dma((ITERS, 2)),
        ],
        compiler_params=pltpu.CompilerParams(
            collective_id=0, has_side_effects=True, vmem_limit_bytes=60 * 1024 * 1024
        ),
    )(quark_mass, proj, fine, links)
    sol, res = stored(sol, res)
    return sol.reshape(1, *vector), res.reshape(1, *vector)


def shards(fine_source, projectors, stencil_links, quark_mass):
    count = lax.axis_size("ta")
    sites = stencil_links.shape[1]
    local_columns = fine_source.shape[1]
    block = projectors.shape[1] // sites
    fits = (
        count == 2 * LZ
        and count == 2 * sites
        and count & (count - 1) == 0
        and block == 2 * local_columns
        and stencil_links.shape[2] % local_columns == 0
        and fine_source.shape[0] == count
        and ITERS == 3
        and fine_source.shape[5] % 2 == 0
    )
    chosen = shards_kernel if fits else shards_general
    return chosen(fine_source, projectors, stencil_links, quark_mass)


def solution(mesh):
    return jax.shard_map(
        shards,
        mesh=mesh,
        in_specs=(
            P("cfg", "ta", None, None, None, None),
            P(("cfg", "ta"), None, None),
            P(("cfg", "ta"), None, None, None),
            P("cfg"),
        ),
        out_specs=(P(("cfg", "ta"), None, None, None), P(("cfg", "ta"), None, None, None)),
        check_vma=False,
    )
```
